32 devices in a mesh: dp: 1 (over z), tp: 4 (over y), cp: 8 (over x, core).
Axes of the slice: x: 4, y: 4, z: 1, core: 2. Of those that a mesh axis runs over, the one named last changes fastest.
The devices are a block of a 4x4x8 slice.
Arguments:
- x: bfloat16 [2048, 5120], P(('dp', 'cp'))
- k_cache: bfloat16 [32768, 8, 128], P(('dp', 'cp'), 'tp')
- v_cache: bfloat16 [32768, 8, 128], P(('dp', 'cp'), 'tp')
- rope_table: float32 [2048, 64], P(('dp', 'cp'))
- norm_gain: bfloat16 [5120], replicated
- w_qkv: bfloat16 [5120, 14336], P(None, 'tp')
- b_qkv: bfloat16 [14336], P('tp')
- w_out: bfloat16 [12288, 5120], P('tp')
Outputs:
- output 1: bfloat16 [2048, 5120], P(('dp', 'cp'))
- output 2: bfloat16 [2048, 8, 128], P(('dp', 'cp'), 'tp')
- output 3: bfloat16 [2048, 8, 128], P(('dp', 'cp'), 'tp')
All inputs are finite; a program needn't handle non-finite values.
Results may differ from the reference program's by a relative error of at most 0.00328593.
Values are sent between devices in bfloat16 or wider.
A program may use at most 768 MiB of HBM per device.

```python
import math
import jax
import jax.numpy as jnp
from jax import lax

D = 5120
HEADS = 96
KV_HEADS = 8
HEAD = 128
NEW_TOKENS = 2048
PREFIX = 32768
EPS = 1.5625e-07
MASK_VALUE = -1e30
GROUP = HEADS // KV_HEADS
QKV_WIDTH = (HEADS + 2 * KV_HEADS) * HEAD
PAIR_COUNT = HEAD // 4
QUERY_BLOCK = math.gcd(NEW_TOKENS, 128)
KEY_BLOCK = math.gcd(PREFIX + NEW_TOKENS, 512)


def setup_inputs(seed: int = 0, part: int = 0) -> dict:
    part_keys = jax.random.split(jax.random.fold_in(jax.random.key(seed), part), 4)
    shared_keys = jax.random.split(jax.random.key(seed + 1), 4)
    x = jax.random.normal(part_keys[0], (NEW_TOKENS, D), jnp.float32)
    k_cache = 1.6 * jax.random.normal(part_keys[1], (PREFIX, KV_HEADS, HEAD), jnp.float32)
    v_cache = 1.6 * jax.random.normal(part_keys[2], (PREFIX, KV_HEADS, HEAD), jnp.float32)
    log_ratio = jax.random.uniform(part_keys[3], (), jnp.float32, math.log(100.0), math.log(10000.0))
    rope_base = 10000.0 * jnp.exp(log_ratio)
    inv_freq = rope_base ** (-jnp.arange(PAIR_COUNT, dtype=jnp.float32) / PAIR_COUNT)
    positions = (PREFIX + jnp.arange(NEW_TOKENS)).astype(jnp.float32)
    angles = positions[:, None] * inv_freq[None, :]
    rope_table = jnp.concatenate([jnp.cos(angles), jnp.sin(angles)], axis=1)
    norm_gain = 1.0 + 0.3 * jax.random.normal(shared_keys[0], (D,), jnp.float32)
    w_qkv = jax.random.normal(shared_keys[1], (D, QKV_WIDTH), jnp.float32) * (1.5 / math.sqrt(D))
    b_qkv = 0.5 * jax.random.normal(shared_keys[2], (QKV_WIDTH,), jnp.float32)
    w_out = jax.random.normal(shared_keys[3], (HEADS * HEAD, D), jnp.float32) / math.sqrt(HEADS * HEAD)
    return dict(x=x.astype(jnp.bfloat16), k_cache=k_cache.astype(jnp.bfloat16), v_cache=v_cache.astype(jnp.bfloat16), rope_table=rope_table.astype(jnp.float32), norm_gain=norm_gain.astype(jnp.bfloat16), w_qkv=w_qkv.astype(jnp.bfloat16), b_qkv=b_qkv.astype(jnp.bfloat16), w_out=w_out.astype(jnp.bfloat16))


def apply_rotary(vals, cos_t, sin_t):
    pair_count = cos_t.shape[-1]
    lead_shape = vals.shape[:-1]
    paired = vals[..., :2 * pair_count].reshape(lead_shape + (pair_count, 2))
    even_part = paired[..., 0]
    odd_part = paired[..., 1]
    turned = jnp.stack([even_part * cos_t - odd_part * sin_t, odd_part * cos_t + even_part * sin_t], axis=-1)
    return jnp.concatenate([turned.reshape(lead_shape + (2 * pair_count,)), vals[..., 2 * pair_count:]], axis=-1)


def reference(x, k_cache, v_cache, rope_table, norm_gain, w_qkv, b_qkv, w_out):
    x_f32 = x.astype(jnp.float32)
    inv_rms = lax.rsqrt(jnp.mean(x_f32 * x_f32, axis=-1, keepdims=True) + EPS)
    hidden = (x_f32 * inv_rms * norm_gain.astype(jnp.float32)).astype(jnp.bfloat16)
    qkv_all = jnp.dot(hidden, w_qkv, preferred_element_type=jnp.float32) + b_qkv.astype(jnp.float32)
    qkv_all = qkv_all.reshape(NEW_TOKENS, KV_HEADS, GROUP + 2, HEAD)
    cos_t = rope_table[:, :PAIR_COUNT]
    sin_t = rope_table[:, PAIR_COUNT:]
    queries = apply_rotary(qkv_all[:, :, :GROUP], cos_t[:, None, None], sin_t[:, None, None]).astype(jnp.bfloat16)
    new_k = apply_rotary(qkv_all[:, :, GROUP], cos_t[:, None], sin_t[:, None]).astype(jnp.bfloat16)
    new_v = qkv_all[:, :, GROUP + 1].astype(jnp.bfloat16)
    key_count = PREFIX + NEW_TOKENS
    key_blocks = key_count // KEY_BLOCK
    keys_all = jnp.concatenate([k_cache, new_k], axis=0).reshape(key_blocks, KEY_BLOCK, KV_HEADS, HEAD)
    vals_all = jnp.concatenate([v_cache, new_v], axis=0).reshape(key_blocks, KEY_BLOCK, KV_HEADS, HEAD)
    key_pos = jnp.arange(key_count).reshape(key_blocks, KEY_BLOCK)
    q_blocks = queries.reshape(NEW_TOKENS // QUERY_BLOCK, QUERY_BLOCK, KV_HEADS, GROUP, HEAD)
    q_pos = (PREFIX + jnp.arange(NEW_TOKENS)).reshape(NEW_TOKENS // QUERY_BLOCK, QUERY_BLOCK)
    scale = HEAD ** -0.5

    def query_block(block):
        q_vals, q_at = block
        q_f32 = q_vals.astype(jnp.float32)

        def key_step(carry, kv_block):
            run_max, run_sum, weighted = carry
            k_vals, v_vals, k_at = kv_block
            scores = jnp.einsum('qngd,knd->qngk', q_f32, k_vals.astype(jnp.float32)) * scale
            visible = (k_at[None, :] <= q_at[:, None])[:, None, None, :]
            scores = jnp.where(visible, scores, MASK_VALUE)
            new_max = jnp.maximum(run_max, scores.max(axis=-1))
            rescale = jnp.exp(run_max - new_max)
            probs = jnp.exp(scores - new_max[..., None])
            run_sum = run_sum * rescale + probs.sum(axis=-1)
            weighted = weighted * rescale[..., None] + jnp.einsum('qngk,knd->qngd', probs.astype(jnp.bfloat16).astype(jnp.float32), v_vals.astype(jnp.float32))
            return (new_max, run_sum, weighted), None

        start_carry = (jnp.full((QUERY_BLOCK, KV_HEADS, GROUP), MASK_VALUE, jnp.float32), jnp.zeros((QUERY_BLOCK, KV_HEADS, GROUP), jnp.float32), jnp.zeros((QUERY_BLOCK, KV_HEADS, GROUP, HEAD), jnp.float32))
        (run_max, run_sum, weighted), _ = lax.scan(key_step, start_carry, (keys_all, vals_all, key_pos))
        return weighted / run_sum[..., None]

    attn = lax.map(query_block, (q_blocks, q_pos))
    attn = attn.reshape(NEW_TOKENS, HEADS * HEAD).astype(jnp.bfloat16)
    y = (x_f32 + jnp.dot(attn, w_out, preferred_element_type=jnp.float32)).astype(jnp.bfloat16)
    return y, new_k, new_v
```

```python
import functools
import math

import jax
import jax.numpy as jnp
from jax import lax
from jax.experimental import pallas as pl
from jax.experimental.pallas import tpu as pltpu
from jax.sharding import PartitionSpec as P

EPS = 1.5625e-07
MASK_VALUE = -1e30
LANES = 128
SUB = 256
NC = 512
PHASE_TOKENS = 128
CHUNKS = 4
MESH = pl.DeviceIdType.MESH
F32 = jnp.float32
BF16 = jnp.bfloat16


def dot(a, b, dims=(((1,), (0,)), ((), ()))):
    return lax.dot_general(a, b, dims, preferred_element_type=F32)


def relayout_kernel(k_ref, v_ref, out_ref):
    rows = 2 * LANES
    wide = lax.broadcasted_iota(jnp.int32, (rows, rows), 0)
    tall = lax.broadcasted_iota(jnp.int32, (rows, rows), 1)
    pick = (wide // 2 + (wide % 2) * LANES == tall).astype(BF16)
    pick_t = (tall // 2 + (tall % 2) * LANES == wide).astype(BF16)
    for i in range(k_ref.shape[0] // rows):
        here = slice(i * LANES, (i + 1) * LANES)
        keys = dot(pick_t, k_ref[i * rows:(i + 1) * rows, :]).astype(BF16)
        vals = dot(v_ref[i * rows:(i + 1) * rows, :], pick, (((0,), (0,)), ((), ()))).astype(BF16)
        for g in range(2):
            out_ref[0, g, 0, here, :] = keys[g * LANES:(g + 1) * LANES, :]
            out_ref[0, g, 1, here, :] = vals[:, g * LANES:(g + 1) * LANES]


def relayout_cache(k_cache, v_cache):
    positions, groups, head_dim = k_cache.shape
    part = positions // CHUNKS
    flat = (positions * groups, head_dim)
    in_spec = pl.BlockSpec((part * groups, head_dim), lambda i: (i, 0))
    return pl.pallas_call(
        relayout_kernel,
        grid=(CHUNKS,),
        in_specs=[in_spec, in_spec],
        out_specs=pl.BlockSpec((1, groups, 2, part, head_dim), lambda i: (i, 0, 0, 0, 0)),
        out_shape=jax.ShapeDtypeStruct((CHUNKS, groups, 2, part, head_dim), BF16),
        compiler_params=pltpu.CompilerParams(vmem_limit_bytes=40 << 20),
        name="relayout",
    )(k_cache.reshape(flat), v_cache.reshape(flat))


def project_kernel(pairs_per_group, x_ref, g_ref, w_ref, b_ref, table_ref, qt_ref, kvn_ref, kn_ref, vn_ref, hid_ref, cos_ref, sin_ref):
    step = pl.program_id(0)
    tok = x_ref.shape[0]
    pair_count = table_ref.shape[1] // 2
    lane = lax.broadcasted_iota(jnp.int32, (tok, LANES), 1)

    @pl.when(step == 0)
    def _():
        x = x_ref[...].astype(F32)
        inv_rms = lax.rsqrt(jnp.mean(x * x, axis=-1, keepdims=True) + EPS)
        hid_ref[...] = (x * inv_rms * g_ref[...].astype(F32)).astype(BF16)
        table = jnp.concatenate([table_ref[...], jnp.zeros((tok, LANES - 2 * pair_count), F32)], axis=1)
        at = jnp.where(lane < 2 * pair_count, lane // 2, 0)
        cos_ref[...] = jnp.take_along_axis(table, at, axis=1)
        sin = jnp.take_along_axis(table, at + pair_count, axis=1)
        sin_ref[...] = jnp.where(lane % 2 == 0, -sin, sin)

    def rotate(head):
        swapped = jnp.where(lane % 2 == 0, pltpu.roll(head, LANES - 1, 1), pltpu.roll(head, 1, 1))
        turned = head * cos_ref[...] + swapped * sin_ref[...]
        return jnp.where(lane < 2 * pair_count, turned, head)

    both = dot(hid_ref[...], w_ref[...]) + b_ref[...].astype(F32)
    first, second = both[:, :LANES], both[:, LANES:]
    kind = lax.rem(step, pairs_per_group)

    @pl.when(kind < pairs_per_group - 1)
    def _():
        for j, head in enumerate((first, second)):
            turned = rotate(head).T.astype(BF16)
            for p in range(tok // PHASE_TOKENS):
                qt_ref[0, p, 0, :, j * LANES:(j + 1) * LANES] = turned[:, p * PHASE_TOKENS:(p + 1) * PHASE_TOKENS]

    @pl.when(kind == pairs_per_group - 1)
    def _():
        keys = rotate(first).astype(BF16)
        kvn_ref[0, 0] = keys
        kn_ref[...] = keys
        vn_ref[...] = second.astype(BF16)
        for i in range(tok // LANES):
            here = slice(i * LANES, (i + 1) * LANES)
            kvn_ref[0, 1, here, :] = second[here, :].T.astype(BF16)


def project_new(x, rope_table, norm_gain, w_qkv, b_qkv, groups):
    tok, width = x.shape
    cols = w_qkv.shape[1]
    per_group = cols // groups // (2 * LANES)
    query_heads = cols // groups // LANES - 2
    phases = tok // PHASE_TOKENS
    heads_per_tile = NC // PHASE_TOKENS
    tiles = query_heads // heads_per_tile
    steps_per_tile = heads_per_tile // 2

    def qt_map(i):
        j = jnp.minimum(i % per_group, per_group - 2)
        return (i // per_group, 0, j // steps_per_tile, 0, j % steps_per_tile)

    full = lambda shape: pl.BlockSpec(shape, lambda i: (0,) * len(shape))
    return pl.pallas_call(
        functools.partial(project_kernel, per_group),
        grid=(groups * per_group,),
        in_specs=[
            full((tok, width)),
            full((1, width)),
            pl.BlockSpec((width, 2 * LANES), lambda i: (0, i)),
            pl.BlockSpec((1, 2 * LANES), lambda i: (0, i)),
            full(rope_table.shape),
        ],
        out_specs=[
            pl.BlockSpec((1, phases, 1, LANES, 2 * LANES), qt_map),
            pl.BlockSpec((1, 2, tok, LANES), lambda i: (i // per_group, 0, 0, 0)),
            pl.BlockSpec((tok, LANES), lambda i: (0, i // per_group)),
            pl.BlockSpec((tok, LANES), lambda i: (0, i // per_group)),
        ],
        out_shape=[
            jax.ShapeDtypeStruct((groups, phases, tiles, LANES, NC), BF16),
            jax.ShapeDtypeStruct((groups, 2, tok, LANES), BF16),
            jax.ShapeDtypeStruct((tok, groups * LANES), BF16),
            jax.ShapeDtypeStruct((tok, groups * LANES), BF16),
        ],
        scratch_shapes=[pltpu.VMEM((tok, width), BF16), pltpu.VMEM((tok, LANES), F32), pltpu.VMEM((tok, LANES), F32)],
        compiler_params=pltpu.CompilerParams(vmem_limit_bytes=40 << 20),
        name="project",
    )(x, norm_gain.reshape(1, width), w_qkv, b_qkv.reshape(1, cols), rope_table)


def attention_kernel(n, heads, phases, qt_ref, kv_ref, kvn_ref, o_ref, ring_ref, ringn_ref,
                     k_buf, v_buf, s_ref, p_ref, acc_ref, m_ref, l_ref, mc_ref, al_ref, bias_ref,
                     fetch_sem, newest_sem, own_send, pair_send, hop_send, new_send, recv, new_recv):
    me = lax.axis_index("cp")
    pair = me + 1 - 2 * lax.rem(me, 2)
    right, left = lax.rem(me + 2, n), lax.rem(me + n - 2, n)
    groups, part = kv_ref.shape[1], kv_ref.shape[3]
    tok = kvn_ref.shape[2]
    span = CHUNKS * part
    span_new = n * tok
    sets = n
    per_group = qt_ref.shape[0] // groups
    spare = qt_ref.shape[0]
    scale = LANES ** -0.5 * math.log2(math.e)

    def remote(src, dst, send, got, where):
        return pltpu.make_async_remote_copy(src_ref=src, dst_ref=dst, send_sem=send, recv_sem=got, device_id={"cp": where}, device_id_type=MESH)

    def own_pair(c):
        return remote(kv_ref.at[c], ring_ref.at[1, c], own_send.at[0, c], recv.at[1, c], pair)

    def own_right(c):
        return remote(kv_ref.at[c], ring_ref.at[2 + c, 0], own_send.at[1, c], recv.at[2 + c, 0], right)

    def own_left(c):
        return remote(kv_ref.at[c], ring_ref.at[2 + c, 1], own_send.at[2, c], recv.at[2 + c, 1], left)

    def to_pair(s, side):
        return remote(ring_ref.at[s, side], ring_ref.at[s, 2 + side], pair_send.at[s, side], recv.at[s, 2 + side], pair)

    def hop_right(s):
        return remote(ring_ref.at[s, 0], ring_ref.at[s + 4, 0], hop_send.at[s], recv.at[s + 4, 0], right)

    def hop_left(s):
        return remote(ring_ref.at[s, 1], ring_ref.at[s + 2, 1], hop_send.at[s], recv.at[s + 2, 1], left)

    def new_copy(source, send, got, where, own=False):
        src = kvn_ref if own else ringn_ref.at[source]
        return remote(src, ringn_ref.at[source], new_send.at[send], new_recv.at[got], where)

    far = lax.rem(me + 4, n)
    new_right = new_copy(me, 0, 0, right, own=True)
    new_left = new_copy(me, 1, 1, left, own=True)
    new_pair = new_copy(me, 2, 3, pair, own=True)
    new_hop = new_copy(left, 3, 2, right)
    new_left_pair = new_copy(left, 4, 4, pair)
    new_right_pair = new_copy(right, 5, 5, pair)
    new_far_pair = new_copy(far, 6, 6, pair)

    barrier = pltpu.get_barrier_semaphore()
    for other in (pair, right, left):
        pl.semaphore_signal(barrier, inc=1, device_id={"cp": other}, device_id_type=MESH)
    pl.semaphore_wait(barrier, 3)
    for c in range(CHUNKS):
        own_right(c).start()
        own_left(c).start()
        own_pair(c).start()
    for copy in (new_right, new_left, new_pair):
        copy.start()

    def fetch_copies(source, slot, g):
        copies = []
        for c in range(CHUNKS):
            here = pl.ds(c * part, part)
            copies.append(pltpu.make_async_copy(source(c).at[g, 0], k_buf.at[slot, here], fetch_sem.at[slot, 0, c]))
            copies.append(pltpu.make_async_copy(source(c).at[g, 1], v_buf.at[slot, here], fetch_sem.at[slot, 1, c]))
        return copies

    def fetch_new(act):
        for g in range(groups):
            for j in range(n):
                here = pl.ds(g * span_new + j * tok, tok)

                def both(source):
                    for kind, buf in ((0, k_buf), (1, v_buf)):
                        copy = pltpu.make_async_copy(source.at[g, kind], buf.at[0, here], newest_sem.at[kind, g, j])
                        getattr(copy, act)()

                if act == "wait":
                    both(kvn_ref)
                else:
                    pl.when(j == me)(lambda: both(kvn_ref))
                    pl.when(j != me)(lambda: both(ringn_ref.at[j]))

    own = lambda c: kv_ref.at[c]
    for copy in fetch_copies(own, 0, 0):
        copy.start()

    row = lax.broadcasted_iota(jnp.int32, (tok, NC), 0)
    col = lax.rem(lax.broadcasted_iota(jnp.int32, (tok, NC), 1), PHASE_TOKENS)
    bias_ref[0] = jnp.zeros((tok, NC), F32)
    for p in range(phases):
        bias_ref[1 + p] = jnp.where(row <= col + p * PHASE_TOKENS, 0.0, MASK_VALUE)
    bias_ref[1 + phases] = jnp.full((tok, NC), MASK_VALUE, F32)

    m_ref[...] = jnp.full(m_ref.shape, MASK_VALUE, F32)
    l_ref[...] = jnp.zeros(l_ref.shape, F32)
    acc_ref[...] = jnp.zeros(acc_ref.shape, F32)
    s_ref[...] = jnp.zeros(s_ref.shape, F32)
    p_ref[...] = jnp.zeros(p_ref.shape, BF16)
    mc_ref[...] = jnp.zeros(mc_ref.shape, F32)
    al_ref[...] = jnp.ones(al_ref.shape, F32)

    def step(a=None, b=None, c=None):
        alpha_b, alpha_c = al_ref[0], al_ref[1]
        shift = mc_ref[...]
        run = {"max": None, "sum": None, "out": None}

        def scores(i):
            keys = k_buf[a["slot"], pl.ds(a["base"] + i * SUB, SUB), :]
            s = dot(keys, qt_ref[a["tile"]])
            if a["new"]:
                edge = 1 + lax.rem(a["tile"], per_group) // (per_group // phases)
                which = jnp.where(i < me, 0, jnp.where(i == me, edge, 1 + phases))
                s = s + bias_ref[which]
            s_ref[i * SUB:(i + 1) * SUB, :] = s
            top = jnp.max(s.reshape(SUB // 8, 8, NC), axis=0)
            run["max"] = top if run["max"] is None else jnp.maximum(run["max"], top)

        def weights(i):
            s = s_ref[i * SUB:(i + 1) * SUB, :]
            e = jnp.exp2((s * scale).reshape(SUB // 8, 8, NC) - shift[None])
            part_sum = jnp.sum(e, axis=0)
            run["sum"] = part_sum if run["sum"] is None else run["sum"] + part_sum
            p_ref[i * SUB:(i + 1) * SUB, :] = e.reshape(SUB, NC).astype(BF16)

        def values(i):
            at = c["base"] + i * SUB
            block = jnp.concatenate([v_buf[c["slot"], pl.ds(at + h * LANES, LANES), :] for h in range(SUB // LANES)], axis=1)
            out = dot(block, p_ref[i * SUB:(i + 1) * SUB, :])
            run["out"] = out if run["out"] is None else run["out"] + out

        stages = ((c, values), (b, weights), (a, scores))
        for i in range(max(spec["keys"] for spec, _ in stages if spec is not None) // SUB):
            for spec, stage in stages:
                if spec is not None and i < spec["keys"] // SUB:
                    stage(i)
        if c is not None:
            acc_ref[c["tile"]] = acc_ref[c["tile"]] * alpha_c + run["out"]
        if b is not None:
            l_ref[b["tile"]] = l_ref[b["tile"]] * alpha_b + run["sum"]
            al_ref[1] = alpha_b
        if a is not None:
            old = m_ref[a["tile"]]
            new = jnp.maximum(old, jnp.max(run["max"], axis=0, keepdims=True))
            m_ref[a["tile"]] = new
            mc_ref[...] = jnp.broadcast_to(new * scale, mc_ref.shape)
            al_ref[0] = jnp.exp2((old - new) * scale)

    def main(tile, slot):
        return {"tile": tile, "slot": slot, "base": 0, "keys": span, "new": False}

    def recent(at):
        return {"tile": at, "slot": 0, "base": at // per_group * span_new, "keys": span_new, "new": True}

    def one_set(st, _):
        for g in range(groups):
            for copy in fetch_copies(own, g, g):
                copy.wait()
            if g == groups - 1:
                nxt = st + 1

                @pl.when((st >= 1) & (st <= sets - 2))
                def _():
                    remote(kv_ref.at[0], ring_ref.at[nxt, 0], own_send.at[0, 0], recv.at[nxt, 0], left).wait_recv()
                    to_pair(nxt, 0).start()
                    remote(kv_ref.at[0], ring_ref.at[nxt, 1], own_send.at[0, 0], recv.at[nxt, 1], right).wait_recv()
                    to_pair(nxt, 1).start()

                @pl.when((st >= 1) & (st <= 2))
                def _():
                    hop_right(nxt).start()

                @pl.when((st >= 3) & (st <= 4))
                def _():
                    hop_left(nxt).start()

                @pl.when(st == sets - 3)
                def _():
                    new_copy(left, 0, 0, right).wait_recv()
                    new_hop.start()
                    new_left_pair.start()
                    new_copy(right, 0, 1, left).wait_recv()
                    new_right_pair.start()

                @pl.when(st == sets - 2)
                def _():
                    new_copy(far, 0, 2, right).wait_recv()
                    new_far_pair.start()

            def one_tile(t, _):
                @pl.when(t == per_group - 2)
                def _():
                    if g < groups - 1:
                        @pl.when(st == 0)
                        def _():
                            for copy in fetch_copies(own, g + 1, g + 1):
                                copy.start()

                        @pl.when(st > 0)
                        def _():
                            for copy in fetch_copies(lambda c: ring_ref.at[st, c], g + 1, g + 1):
                                copy.start()
                    else:
                        @pl.when(st == 0)
                        def _():
                            for c in range(CHUNKS):
                                own_pair(c).wait_recv()

                        @pl.when((st >= 1) & (st <= sets - 2))
                        def _():
                            for side in range(2):
                                to_pair(st + 1, side).wait_recv()

                        @pl.when(st <= sets - 2)
                        def _():
                            for copy in fetch_copies(lambda c: ring_ref.at[st + 1, c], 0, 0):
                                copy.start()

                before = (groups + g - 1) % groups
                early = (st == 0) & (g == 0)
                last = jnp.where(t >= 1, g * per_group + t - 1, jnp.where(early, spare, before * per_group + per_group - 1))
                older = jnp.where(t >= 2, g * per_group + t - 2, jnp.where(early, spare, before * per_group + per_group - 2 + t))
                step(main(g * per_group + t, g), main(last, 0), main(older, jnp.where(t >= 2, g, before)))
                return 0

            lax.fori_loop(0, per_group, one_tile, 0)
        return 0

    lax.fori_loop(0, sets, one_set, 0)

    for got in (3, 4, 5, 6):
        new_copy(pair, 0, got, pair).wait_recv()
    fetch_new("start")
    final = groups * per_group - 1
    fetch_new("wait")
    step(recent(0), main(final, 0), main(final - 1, groups - 1))
    step(recent(1), recent(0), main(final, groups - 1))

    def new_tile(t, _):
        step(recent(t), recent(t - 1), recent(t - 2))
        return 0

    lax.fori_loop(2, groups * per_group, new_tile, 0)
    step(None, recent(final), recent(final - 1))
    step(None, None, recent(final))

    heads_per_tile = NC // PHASE_TOKENS
    tiles = per_group // phases

    def finish(t, _):
        total = jnp.sum(l_ref[t], axis=0, keepdims=True)
        out = (acc_ref[t] / total).T.astype(BF16)
        g, p, h = t // per_group, lax.rem(t, per_group) // tiles, lax.rem(t, tiles)
        for i in range(heads_per_tile):
            at = pl.multiple_of((g * heads + h * heads_per_tile + i) * LANES, LANES)
            rows = pl.ds(pl.multiple_of(p * PHASE_TOKENS, PHASE_TOKENS), PHASE_TOKENS)
            o_ref[rows, pl.ds(at, LANES)] = out[i * PHASE_TOKENS:(i + 1) * PHASE_TOKENS, :]
        return 0

    lax.fori_loop(0, groups * per_group, finish, 0)

    for c in range(CHUNKS):
        own_right(c).wait_send()
        own_left(c).wait_send()
        own_pair(c).wait_send()
    for s in range(2, sets):
        for side in range(2):
            to_pair(s, side).wait_send()
    for s in (2, 3):
        hop_right(s).wait_send()
    for s in (4, 5):
        hop_left(s).wait_send()
    for copy in (new_right, new_left, new_pair, new_hop, new_left_pair, new_right_pair, new_far_pair):
        copy.wait_send()


def attend(qt, kv, kvn, n, heads):
    groups, phases, tiles = qt.shape[:3]
    part, tok = kv.shape[3], kvn.shape[2]
    span, span_new = CHUNKS * part, n * tok
    count = groups * phases * tiles
    rows = max(span, groups * span_new)
    any_spec = pl.BlockSpec(memory_space=pl.ANY)
    vmem_spec = pl.BlockSpec(memory_space=pltpu.VMEM)
    dma = pltpu.SemaphoreType.DMA
    flops = 4 * count * NC * LANES * n * (span + tok)
    out = pl.pallas_call(
        functools.partial(attention_kernel, n, heads, phases),
        in_specs=[vmem_spec, any_spec, any_spec],
        out_specs=[vmem_spec, any_spec, any_spec],
        out_shape=[
            jax.ShapeDtypeStruct((tok, groups * heads * LANES), BF16),
            jax.ShapeDtypeStruct((n,) + kv.shape, BF16),
            jax.ShapeDtypeStruct((n,) + kvn.shape, BF16),
        ],
        scratch_shapes=[
            pltpu.VMEM((groups, rows, LANES), BF16),
            pltpu.VMEM((groups, rows, LANES), BF16),
            pltpu.VMEM((max(span, span_new), NC), F32),
            pltpu.VMEM((max(span, span_new), NC), BF16),
            pltpu.VMEM((count + 1, LANES, NC), F32),
            pltpu.VMEM((count, 1, NC), F32),
            pltpu.VMEM((count + 1, 8, NC), F32),
            pltpu.VMEM((8, NC), F32),
            pltpu.VMEM((2, 1, NC), F32),
            pltpu.VMEM((2 + phases, tok, NC), F32),
            dma((groups, 2, CHUNKS)),
            dma((2, groups, n)),
            dma((3, CHUNKS)),
            dma((n, 2)),
            dma((n,)),
            dma((7,)),
            dma((n, CHUNKS)),
            dma((7,)),
        ],
        cost_estimate=pl.CostEstimate(flops=flops, bytes_accessed=4 * kv.size * n, transcendentals=flops // (4 * LANES)),
        compiler_params=pltpu.CompilerParams(collective_id=0, has_side_effects=True, vmem_limit_bytes=60 << 20),
        name="attend",
    )(qt.reshape((count,) + qt.shape[3:]), kv, kvn)
    return out[0]


OUT_COLS = 512


def output_kernel(n, o_ref, x_ref, w_ref, y_ref, w_buf, x_buf, full_buf, send_buf, got_buf, y_buf, w_sem, x_sem, part_send, part_recv, y_send, y_recv, y_sem):
    me = lax.axis_index("tp")
    tok, width = x_ref.shape
    rows = tok // n
    pieces = width // OUT_COLS
    slots = w_buf.shape[0]
    my_rows = pl.ds(pl.multiple_of(me * rows, rows), rows)

    def cols(k):
        return slice(k * OUT_COLS, (k + 1) * OUT_COLS)

    def weight(k):
        return pltpu.make_async_copy(w_ref.at[:, cols(k)], w_buf.at[k % slots], w_sem.at[k % slots])

    def partial(k, d):
        to = lax.rem(me + d, n)
        src = send_buf.at[k, pl.ds(pl.multiple_of(to * rows, rows), rows)]
        return pltpu.make_async_remote_copy(src_ref=src, dst_ref=got_buf.at[k, d - 1], send_sem=part_send.at[k, d - 1], recv_sem=part_recv.at[k, d - 1], device_id={"tp": to}, device_id_type=MESH)

    def result(k, d):
        to = lax.rem(me + d, n)
        return pltpu.make_async_remote_copy(src_ref=y_buf.at[k], dst_ref=y_ref.at[my_rows, cols(k)], send_sem=y_send.at[k, d - 1], recv_sem=y_recv.at[k, d - 1], device_id={"tp": to}, device_id_type=MESH)

    def local(k):
        return pltpu.make_async_copy(y_buf.at[k], y_ref.at[my_rows, cols(k)], y_sem.at[k])

    own_x = pltpu.make_async_copy(x_ref.at[my_rows], x_buf, x_sem)
    own_x.start()
    for k in range(slots):
        weight(k).start()
    barrier = pltpu.get_barrier_semaphore()
    for d in range(1, n):
        pl.semaphore_signal(barrier, inc=1, device_id={"tp": lax.rem(me + d, n)}, device_id_type=MESH)
    pl.semaphore_wait(barrier, n - 1)
    own_x.wait()
    for k in range(pieces + 4):
        if k < pieces:
            weight(k).wait()
            part = dot(o_ref[...], w_buf[k % slots])
            full_buf[k % 4] = part
            send_buf[k] = part.astype(BF16)
            if k + slots < pieces:
                weight(k + slots).start()
        if 1 <= k <= pieces:
            for d in range(1, n):
                partial(k - 1, d).start()
        if 3 <= k < pieces + 3:
            j = k - 3
            total = full_buf[j % 4, my_rows, :]
            for d in range(1, n):
                partial(j, d).wait_recv()
                total = total + got_buf[j, d - 1].astype(F32)
            y_buf[j] = (x_buf[:, cols(j)].astype(F32) + total).astype(BF16)
        if k >= 4:
            local(k - 4).start()
            for d in range(1, n):
                result(k - 4, d).start()
    for k in range(pieces):
        local(k).wait()
        for d in range(1, n):
            partial(k, d).wait_send()
            result(k, d).wait_send()
            result(k, d).wait_recv()


def project_out(o, x, w_out, n):
    tok, width = x.shape
    pieces = width // OUT_COLS
    rows = tok // n
    any_spec = pl.BlockSpec(memory_space=pl.ANY)
    vmem_spec = pl.BlockSpec(memory_space=pltpu.VMEM)
    dma = pltpu.SemaphoreType.DMA
    slots = 3
    return pl.pallas_call(
        functools.partial(output_kernel, n),
        in_specs=[vmem_spec, any_spec, any_spec],
        out_specs=any_spec,
        out_shape=jax.ShapeDtypeStruct((tok, width), BF16),
        scratch_shapes=[
            pltpu.VMEM((slots, o.shape[1], OUT_COLS), BF16),
            pltpu.VMEM((rows, width), BF16),
            pltpu.VMEM((4, tok, OUT_COLS), F32),
            pltpu.VMEM((pieces, tok, OUT_COLS), BF16),
            pltpu.VMEM((pieces, n - 1, rows, OUT_COLS), BF16),
            pltpu.VMEM((pieces, rows, OUT_COLS), BF16),
            dma((slots,)),
            dma,
            dma((pieces, n - 1)),
            dma((pieces, n - 1)),
            dma((pieces, n - 1)),
            dma((pieces, n - 1)),
            dma((pieces,)),
        ],
        cost_estimate=pl.CostEstimate(flops=2 * tok * o.shape[1] * width, bytes_accessed=2 * w_out.size, transcendentals=0),
        compiler_params=pltpu.CompilerParams(collective_id=1, has_side_effects=True, vmem_limit_bytes=40 << 20),
        name="project_out",
    )(o, x, w_out)


def local_step(cp, tp, x, k_cache, v_cache, rope_table, norm_gain, w_qkv, b_qkv, w_out):
    groups = k_cache.shape[1]
    heads = w_qkv.shape[1] // groups // LANES - 2
    kv = relayout_cache(k_cache, v_cache)
    qt, kvn, new_k, new_v = project_new(x, rope_table, norm_gain, w_qkv, b_qkv, groups)
    o = attend(qt, kv, kvn, cp, heads)
    y = project_out(o, x, w_out, tp)
    new_shape = (x.shape[0],) + k_cache.shape[1:]
    return y, new_k.reshape(new_shape), new_v.reshape(new_shape)


def solution(mesh):
    row_spec = P(("dp", "cp"), None)
    cache_spec = P(("dp", "cp"), "tp", None)
    body = functools.partial(local_step, mesh.shape["cp"], mesh.shape["tp"])
    return jax.shard_map(body, mesh=mesh, in_specs=(row_spec, cache_spec, cache_spec, row_spec, P(None), P(None, "tp"), P("tp"), P("tp", None)), out_specs=(row_spec, cache_spec, cache_spec), check_vma=False)
```

```python
import functools
import math

import jax
import jax.numpy as jnp
from jax import lax
from jax.experimental import pallas as pl
from jax.experimental.pallas import tpu as pltpu
from jax.sharding import PartitionSpec as P

EPS = 1.5625e-07
MASK_VALUE = -1e30
LANES = 128
SUB = 256
NC = 512
PHASE_TOKENS = 128
CHUNKS = 4
COLS = 512
OUT_SLOTS = 6
MESH = pl.DeviceIdType.MESH
F32 = jnp.float32
BF16 = jnp.bfloat16
DMA = pltpu.SemaphoreType.DMA


def dot(a, b, dims=(((1,), (0,)), ((), ()))):
    return lax.dot_general(a, b, dims, preferred_element_type=F32)


def block_kernel(dims, x_ref, kc_ref, vc_ref, table_ref, g_ref, wq_ref, b_ref, wo_ref,
                 y_ref, kn_ref, vn_ref, ring_ref, ringn_ref,
                 k_buf, v_buf, stage, kvn, qt_ref, hid_ref, x_buf, w_buf, a_buf, cos_ref, sin_ref, kn_buf, vn_buf,
                 s_ref, p_ref, acc_ref, m_ref, l_ref, mc_ref, al_ref, bias_ref,
                 o_buf, res_buf, full_buf, mine_buf, send_buf, got_buf, y_buf,
                 in_sem, w_sem, out_sem, fetch_sem, newest_sem, own_send, pair_send, hop_send, new_send, recv, new_recv,
                 part_send, part_recv, y_send, y_recv, y_sem):
    n, ranks, groups, heads = dims
    me = lax.axis_index("cp")
    rank = lax.axis_index("tp")
    pair = me + 1 - 2 * lax.rem(me, 2)
    right, left, far = lax.rem(me + 2, n), lax.rem(me + n - 2, n), lax.rem(me + 4, n)
    tok, width = x_ref.shape
    part = stage.shape[3]
    span, span_new = CHUNKS * part, n * tok
    phases = tok // PHASE_TOKENS
    heads_per_tile = NC // PHASE_TOKENS
    tiles = heads // heads_per_tile
    per_group = phases * tiles
    count = groups * per_group
    spare = count
    half = kc_ref.shape[0] // 2
    scale = LANES ** -0.5 * math.log2(math.e)
    head_count = groups * (heads + 2)
    w_blocks = head_count * LANES // COLS
    heads_per_block = COLS // LANES
    pieces = width // COLS
    out_depth = wo_ref.shape[0]
    rows = PHASE_TOKENS // ranks

    def remote(src, dst, send, got, axis, where):
        return pltpu.make_async_remote_copy(src_ref=src, dst_ref=dst, send_sem=send, recv_sem=got, device_id={axis: where}, device_id_type=MESH)

    def own_pair(c):
        return remote(stage.at[c], ring_ref.at[1, c], own_send.at[0, c], recv.at[1, c], "cp", pair)

    def own_right(c):
        return remote(stage.at[c], ring_ref.at[2 + c, 0], own_send.at[1, c], recv.at[2 + c, 0], "cp", right)

    def own_left(c):
        return remote(stage.at[c], ring_ref.at[2 + c, 1], own_send.at[2, c], recv.at[2 + c, 1], "cp", left)

    def to_pair(s, side):
        return remote(ring_ref.at[s, side], ring_ref.at[s, 2 + side], pair_send.at[s, side], recv.at[s, 2 + side], "cp", pair)

    def from_side(s, side):
        return remote(stage.at[0], ring_ref.at[s, side], own_send.at[0, 0], recv.at[s, side], "cp", pair)

    def hop_right(s):
        return remote(ring_ref.at[s, 0], ring_ref.at[s + 4, 0], hop_send.at[s], recv.at[s + 4, 0], "cp", right)

    def hop_left(s):
        return remote(ring_ref.at[s, 1], ring_ref.at[s + 2, 1], hop_send.at[s], recv.at[s + 2, 1], "cp", left)

    def new_copy(source, send, got, where, own=False):
        src = kvn if own else ringn_ref.at[source]
        return remote(src, ringn_ref.at[source], new_send.at[send], new_recv.at[got], "cp", where)

    new_right = new_copy(me, 0, 0, right, own=True)
    new_left = new_copy(me, 1, 1, left, own=True)
    new_pair = new_copy(me, 2, 3, pair, own=True)
    new_hop = new_copy(left, 3, 2, right)
    new_left_pair = new_copy(left, 4, 4, pair)
    new_right_pair = new_copy(right, 5, 5, pair)
    new_far_pair = new_copy(far, 6, 6, pair)

    def pass_on(s):
        for side in range(2):
            from_side(s, side).wait_recv()
            to_pair(s, side).start()

    def cache_in(i):
        here = pl.ds(i * half, half)
        return (pltpu.make_async_copy(kc_ref.at[here], k_buf.at[i, pl.ds(0, half)], in_sem.at[0, i]),
                pltpu.make_async_copy(vc_ref.at[here], v_buf.at[i, pl.ds(0, half)], in_sem.at[1, i]))

    x_in = pltpu.make_async_copy(x_ref, x_buf, in_sem.at[2, 0])

    def res_in(p):
        here = pl.ds(pl.multiple_of(p * PHASE_TOKENS + rank * rows, rows), rows)
        return pltpu.make_async_copy(x_ref.at[here], res_buf.at[p], in_sem.at[2 + p, 1])

    def w_in(j, slot):
        cols = pl.ds(pl.multiple_of(j * COLS, COLS), COLS)
        here = pl.ds(pl.multiple_of(slot * width, width), width)
        return pltpu.make_async_copy(wq_ref.at[:, cols], w_buf.at[here], w_sem.at[slot])

    def wo_at(slot):
        return pl.ds(pl.multiple_of(slot * out_depth, out_depth), out_depth)

    def wo_in(k):
        slot = lax.rem(k, OUT_SLOTS)
        cols = pl.ds(pl.multiple_of(k * COLS, COLS), COLS)
        return pltpu.make_async_copy(wo_ref.at[:, cols], w_buf.at[wo_at(slot)], w_sem.at[slot])

    for i in range(2):
        for copy in cache_in(i):
            copy.start()
    x_in.start()
    w_in(0, 0).start()
    w_in(1, 1).start()
    for p in range(phases):
        res_in(p).start()

    barrier = pltpu.get_barrier_semaphore()
    for other in (pair, right, left):
        pl.semaphore_signal(barrier, inc=1, device_id={"cp": other}, device_id_type=MESH)
    for d in range(1, ranks):
        pl.semaphore_signal(barrier, inc=1, device_id={"tp": lax.rem(rank + d, ranks)}, device_id_type=MESH)

    pair_rows = groups * LANES
    wide = lax.broadcasted_iota(jnp.int32, (pair_rows, pair_rows), 0)
    tall = lax.broadcasted_iota(jnp.int32, (pair_rows, pair_rows), 1)
    pick = (wide // groups + (wide % groups) * LANES == tall).astype(BF16)
    pick_t = (tall // groups + (tall % groups) * LANES == wide).astype(BF16)
    blocks = part // LANES

    def stage_out(c):
        return pltpu.make_async_copy(stage.at[c], ring_ref.at[0, c], out_sem.at[c])

    for c in range(CHUNKS):
        if c % (CHUNKS // 2) == 0:
            for copy in cache_in(c // (CHUNKS // 2)):
                copy.wait()

        def relayout(i, _):
            i_half = c // (CHUNKS // 2)
            src = pl.ds(pl.multiple_of((c % (CHUNKS // 2)) * part * groups + i * pair_rows, pair_rows), pair_rows)
            here = pl.ds(pl.multiple_of(i * LANES, LANES), LANES)
            keys = dot(pick_t, k_buf[i_half, src, :]).astype(BF16)
            vals = dot(v_buf[i_half, src, :], pick, (((0,), (0,)), ((), ()))).astype(BF16)
            for g in range(groups):
                stage[c, g, 0, here, :] = keys[g * LANES:(g + 1) * LANES, :]
                stage[c, g, 1, here, :] = vals[:, g * LANES:(g + 1) * LANES]
            return 0

        lax.fori_loop(0, blocks, relayout, 0, unroll=4)
        stage_out(c).start()
        if c == 0:
            pl.semaphore_wait(barrier, 3 + ranks - 1)
        own_right(c).start()
        own_left(c).start()
        own_pair(c).start()

    x_in.wait()
    gain = g_ref[...].astype(F32)

    def norm(i, _):
        here = pl.ds(pl.multiple_of(i * 32, 32), 32)
        x = x_buf[here, :].astype(F32)
        inv_rms = lax.rsqrt(jnp.mean(x * x, axis=-1, keepdims=True) + EPS)
        hid_ref[here, :] = (x * inv_rms * gain).astype(BF16)
        return 0

    lax.fori_loop(0, tok // 32, norm, 0)
    lane = lax.broadcasted_iota(jnp.int32, (tok, LANES), 1)
    rope_lanes = table_ref.shape[0]
    table = jnp.concatenate([table_ref[...].T, jnp.zeros((tok, LANES - rope_lanes), F32)], axis=1)
    at = jnp.where(lane < rope_lanes, lane // 2, 0)
    sin = jnp.take_along_axis(table, at + rope_lanes // 2, axis=1)
    cos_ref[...] = jnp.take_along_axis(table, at, axis=1)
    sin_ref[...] = jnp.where(lane % 2 == 0, -sin, sin)

    def rotate(head):
        swapped = jnp.where(lane % 2 == 0, pltpu.roll(head, LANES - 1, 1), pltpu.roll(head, 1, 1))
        turned = head * cos_ref[...] + swapped * sin_ref[...]
        return jnp.where(lane < rope_lanes, turned, head)

    def queries(j, i):
        head = j * heads_per_block + i
        g, h = head // (heads + 2), lax.rem(head, heads + 2)
        turned = rotate(a_buf[j, :, i * LANES:(i + 1) * LANES]).T.astype(BF16)
        for p in range(phases):
            tile = jnp.where(h < heads, g * per_group + p * tiles + h // heads_per_tile, spare)
            at = pl.multiple_of(lax.rem(h, heads_per_tile) * PHASE_TOKENS, PHASE_TOKENS)
            qt_ref[tile, :, pl.ds(at, PHASE_TOKENS)] = turned[:, p * PHASE_TOKENS:(p + 1) * PHASE_TOKENS]

    def project(j, _):
        slot = lax.rem(j, 2)
        w_in(j, slot).wait()
        here = pl.ds(pl.multiple_of(slot * width, width), width)
        cols = pl.ds(pl.multiple_of(j * COLS, COLS), COLS)
        before = jnp.maximum(j - 1, 0)
        for i in range(heads_per_block):
            queries(before, i)
        a_buf[j] = dot(hid_ref[...], w_buf[here, :]) + b_ref[:, cols].astype(F32)

        @pl.when(j + 2 < w_blocks)
        def _():
            w_in(j + 2, slot).start()
        return 0

    a_buf[0] = jnp.zeros(a_buf.shape[1:], F32)
    lax.fori_loop(0, w_blocks, project, 0)
    for i in range(heads_per_block):
        queries(w_blocks - 1, i)

    kn_out = pltpu.make_async_copy(kn_buf, kn_ref, out_sem.at[CHUNKS])
    vn_out = pltpu.make_async_copy(vn_buf, vn_ref, out_sem.at[CHUNKS + 1])
    kvn_out = pltpu.make_async_copy(kvn, ringn_ref.at[me], out_sem.at[CHUNKS + 2])
    for g in range(groups):
        at = (g * (heads + 2) + heads) * LANES
        keys = rotate(a_buf[at // COLS, :, at % COLS:at % COLS + LANES]).astype(BF16)
        at += LANES
        vals = a_buf[at // COLS, :, at % COLS:at % COLS + LANES]
        kn_buf[:, g * LANES:(g + 1) * LANES] = keys
        vn_buf[:, g * LANES:(g + 1) * LANES] = vals.astype(BF16)
        kvn[g, 0] = keys
        for i in range(tok // LANES):
            here = slice(i * LANES, (i + 1) * LANES)
            kvn[g, 1, here, :] = vals[here, :].T.astype(BF16)
    for c in range(CHUNKS):
        stage_out(c).wait()

    def fetch(s, g, act):
        for c in range(CHUNKS):
            here = pl.ds(c * part, part)
            for kind, buf in ((0, k_buf), (1, v_buf)):
                getattr(pltpu.make_async_copy(ring_ref.at[s, c, g, kind], buf.at[g, here], fetch_sem.at[g, kind, c]), act)()

    def fetch_new(act):
        for g in range(groups):
            for j in range(n):
                here = pl.ds(g * span_new + j * tok, tok)
                for kind, buf in ((0, k_buf), (1, v_buf)):
                    getattr(pltpu.make_async_copy(ringn_ref.at[j, g, kind], buf.at[0, here], newest_sem.at[kind, g, j]), act)()

    fetch(0, 0, "start")
    kn_out.start()
    vn_out.start()
    kvn_out.start()

    row = lax.broadcasted_iota(jnp.int32, (tok, NC), 0)
    col = lax.rem(lax.broadcasted_iota(jnp.int32, (tok, NC), 1), PHASE_TOKENS)
    bias_ref[0] = jnp.zeros((tok, NC), F32)
    for p in range(phases):
        bias_ref[1 + p] = jnp.where(row <= col + p * PHASE_TOKENS, 0.0, MASK_VALUE)
    bias_ref[1 + phases] = jnp.full((tok, NC), MASK_VALUE, F32)

    m_ref[...] = jnp.full(m_ref.shape, MASK_VALUE, F32)
    l_ref[...] = jnp.zeros(l_ref.shape, F32)
    acc_ref[...] = jnp.zeros(acc_ref.shape, F32)
    s_ref[...] = jnp.zeros(s_ref.shape, F32)
    p_ref[...] = jnp.zeros(p_ref.shape, BF16)
    mc_ref[...] = jnp.zeros(mc_ref.shape, F32)
    al_ref[...] = jnp.ones(al_ref.shape, F32)
    kvn_out.wait()
    for copy in (new_right, new_left, new_pair):
        copy.start()

    def step(a=None, b=None, c=None):
        alpha_b, alpha_c = al_ref[0], al_ref[1]
        shift = mc_ref[...]
        run = {"max": None, "sum": None, "out": None}

        def scores(i):
            keys = k_buf[a["slot"], pl.ds(a["base"] + i * SUB, SUB), :]
            s = dot(keys, qt_ref[a["tile"]])
            if a["new"]:
                edge = 1 + lax.rem(a["tile"], per_group) // tiles
                which = jnp.where(i < me, 0, jnp.where(i == me, edge, 1 + phases))
                s = s + bias_ref[which]
            s_ref[i * SUB:(i + 1) * SUB, :] = s
            top = jnp.max(s.reshape(SUB // 8, 8, NC), axis=0)
            run["max"] = top if run["max"] is None else jnp.maximum(run["max"], top)

        def weights(i):
            s = s_ref[i * SUB:(i + 1) * SUB, :]
            e = jnp.exp2((s * scale).reshape(SUB // 8, 8, NC) - shift[None])
            part_sum = jnp.sum(e, axis=0)
            run["sum"] = part_sum if run["sum"] is None else run["sum"] + part_sum
            p_ref[i * SUB:(i + 1) * SUB, :] = e.reshape(SUB, NC).astype(BF16)

        def values(i):
            at = c["base"] + i * SUB
            block = jnp.concatenate([v_buf[c["slot"], pl.ds(at + h * LANES, LANES), :] for h in range(SUB // LANES)], axis=1)
            out = dot(block, p_ref[i * SUB:(i + 1) * SUB, :])
            run["out"] = out if run["out"] is None else run["out"] + out

        stages = ((c, values), (b, weights), (a, scores))
        for i in range(max(spec["keys"] for spec, _ in stages if spec is not None) // SUB):
            for spec, stage_fn in stages:
                if spec is not None and i < spec["keys"] // SUB:
                    stage_fn(i)
        if c is not None:
            acc_ref[c["tile"]] = acc_ref[c["tile"]] * alpha_c + run["out"]
        if b is not None:
            l_ref[b["tile"]] = l_ref[b["tile"]] * alpha_b + run["sum"]
            al_ref[1] = alpha_b
        if a is not None:
            old = m_ref[a["tile"]]
            new = jnp.maximum(old, jnp.max(run["max"], axis=0, keepdims=True))
            m_ref[a["tile"]] = new
            mc_ref[...] = jnp.broadcast_to(new * scale, mc_ref.shape)
            al_ref[0] = jnp.exp2((old - new) * scale)

    def main(tile, slot):
        return {"tile": tile, "slot": slot, "base": 0, "keys": span, "new": False}

    def run_unit(g, first, tile_count, carry, fetch_next):
        fetch(0, g, "wait")

        def one_tile(t, carry):
            pl.when(t == tile_count - 1)(fetch_next)
            last, last_slot, older, older_slot = carry
            tile = g * per_group + first + t
            step(main(tile, g), main(last, last_slot), main(older, older_slot))
            return tile, jnp.int32(g), last, last_slot

        return lax.fori_loop(0, tile_count, one_tile, carry)

    start = tuple(jnp.int32(v) for v in (spare, 0, spare, 0))

    def one_set(s, carry):
        nxt = s + 1
        carry = run_unit(0, 0, per_group, carry, lambda: fetch(s, 1, "start"))
        pl.when(s >= 1)(lambda: pass_on(nxt))
        pl.when((s >= 1) & (s <= 2))(lambda: hop_right(nxt).start())
        pl.when((s >= 3) & (s <= 4))(lambda: hop_left(nxt).start())

        def fetch_next():
            @pl.when(s == 0)
            def _():
                for c in range(CHUNKS):
                    own_pair(c).wait_recv()

            @pl.when(s >= 1)
            def _():
                for side in range(2):
                    to_pair(nxt, side).wait_recv()
            fetch(nxt, 0, "start")

        return run_unit(1, 0, per_group, carry, fetch_next)

    carry = lax.fori_loop(0, n - 2, one_set, start)
    kn_out.wait()
    vn_out.wait()

    def part_copy(p, k, d):
        to = lax.rem(rank + d, ranks)
        src = send_buf.at[k, pl.ds(pl.multiple_of(to * rows, rows), rows)]
        return remote(src, got_buf.at[p, k, d - 1], part_send.at[p, k, d - 1], part_recv.at[p, k, d - 1], "tp", to)

    def y_rows(p):
        return pl.ds(pl.multiple_of(p * PHASE_TOKENS + rank * rows, rows), rows)

    def y_copy(p, k, d):
        cols = pl.ds(pl.multiple_of(k * COLS, COLS), COLS)
        to = lax.rem(rank + d, ranks)
        return remote(y_buf.at[p, k], y_ref.at[y_rows(p), cols], y_send.at[p, k, d - 1], y_recv.at[p, k, d - 1], "tp", to)

    def y_own(p, k):
        cols = pl.ds(pl.multiple_of(k * COLS, COLS), COLS)
        return pltpu.make_async_copy(y_buf.at[p, k], y_ref.at[y_rows(p), cols], y_sem.at[p, k])

    def project_out(p):
        def piece(k, _):
            @pl.when(k < pieces)
            def _():
                wo_in(k).wait()
                out = dot(o_buf[...], w_buf[wo_at(lax.rem(k, OUT_SLOTS)), :])
                full_buf[...] = out
                send_buf[k] = out.astype(BF16)
                mine_buf[k] = full_buf[pl.ds(pl.multiple_of(rank * rows, rows), rows), :]
                pl.when(k + OUT_SLOTS < pieces)(lambda: wo_in(k + OUT_SLOTS).start())

            @pl.when(k >= 1)
            def _():
                for d in range(1, ranks):
                    part_copy(p, k - 1, d).start()
            return 0

        lax.fori_loop(0, pieces + 1, piece, 0)

    def reduce_out(p, lo, hi):
        def piece(k, _):
            @pl.when(k < hi)
            def _():
                for d in range(1, ranks):
                    part_copy(p, k, d).wait_recv()
                total = mine_buf[k]
                for d in range(1, ranks):
                    total = total + got_buf[p, k, d - 1].astype(F32)
                cols = pl.ds(pl.multiple_of(k * COLS, COLS), COLS)
                y_buf[p, k] = (res_buf[p, :, cols].astype(F32) + total).astype(BF16)

            @pl.when(k > lo)
            def _():
                y_own(p, k - 1).start()
                for d in range(1, ranks):
                    y_copy(p, k - 1, d).start()
            return 0

        lax.fori_loop(lo, hi + 1, piece, 0)

    def finish(p, g):
        def tile(h, _):
            t = g * per_group + p * tiles + h
            total = jnp.sum(l_ref[t], axis=0, keepdims=True)
            out = (acc_ref[t] / total).T.astype(BF16)
            for i in range(heads_per_tile):
                at = pl.multiple_of((g * heads + h * heads_per_tile + i) * LANES, LANES)
                o_buf[:, pl.ds(at, LANES)] = out[i * PHASE_TOKENS:(i + 1) * PHASE_TOKENS, :]
            return 0

        lax.fori_loop(0, tiles, tile, 0)

    for p in range(phases):
        res_in(p).wait()

    def one_phase(p, carry):
        first = p * tiles

        def late_set(s, carry):
            carry = run_unit(0, first, tiles, carry, lambda: fetch(s, 1, "start"))

            @pl.when((p == 0) & (s == n - 2))
            def _():
                pass_on(n - 1)
                new_copy(left, 0, 0, right).wait_recv()
                new_hop.start()
                new_left_pair.start()
                new_copy(right, 0, 1, left).wait_recv()
                new_right_pair.start()

            @pl.when((p == 0) & (s == n - 1))
            def _():
                new_copy(far, 0, 2, right).wait_recv()
                new_far_pair.start()

            @pl.when((p > 0) & (s == n - 1))
            def _():
                reduce_out(p - 1, 0, pieces // 2)

            def fetch_next():
                @pl.when(s == n - 2)
                def _():
                    @pl.when(p == 0)
                    def _():
                        for side in range(2):
                            to_pair(n - 1, side).wait_recv()
                    fetch(n - 1, 0, "start")

            return run_unit(1, first, tiles, carry, fetch_next)

        carry = lax.fori_loop(n - 2, n, late_set, carry)
        last, last_slot, older, older_slot = carry

        @pl.when(p == 0)
        def _():
            for got in (3, 4, 5, 6):
                new_copy(pair, 0, got, pair).wait_recv()

        @pl.when(p > 0)
        def _():
            reduce_out(p - 1, pieces // 2, pieces)
        fetch_new("start")
        for k in range(OUT_SLOTS):
            wo_in(k).start()
        fetch_new("wait")

        def recent(i):
            g = i // tiles
            return {"tile": g * per_group + first + lax.rem(i, tiles), "slot": 0, "base": pl.multiple_of(g * span_new, span_new), "keys": span_new, "new": True}

        step(recent(0), main(last, last_slot), main(older, older_slot))
        step(recent(1), recent(0), main(last, last_slot))

        def new_tile(i, _):
            step(recent(i), recent(i - 1), recent(i - 2))
            return 0

        end = groups * tiles
        lax.fori_loop(2, end, new_tile, 0)
        step(None, recent(end - 1), recent(end - 2))
        step(None, None, recent(end - 1))

        @pl.when(p < phases - 1)
        def _():
            fetch(n - 2, 0, "start")
        for g in range(groups):
            finish(p, g)

        @pl.when(p > 0)
        def _():
            def sent(k, _):
                for d in range(1, ranks):
                    part_copy(p - 1, k, d).wait_send()
                return 0
            lax.fori_loop(0, pieces, sent, 0)
        project_out(p)
        return start

    lax.fori_loop(0, phases, one_phase, carry)
    reduce_out(phases - 1, 0, pieces)

    for c in range(CHUNKS):
        own_right(c).wait_send()
        own_left(c).wait_send()
        own_pair(c).wait_send()
    for s in range(2, n):
        for side in range(2):
            to_pair(s, side).wait_send()
    for s in (2, 3):
        hop_right(s).wait_send()
    for s in (4, 5):
        hop_left(s).wait_send()
    for copy in (new_right, new_left, new_pair, new_hop, new_left_pair, new_right_pair, new_far_pair):
        copy.wait_send()

    def drain(k, _):
        for d in range(1, ranks):
            part_copy(phases - 1, k, d).wait_send()
        for p in range(phases):
            y_own(p, k).wait()
            for d in range(1, ranks):
                y_copy(p, k, d).wait_send()
                y_copy(p, k, d).wait_recv()
        return 0

    lax.fori_loop(0, pieces, drain, 0)


def local_step(n, ranks, x, k_cache, v_cache, rope_table, norm_gain, w_qkv, b_qkv, w_out):
    positions, groups, head_dim = k_cache.shape
    tok, width = x.shape
    heads = w_qkv.shape[1] // groups // head_dim - 2
    part = positions // CHUNKS
    span, span_new = positions, n * tok
    phases = tok // PHASE_TOKENS
    tiles = heads * PHASE_TOKENS // NC
    count = groups * phases * tiles
    rows_max = max(span, groups * span_new)
    pieces = width // COLS
    w_blocks = w_qkv.shape[1] // COLS
    rows = PHASE_TOKENS // ranks
    depth = w_out.shape[0]
    any_spec = pl.BlockSpec(memory_space=pl.ANY)
    vmem_spec = pl.BlockSpec(memory_space=pltpu.VMEM)
    flat = (positions * groups, head_dim)
    flops = 4 * count * NC * LANES * n * (span + tok)
    y, new_k, new_v, _, _ = pl.pallas_call(
        functools.partial(block_kernel, (n, ranks, groups, heads)),
        in_specs=[any_spec, any_spec, any_spec, vmem_spec, vmem_spec, any_spec, vmem_spec, any_spec],
        out_specs=[any_spec] * 5,
        out_shape=[
            jax.ShapeDtypeStruct((tok, width), BF16),
            jax.ShapeDtypeStruct((tok, groups * head_dim), BF16),
            jax.ShapeDtypeStruct((tok, groups * head_dim), BF16),
            jax.ShapeDtypeStruct((n, CHUNKS, groups, 2, part, head_dim), BF16),
            jax.ShapeDtypeStruct((n, groups, 2, tok, head_dim), BF16),
        ],
        scratch_shapes=[
            pltpu.VMEM((2, rows_max, LANES), BF16),
            pltpu.VMEM((2, rows_max, LANES), BF16),
            pltpu.VMEM((CHUNKS, groups, 2, part, LANES), BF16),
            pltpu.VMEM((groups, 2, tok, LANES), BF16),
            pltpu.VMEM((count + 1, LANES, NC), BF16),
            pltpu.VMEM((tok, width), BF16),
            pltpu.VMEM((tok, width), BF16),
            pltpu.VMEM((max(2 * width, OUT_SLOTS * depth), COLS), BF16),
            pltpu.VMEM((w_blocks, tok, COLS), F32),
            pltpu.VMEM((tok, LANES), F32),
            pltpu.VMEM((tok, LANES), F32),
            pltpu.VMEM((tok, groups * LANES), BF16),
            pltpu.VMEM((tok, groups * LANES), BF16),
            pltpu.VMEM((max(span, span_new), NC), F32),
            pltpu.VMEM((max(span, span_new), NC), BF16),
            pltpu.VMEM((count + 1, LANES, NC), F32),
            pltpu.VMEM((count, 1, NC), F32),
            pltpu.VMEM((count + 1, 8, NC), F32),
            pltpu.VMEM((8, NC), F32),
            pltpu.VMEM((2, 1, NC), F32),
            pltpu.VMEM((2 + phases, tok, NC), F32),
            pltpu.VMEM((PHASE_TOKENS, groups * heads * LANES), BF16),
            pltpu.VMEM((phases, rows, width), BF16),
            pltpu.VMEM((PHASE_TOKENS, COLS), F32),
            pltpu.VMEM((pieces, rows, COLS), F32),
            pltpu.VMEM((pieces, PHASE_TOKENS, COLS), BF16),
            pltpu.VMEM((phases, pieces, ranks - 1, rows, COLS), BF16),
            pltpu.VMEM((phases, pieces, rows, COLS), BF16),
            DMA((2 + phases, 2)),
            DMA((max(2, OUT_SLOTS),)),
            DMA((CHUNKS + 3,)),
            DMA((groups, 2, CHUNKS)),
            DMA((2, groups, n)),
            DMA((3, CHUNKS)),
            DMA((n, 2)),
            DMA((n,)),
            DMA((7,)),
            DMA((n, CHUNKS)),
            DMA((7,)),
            DMA((phases, pieces, ranks - 1)),
            DMA((phases, pieces, ranks - 1)),
            DMA((phases, pieces, ranks - 1)),
            DMA((phases, pieces, ranks - 1)),
            DMA((phases, pieces)),
        ],
        cost_estimate=pl.CostEstimate(flops=flops, bytes_accessed=4 * positions * n * groups * head_dim, transcendentals=flops // (4 * LANES)),
        compiler_params=pltpu.CompilerParams(collective_id=0, has_side_effects=True, vmem_limit_bytes=63 << 20),
        name="block",
    )(x, k_cache.reshape(flat), v_cache.reshape(flat), rope_table.T, norm_gain.reshape(1, width), w_qkv, b_qkv.reshape(1, -1), w_out)
    new_shape = (tok,) + k_cache.shape[1:]
    return y, new_k.reshape(new_shape), new_v.reshape(new_shape)


def solution(mesh):
    row_spec = P(("dp", "cp"), None)
    cache_spec = P(("dp", "cp"), "tp", None)
    body = functools.partial(local_step, mesh.shape["cp"], mesh.shape["tp"])
    return jax.shard_map(body, mesh=mesh, in_specs=(row_spec, cache_spec, cache_spec, row_spec, P(None), P(None, "tp"), P("tp"), P("tp", None)), out_specs=(row_spec, cache_spec, cache_spec), check_vma=False)
```

```python
import functools
import math

import jax
import jax.numpy as jnp
from jax import lax
from jax.experimental import pallas as pl
from jax.experimental.pallas import tpu as pltpu
from jax.sharding import PartitionSpec as P

EPS = 1.5625e-07
MASK_VALUE = -1e30
LANES = 128
SUB = 256
NC = 512
PHASE_TOKENS = 128
CHUNKS = 4
COLS = 512
OUT_SLOTS = 5
MESH = pl.DeviceIdType.MESH
F32 = jnp.float32
BF16 = jnp.bfloat16
DMA = pltpu.SemaphoreType.DMA
scope = jax.named_scope


def dot(a, b, dims=(((1,), (0,)), ((), ()))):
    return lax.dot_general(a, b, dims, preferred_element_type=F32)


def block_kernel(dims, x_ref, kc_ref, vc_ref, table_ref, g_ref, wq_ref, b_ref, wo_ref,
                 y_ref, kn_ref, vn_ref, ring_ref, ringn_ref,
                 k_buf, v_buf, stage, kvn, qt_ref, hid_ref, x_buf, w_buf, cos_ref, sin_ref, kn_buf, vn_buf,
                 s_ref, p_ref, acc_ref, m_ref, l_ref, mc_ref, al_ref, bias_ref,
                 o_buf, res_buf, full_buf, mine_buf, send_buf, got_buf, y_buf,
                 in_sem, w_sem, out_sem, fetch_sem, own_send, pair_send, hop_send, new_send, recv, new_recv,
                 part_send, part_recv, y_send, y_recv, y_sem):
    n, ranks, groups, heads = dims
    me = lax.axis_index("cp")
    rank = lax.axis_index("tp")
    pair = me + 1 - 2 * lax.rem(me, 2)
    right, left, far = lax.rem(me + 2, n), lax.rem(me + n - 2, n), lax.rem(me + 4, n)
    tok, width = x_ref.shape
    part = stage.shape[3]
    span = CHUNKS * part + tok
    phases = tok // PHASE_TOKENS
    heads_per_tile = NC // PHASE_TOKENS
    tiles = heads // heads_per_tile
    per_group = phases * tiles
    count = groups * per_group
    spare = count
    half = kc_ref.shape[0] // 2
    scale = LANES ** -0.5 * math.log2(math.e)
    head_count = groups * (heads + 2)
    w_blocks = head_count * LANES // COLS
    heads_per_block = COLS // LANES
    pieces = width // COLS
    w_slots = w_buf.shape[0] // width
    out_depth = wo_ref.shape[0]
    rows = PHASE_TOKENS // ranks

    def remote(src, dst, send, got, axis, where):
        return pltpu.make_async_remote_copy(src_ref=src, dst_ref=dst, send_sem=send, recv_sem=got, device_id={axis: where}, device_id_type=MESH)

    def own_pair(c):
        return remote(stage.at[c], ring_ref.at[1, c], own_send.at[0, c], recv.at[1, c], "cp", pair)

    def own_right(c):
        return remote(stage.at[c], ring_ref.at[2 + c, 0], own_send.at[1, c], recv.at[2 + c, 0], "cp", right)

    def own_left(c):
        return remote(stage.at[c], ring_ref.at[2 + c, 1], own_send.at[2, c], recv.at[2 + c, 1], "cp", left)

    def to_pair(s, side):
        return remote(ring_ref.at[s, side], ring_ref.at[s, 2 + side], pair_send.at[s, side], recv.at[s, 2 + side], "cp", pair)

    def from_side(s, side):
        return remote(stage.at[0], ring_ref.at[s, side], own_send.at[0, 0], recv.at[s, side], "cp", pair)

    def hop_right(s):
        return remote(ring_ref.at[s, 0], ring_ref.at[s + 4, 0], hop_send.at[s], recv.at[s + 4, 0], "cp", right)

    def hop_left(s):
        return remote(ring_ref.at[s, 1], ring_ref.at[s + 2, 1], hop_send.at[s], recv.at[s + 2, 1], "cp", left)

    def new_copy(source, send, got, where, own=False):
        src = kvn if own else ringn_ref.at[source]
        return remote(src, ringn_ref.at[source], new_send.at[send], new_recv.at[got], "cp", where)

    new_right = new_copy(me, 0, 0, right, own=True)
    new_left = new_copy(me, 1, 1, left, own=True)
    new_pair = new_copy(me, 2, 3, pair, own=True)
    new_hop = new_copy(left, 3, 2, right)
    new_left_pair = new_copy(left, 4, 4, pair)
    new_right_pair = new_copy(right, 5, 5, pair)
    new_far_pair = new_copy(far, 6, 6, pair)

    def pass_on(s):
        for side in range(2):
            from_side(s, side).wait_recv()
            to_pair(s, side).start()

    def cache_in(i):
        here = pl.ds(i * half, half)
        return (pltpu.make_async_copy(kc_ref.at[here], k_buf.at[i, pl.ds(0, half)], in_sem.at[0, i]),
                pltpu.make_async_copy(vc_ref.at[here], v_buf.at[i, pl.ds(0, half)], in_sem.at[1, i]))

    x_in = pltpu.make_async_copy(x_ref, x_buf, in_sem.at[2, 0])

    def res_in(p):
        here = pl.ds(pl.multiple_of(p * PHASE_TOKENS + rank * rows, rows), rows)
        return pltpu.make_async_copy(x_ref.at[here], res_buf.at[p], in_sem.at[2 + p, 1])

    def w_in(j, slot):
        cols = pl.ds(pl.multiple_of(j * COLS, COLS), COLS)
        here = pl.ds(pl.multiple_of(slot * width, width), width)
        return pltpu.make_async_copy(wq_ref.at[:, cols], w_buf.at[here], w_sem.at[slot])

    def wo_at(slot):
        return pl.ds(pl.multiple_of(slot * out_depth, out_depth), out_depth)

    def wo_in(k):
        slot = lax.rem(k, OUT_SLOTS)
        cols = pl.ds(pl.multiple_of(k * COLS, COLS), COLS)
        return pltpu.make_async_copy(wo_ref.at[:, cols], w_buf.at[wo_at(slot)], w_sem.at[slot])

    x_in.start()
    for i in range(2):
        for copy in cache_in(i):
            copy.start()
    for j in range(w_slots):
        w_in(j, j).start()
    for p in range(phases):
        res_in(p).start()

    barrier = pltpu.get_barrier_semaphore()
    for other in (pair, right, left):
        pl.semaphore_signal(barrier, inc=1, device_id={"cp": other}, device_id_type=MESH)
    for d in range(1, ranks):
        pl.semaphore_signal(barrier, inc=1, device_id={"tp": lax.rem(rank + d, ranks)}, device_id_type=MESH)

    row = lax.broadcasted_iota(jnp.int32, (tok, NC), 0)
    col = lax.rem(lax.broadcasted_iota(jnp.int32, (tok, NC), 1), PHASE_TOKENS)
    bias_ref[0] = jnp.zeros((tok, NC), F32)
    for p in range(phases):
        bias_ref[1 + p] = jnp.where(row <= col + p * PHASE_TOKENS, 0.0, MASK_VALUE)
    bias_ref[1 + phases] = jnp.full((tok, NC), MASK_VALUE, F32)

    m_ref[...] = jnp.full(m_ref.shape, MASK_VALUE, F32)
    l_ref[...] = jnp.zeros(l_ref.shape, F32)
    acc_ref[...] = jnp.zeros(acc_ref.shape, F32)
    mc_ref[...] = jnp.zeros(mc_ref.shape, F32)
    al_ref[...] = jnp.ones(al_ref.shape, F32)

    with scope("wait_x"):
        x_in.wait()
    gain = g_ref[...].astype(F32).reshape(1, width)

    def norm(i, _):
        here = pl.ds(pl.multiple_of(i * 32, 32), 32)
        x = x_buf[here, :].astype(F32)
        inv_rms = lax.rsqrt(jnp.mean(x * x, axis=-1, keepdims=True) + EPS)
        hid_ref[here, :] = (x * inv_rms * gain).astype(BF16)
        return 0

    with scope("norm"):
        lax.fori_loop(0, tok // 32, norm, 0)
    lane = lax.broadcasted_iota(jnp.int32, (tok, LANES), 1)
    rope_lanes = table_ref.shape[0]
    table = jnp.concatenate([table_ref[...].T, jnp.zeros((tok, LANES - rope_lanes), F32)], axis=1)
    at = jnp.where(lane < rope_lanes, lane // 2, 0)
    sin = jnp.take_along_axis(table, at + rope_lanes // 2, axis=1)
    cos_ref[...] = jnp.take_along_axis(table, at, axis=1)
    sin_ref[...] = jnp.where(lane % 2 == 0, -sin, sin)

    def rotate(head):
        swapped = jnp.where(lane % 2 == 0, pltpu.roll(head, LANES - 1, 1), pltpu.roll(head, 1, 1))
        turned = head * cos_ref[...] + swapped * sin_ref[...]
        return jnp.where(lane < rope_lanes, turned, head)

    pair_rows = groups * LANES
    wide = lax.broadcasted_iota(jnp.int32, (pair_rows, pair_rows), 0)
    tall = lax.broadcasted_iota(jnp.int32, (pair_rows, pair_rows), 1)
    pick = (wide // groups + (wide % groups) * LANES == tall).astype(BF16)
    pick_t = (tall // groups + (tall % groups) * LANES == wide).astype(BF16)
    blocks = part // LANES

    def stage_out(c):
        return pltpu.make_async_copy(stage.at[c], ring_ref.at[0, c], out_sem.at[c])

    for c in range(CHUNKS):
        if c % (CHUNKS // 2) == 0:
            for copy in cache_in(c // (CHUNKS // 2)):
                copy.wait()

        def relayout(i, _):
            i_half = c // (CHUNKS // 2)
            src = pl.ds(pl.multiple_of((c % (CHUNKS // 2)) * part * groups + i * pair_rows, pair_rows), pair_rows)
            here = pl.ds(pl.multiple_of(i * LANES, LANES), LANES)
            keys = dot(pick_t, k_buf[i_half, src, :]).astype(BF16)
            vals = dot(v_buf[i_half, src, :], pick, (((0,), (0,)), ((), ()))).astype(BF16)
            for g in range(groups):
                stage[c, g, 0, here, :] = keys[g * LANES:(g + 1) * LANES, :]
                stage[c, g, 1, here, :] = vals[:, g * LANES:(g + 1) * LANES]
            return 0

        with scope("relayout"):
            lax.fori_loop(0, blocks, relayout, 0, unroll=4)
        stage_out(c).start()

    def send_own(chunks):
        for c in chunks:
            own_right(c).start()
            own_left(c).start()
            own_pair(c).start()

    with scope("barrier"):
        pl.semaphore_wait(barrier, 3 + ranks - 1)
    send_own(range(1))

    def a_rows(j):
        return pl.ds(pl.multiple_of(j * tok, tok), tok)

    def queries(j, i):
        head = j * heads_per_block + i
        g, h = head // (heads + 2), lax.rem(head, heads + 2)
        turned = rotate(s_ref[a_rows(j), i * LANES:(i + 1) * LANES]).T.astype(BF16)
        for p in range(phases):
            tile = jnp.where(h < heads, g * per_group + p * tiles + h // heads_per_tile, spare)
            at = pl.multiple_of(lax.rem(h, heads_per_tile) * PHASE_TOKENS, PHASE_TOKENS)
            qt_ref[tile, :, pl.ds(at, PHASE_TOKENS)] = turned[:, p * PHASE_TOKENS:(p + 1) * PHASE_TOKENS]

    def project(j, _):
        slot = lax.rem(j, w_slots)
        w_in(j, slot).wait()
        here = pl.ds(pl.multiple_of(slot * width, width), width)
        cols = pl.ds(pl.multiple_of(j * COLS, COLS), COLS)
        before = jnp.maximum(j - 1, 0)
        for i in range(heads_per_block):
            queries(before, i)
        s_ref[a_rows(j), :] = dot(hid_ref[...], w_buf[here, :]) + b_ref[cols].astype(F32).reshape(1, COLS)

        @pl.when(j + w_slots < w_blocks)
        def _():
            w_in(j + w_slots, slot).start()
        return 0

    s_ref[a_rows(0), :] = jnp.zeros((tok, COLS), F32)
    with scope("project"):
        lax.fori_loop(0, w_blocks, project, 0)
    for i in range(heads_per_block):
        queries(w_blocks - 1, i)

    kn_out = pltpu.make_async_copy(kn_buf, kn_ref, out_sem.at[CHUNKS])
    vn_out = pltpu.make_async_copy(vn_buf, vn_ref, out_sem.at[CHUNKS + 1])
    fresh = []
    kvn_out = pltpu.make_async_copy(kvn, ringn_ref.at[me], out_sem.at[CHUNKS + 2])
    for g in range(groups):
        at = (g * (heads + 2) + heads) * LANES
        keys = rotate(s_ref[a_rows(at // COLS), at % COLS:at % COLS + LANES])
        at += LANES
        vals = s_ref[a_rows(at // COLS), at % COLS:at % COLS + LANES]
        fresh.append((keys.astype(BF16), vals.astype(BF16)))
        kvn[g, 0] = keys.astype(BF16)
        for i in range(tok // LANES):
            here = slice(i * LANES, (i + 1) * LANES)
            kvn[g, 1, here, :] = vals[here, :].T.astype(BF16)
    for i in range(tok // LANES):
        here = slice(i * LANES, (i + 1) * LANES)
        for kind, buf in ((0, kn_buf), (1, vn_buf)):
            block = jnp.concatenate([fresh[g][kind][here, :] for g in range(groups)], axis=0)
            buf[i * pair_rows:(i + 1) * pair_rows, :] = dot(pick, block).astype(BF16)
    for c in range(CHUNKS):
        stage_out(c).wait()

    pair_left, pair_right, pair_far = lax.rem(pair + n - 2, n), lax.rem(pair + 2, n), lax.rem(pair + 4, n)

    def block_of(s):
        out = me
        for i, source in enumerate((pair, left, right, pair_left, pair_right, far, pair_far)):
            out = jnp.where(s == i + 1, source, out)
        return out

    def fetch(s, g, act):
        for kind, buf in ((0, k_buf), (1, v_buf)):
            for c in range(CHUNKS):
                here = pl.ds(c * part, part)
                getattr(pltpu.make_async_copy(ring_ref.at[s, c, g, kind], buf.at[g, here], fetch_sem.at[g, kind, c]), act)()
            here = pl.ds(CHUNKS * part, tok)
            getattr(pltpu.make_async_copy(ringn_ref.at[block_of(s), g, kind], buf.at[g, here], fetch_sem.at[g, kind, CHUNKS]), act)()

    kvn_out.start()
    for copy in (new_right, new_left, new_pair):
        copy.start()
    send_own(range(1, CHUNKS))
    kn_out.start()
    vn_out.start()

    kvn_out.wait()
    fetch(0, 0, "start")

    def step(a=None, b=None, c=None):
        alpha_b, alpha_c = al_ref[0], al_ref[1]
        shift = mc_ref[...]
        run = {"max": None, "sum": None, "out": None}

        def scores(i):
            keys = k_buf[a["slot"], i * SUB:(i + 1) * SUB, :]
            s = dot(keys, qt_ref[a["tile"]])
            if i == (span - tok) // SUB:
                edge = 1 + lax.rem(a["tile"], per_group) // tiles
                which = jnp.where(a["block"] < me, 0, jnp.where(a["block"] == me, edge, 1 + phases))
                s = s + bias_ref[which]
            s_ref[i * SUB:(i + 1) * SUB, :] = s
            top = jnp.max(s.reshape(SUB // 8, 8, NC), axis=0)
            run["max"] = top if run["max"] is None else jnp.maximum(run["max"], top)

        def weights(i):
            s = s_ref[i * SUB:(i + 1) * SUB, :]
            e = jnp.exp2((s * scale).reshape(SUB // 8, 8, NC) - shift[None])
            part_sum = jnp.sum(e, axis=0)
            run["sum"] = part_sum if run["sum"] is None else run["sum"] + part_sum
            p_ref[i * SUB:(i + 1) * SUB, :] = e.reshape(SUB, NC).astype(BF16)

        def values(i):
            at = i * SUB
            block = jnp.concatenate([v_buf[c["slot"], at + h * LANES:at + (h + 1) * LANES, :] for h in range(SUB // LANES)], axis=1)
            out = dot(block, p_ref[i * SUB:(i + 1) * SUB, :])
            run["out"] = out if run["out"] is None else run["out"] + out

        stages = ((c, values), (b, weights), (a, scores))
        for i in range(span // SUB):
            for spec, stage_fn in stages:
                if spec is not None:
                    stage_fn(i)
        if c is not None:
            acc_ref[c["tile"]] = acc_ref[c["tile"]] * alpha_c + run["out"]
        if b is not None:
            l_ref[b["tile"]] = l_ref[b["tile"]] * alpha_b + run["sum"]
            al_ref[1] = alpha_b
        if a is not None:
            old = m_ref[a["tile"]]
            new = jnp.maximum(old, jnp.max(run["max"], axis=0, keepdims=True))
            m_ref[a["tile"]] = new
            mc_ref[...] = jnp.broadcast_to(new * scale, mc_ref.shape)
            al_ref[0] = jnp.exp2((old - new) * scale)

    def main(tile, slot, block=None):
        return {"tile": tile, "slot": slot, "block": block}

    def run_unit(s, g, first, tile_count, carry, fetch_next):
        with scope("wait_fetch"):
            fetch(s, g, "wait")
        block = block_of(s)

        def one_tile(t, carry):
            with scope("fetch_next"):
                pl.when(t == tile_count - 1)(fetch_next)
            last, last_slot, older, older_slot = carry
            tile = g * per_group + first + t
            with scope("tile"):
                step(main(tile, g, block), main(last, last_slot), main(older, older_slot))
            return tile, jnp.int32(g), last, last_slot

        return lax.fori_loop(0, tile_count, one_tile, carry)

    start = tuple(jnp.int32(v) for v in (spare, 0, spare, 0))

    def got_new(i):
        new_copy(pair, 0, i, pair).wait_recv()

    def one_set(s, carry):
        nxt = s + 1
        carry = run_unit(s, 0, 0, per_group, carry, lambda: fetch(s, 1, "start"))
        with scope("pass_on"):
            pl.when(s >= 1)(lambda: pass_on(nxt))
        pl.when((s >= 1) & (s <= 2))(lambda: hop_right(nxt).start())
        pl.when((s >= 3) & (s <= 4))(lambda: hop_left(nxt).start())

        @pl.when(s == 2)
        def _():
            for copy in (new_hop, new_left_pair, new_right_pair):
                copy.start()

        @pl.when(s == n - 3)
        def _():
            got_new(2)
            new_far_pair.start()

        def fetch_next():
            @pl.when(s == 0)
            def _():
                for c in range(CHUNKS):
                    own_pair(c).wait_recv()
                got_new(3)

            @pl.when(s >= 1)
            def _():
                for side in range(2):
                    to_pair(nxt, side).wait_recv()

            @pl.when(s == 1)
            def _():
                got_new(0)
                got_new(1)

            pl.when(s == 3)(lambda: got_new(4))
            pl.when(s == 4)(lambda: got_new(5))
            fetch(nxt, 0, "start")

        return run_unit(s, 1, 0, per_group, carry, fetch_next)

    carry = lax.fori_loop(0, n - 2, one_set, start)
    kn_out.wait()
    vn_out.wait()

    def part_copy(p, k, d):
        to = lax.rem(rank + d, ranks)
        src = send_buf.at[k, pl.ds(pl.multiple_of(to * rows, rows), rows)]
        return remote(src, got_buf.at[p, k, d - 1], part_send.at[p, k, d - 1], part_recv.at[p, k, d - 1], "tp", to)

    def y_rows(p):
        return pl.ds(pl.multiple_of(p * PHASE_TOKENS + rank * rows, rows), rows)

    def y_copy(p, k, d):
        cols = pl.ds(pl.multiple_of(k * COLS, COLS), COLS)
        to = lax.rem(rank + d, ranks)
        return remote(y_buf.at[p, k], y_ref.at[y_rows(p), cols], y_send.at[p, k, d - 1], y_recv.at[p, k, d - 1], "tp", to)

    def y_own(p, k):
        cols = pl.ds(pl.multiple_of(k * COLS, COLS), COLS)
        return pltpu.make_async_copy(y_buf.at[p, k], y_ref.at[y_rows(p), cols], y_sem.at[p, k])

    def project_out(p):
        def piece(k, _):
            @pl.when(k < pieces)
            def _():
                wo_in(k).wait()
                out = dot(o_buf[...], w_buf[wo_at(lax.rem(k, OUT_SLOTS)), :])
                full_buf[...] = out
                send_buf[k] = out.astype(BF16)
                mine_buf[k] = full_buf[pl.ds(pl.multiple_of(rank * rows, rows), rows), :]
                pl.when(k + OUT_SLOTS < pieces)(lambda: wo_in(k + OUT_SLOTS).start())

            @pl.when(k >= 1)
            def _():
                for d in range(1, ranks):
                    part_copy(p, k - 1, d).start()
            return 0

        lax.fori_loop(0, pieces + 1, piece, 0)

    def reduce_out(p, lo, hi):
        def piece(k, _):
            @pl.when(k < hi)
            def _():
                for d in range(1, ranks):
                    part_copy(p, k, d).wait_recv()
                total = mine_buf[k]
                for d in range(1, ranks):
                    total = total + got_buf[p, k, d - 1].astype(F32)
                cols = pl.ds(pl.multiple_of(k * COLS, COLS), COLS)
                y_buf[p, k] = (res_buf[p, :, cols].astype(F32) + total).astype(BF16)

            @pl.when(k > lo)
            def _():
                y_own(p, k - 1).start()
                for d in range(1, ranks):
                    y_copy(p, k - 1, d).start()
            return 0

        lax.fori_loop(lo, hi + 1, piece, 0)

    def finish(p, g):
        def tile(h, _):
            t = g * per_group + p * tiles + h
            total = jnp.sum(l_ref[t], axis=0, keepdims=True)
            out = (acc_ref[t] / total).T.astype(BF16)
            for i in range(heads_per_tile):
                at = pl.multiple_of((g * heads + h * heads_per_tile + i) * LANES, LANES)
                o_buf[:, pl.ds(at, LANES)] = out[i * PHASE_TOKENS:(i + 1) * PHASE_TOKENS, :]
            return 0

        lax.fori_loop(0, tiles, tile, 0)

    for p in range(phases):
        res_in(p).wait()
    for k in range(OUT_SLOTS):
        wo_in(k).start()

    def one_phase(p, carry):
        first = p * tiles

        def late_set(s, carry):
            carry = run_unit(s, 0, first, tiles, carry, lambda: fetch(s, 1, "start"))
            with scope("pass_on_last"):
                pl.when((p == 0) & (s == n - 2))(lambda: pass_on(n - 1))
            with scope("reduce"):
                pl.when((p > 0) & (s == n - 1))(lambda: reduce_out(p - 1, 0, pieces))

            def fetch_next():
                @pl.when((p == 0) & (s == n - 2))
                def _():
                    for side in range(2):
                        to_pair(n - 1, side).wait_recv()
                    got_new(6)

                pl.when(s == n - 2)(lambda: fetch(n - 1, 0, "start"))
                pl.when((s == n - 1) & (p < phases - 1))(lambda: fetch(n - 2, 0, "start"))

            return run_unit(s, 1, first, tiles, carry, fetch_next)

        carry = lax.fori_loop(n - 2, n, late_set, carry)
        last, last_slot, older, older_slot = carry
        with scope("finish"):
            step(None, main(last, last_slot), main(older, older_slot))
            step(None, None, main(last, last_slot))
            for g in range(groups):
                finish(p, g)

        @pl.when(p > 0)
        def _():
            def sent(k, _):
                for d in range(1, ranks):
                    part_copy(p - 1, k, d).wait_send()
                return 0
            lax.fori_loop(0, pieces, sent, 0)
        with scope("project_out"):
            project_out(p)

        @pl.when(p < phases - 1)
        def _():
            for k in range(OUT_SLOTS):
                wo_in(k).start()
        return start

    lax.fori_loop(0, phases, one_phase, carry)
    with scope("reduce_last"):
        reduce_out(phases - 1, 0, pieces)

    for c in range(CHUNKS):
        own_right(c).wait_send()
        own_left(c).wait_send()
        own_pair(c).wait_send()
    for s in range(2, n):
        for side in range(2):
            to_pair(s, side).wait_send()
    for s in (2, 3):
        hop_right(s).wait_send()
    for s in (4, 5):
        hop_left(s).wait_send()
    for copy in (new_right, new_left, new_pair, new_hop, new_left_pair, new_right_pair, new_far_pair):
        copy.wait_send()

    def drain(k, _):
        for d in range(1, ranks):
            part_copy(phases - 1, k, d).wait_send()
        for p in range(phases):
            y_own(p, k).wait()
            for d in range(1, ranks):
                y_copy(p, k, d).wait_send()
                y_copy(p, k, d).wait_recv()
        return 0

    with scope("drain_out"):
        lax.fori_loop(0, pieces, drain, 0)


def results_kernel(y_in, kn_in, vn_in, y_out, kn_out, vn_out, y_buf, kn_buf, vn_buf, sem):
    rows = y_buf.shape[0] // 4
    copies = []
    for i in range(4):
        here = slice(i * rows, (i + 1) * rows)
        copies.append((y_in.at[here], y_buf.at[here], y_out.at[here]))
    copies += [(kn_in, kn_buf, kn_out), (vn_in, vn_buf, vn_out)]
    for i, (src, buf, _) in enumerate(copies):
        pltpu.make_async_copy(src, buf, sem.at[0, i]).start()
    for i, (src, buf, dst) in enumerate(copies):
        pltpu.make_async_copy(src, buf, sem.at[0, i]).wait()
        pltpu.make_async_copy(buf, dst, sem.at[1, i]).start()
    for i, (_, buf, dst) in enumerate(copies):
        pltpu.make_async_copy(buf, dst, sem.at[1, i]).wait()


def results(*arrays):
    any_spec = pl.BlockSpec(memory_space=pl.ANY)
    return pl.pallas_call(
        results_kernel,
        in_specs=[any_spec] * 3,
        out_specs=[any_spec] * 3,
        out_shape=[jax.ShapeDtypeStruct(a.shape, a.dtype) for a in arrays],
        scratch_shapes=[pltpu.VMEM(a.shape, a.dtype) for a in arrays] + [DMA((2, 6))],
        compiler_params=pltpu.CompilerParams(vmem_limit_bytes=62 << 20),
        name="results",
    )(*arrays)


def local_step(n, ranks, x, k_cache, v_cache, rope_table, norm_gain, w_qkv, b_qkv, w_out):
    positions, groups, head_dim = k_cache.shape
    tok, width = x.shape
    heads = w_qkv.shape[1] // groups // head_dim - 2
    part = positions // CHUNKS
    span = positions + tok
    phases = tok // PHASE_TOKENS
    tiles = heads * PHASE_TOKENS // NC
    count = groups * phases * tiles
    pieces = width // COLS
    rows = PHASE_TOKENS // ranks
    depth = w_out.shape[0]
    any_spec = pl.BlockSpec(memory_space=pl.ANY)
    vmem_spec = pl.BlockSpec(memory_space=pltpu.VMEM)
    flat = (positions * groups, head_dim)
    flops = 4 * count * NC * LANES * n * (span + tok)
    y, new_k, new_v, _, _ = pl.pallas_call(
        functools.partial(block_kernel, (n, ranks, groups, heads)),
        in_specs=[any_spec, any_spec, any_spec, vmem_spec, vmem_spec, any_spec, vmem_spec, any_spec],
        out_specs=[any_spec] * 5,
        out_shape=[
            jax.ShapeDtypeStruct((tok, width), BF16),
            jax.ShapeDtypeStruct((tok * groups, head_dim), BF16),
            jax.ShapeDtypeStruct((tok * groups, head_dim), BF16),
            jax.ShapeDtypeStruct((n, CHUNKS, groups, 2, part, head_dim), BF16),
            jax.ShapeDtypeStruct((n, groups, 2, tok, head_dim), BF16),
        ],
        scratch_shapes=[
            pltpu.VMEM((2, span, LANES), BF16),
            pltpu.VMEM((2, span, LANES), BF16),
            pltpu.VMEM((CHUNKS, groups, 2, part, LANES), BF16),
            pltpu.VMEM((groups, 2, tok, LANES), BF16),
            pltpu.VMEM((count + 1, LANES, NC), BF16),
            pltpu.VMEM((tok, width), BF16),
            pltpu.VMEM((tok, width), BF16),
            pltpu.VMEM((max(3 * width, OUT_SLOTS * depth), COLS), BF16),
            pltpu.VMEM((tok, LANES), F32),
            pltpu.VMEM((tok, LANES), F32),
            pltpu.VMEM((tok * groups, LANES), BF16),
            pltpu.VMEM((tok * groups, LANES), BF16),
            pltpu.VMEM((max(span, w_qkv.shape[1] // COLS * tok), NC), F32),
            pltpu.VMEM((span, NC), BF16),
            pltpu.VMEM((count + 1, LANES, NC), F32),
            pltpu.VMEM((count, 1, NC), F32),
            pltpu.VMEM((count + 1, 8, NC), F32),
            pltpu.VMEM((8, NC), F32),
            pltpu.VMEM((2, 1, NC), F32),
            pltpu.VMEM((2 + phases, tok, NC), F32),
            pltpu.VMEM((PHASE_TOKENS, groups * heads * LANES), BF16),
            pltpu.VMEM((phases, rows, width), BF16),
            pltpu.VMEM((PHASE_TOKENS, COLS), F32),
            pltpu.VMEM((pieces, rows, COLS), F32),
            pltpu.VMEM((pieces, PHASE_TOKENS, COLS), BF16),
            pltpu.VMEM((phases, pieces, ranks - 1, rows, COLS), BF16),
            pltpu.VMEM((phases, pieces, rows, COLS), BF16),
            DMA((2 + phases, 2)),
            DMA((OUT_SLOTS,)),
            DMA((CHUNKS + 3,)),
            DMA((groups, 2, CHUNKS + 1)),
            DMA((3, CHUNKS)),
            DMA((n, 2)),
            DMA((n,)),
            DMA((7,)),
            DMA((n, CHUNKS)),
            DMA((7,)),
            DMA((phases, pieces, ranks - 1)),
            DMA((phases, pieces, ranks - 1)),
            DMA((phases, pieces, ranks - 1)),
            DMA((phases, pieces, ranks - 1)),
            DMA((phases, pieces)),
        ],
        cost_estimate=pl.CostEstimate(flops=flops, bytes_accessed=4 * positions * n * groups * head_dim, transcendentals=flops // (4 * LANES)),
        compiler_params=pltpu.CompilerParams(collective_id=0, has_side_effects=True, vmem_limit_bytes=63 << 20),
        name="block",
    )(x, k_cache.reshape(flat), v_cache.reshape(flat), rope_table.T, norm_gain, w_qkv, b_qkv, w_out)
    y, new_k, new_v = results(y, new_k, new_v)
    new_shape = (tok,) + k_cache.shape[1:]
    return y, new_k.reshape(new_shape), new_v.reshape(new_shape)


def solution(mesh):
    row_spec = P(("dp", "cp"), None)
    cache_spec = P(("dp", "cp"), "tp", None)
    body = functools.partial(local_step, mesh.shape["cp"], mesh.shape["tp"])
    return jax.shard_map(body, mesh=mesh, in_specs=(row_spec, cache_spec, cache_spec, row_spec, P(None), P(None, "tp"), P("tp"), P("tp", None)), out_specs=(row_spec, cache_spec, cache_spec), check_vma=False)
```

```python
import functools
import math

import jax
import jax.numpy as jnp
from jax import lax
from jax.experimental import pallas as pl
from jax.experimental.pallas import tpu as pltpu
from jax.sharding import PartitionSpec as P

EPS = 1.5625e-07
MASK_VALUE = -1e30
LANES = 128
SUB = 256
NC = 512
PHASE_TOKENS = 128
CHUNKS = 4
COLS = 512
OUT_SLOTS = 6
MESH = pl.DeviceIdType.MESH
F32 = jnp.float32
BF16 = jnp.bfloat16
DMA = pltpu.SemaphoreType.DMA
scope = jax.named_scope


def dot(a, b, dims=(((1,), (0,)), ((), ()))):
    return lax.dot_general(a, b, dims, preferred_element_type=F32)


def block_kernel(dims, x_ref, kc_ref, vc_ref, table_ref, g_ref, wq_ref, b_ref, wo_ref,
                 y_ref, kn_ref, vn_ref, ring_ref, ringn_ref,
                 k_buf, v_buf, stage, kvn, qt_ref, hid_ref, x_buf, w_buf, cos_ref, sin_ref, kn_buf, vn_buf,
                 s_ref, p_ref, acc_ref, m_ref, l_ref, mc_ref, al_ref, bias_ref,
                 o_buf, res_buf, full_buf, mine_buf, near_buf, send_buf, comb_buf, got_buf, y_buf,
                 in_sem, w_sem, out_sem, fetch_sem, own_send, pair_send, hop_send, new_send, recv, new_recv,
                 part_send, part_recv, y_send, y_recv, y_sem):
    n, ranks, groups, heads = dims
    me = lax.axis_index("cp")
    rank = lax.axis_index("tp")
    pair = me + 1 - 2 * lax.rem(me, 2)
    right, left, far = lax.rem(me + 2, n), lax.rem(me + n - 2, n), lax.rem(me + 4, n)
    tok, width = x_ref.shape
    part = stage.shape[3]
    span = CHUNKS * part + tok
    phases = tok // PHASE_TOKENS
    heads_per_tile = NC // PHASE_TOKENS
    tiles = heads // heads_per_tile
    per_group = phases * tiles
    count = groups * per_group
    spare = count
    half = kc_ref.shape[0] // 2
    scale = LANES ** -0.5 * math.log2(math.e)
    head_count = groups * (heads + 2)
    w_blocks = head_count * LANES // COLS
    heads_per_block = COLS // LANES
    pieces = width // COLS
    w_slots = w_buf.shape[0] // width
    out_depth = wo_ref.shape[0]
    rows = PHASE_TOKENS // ranks

    def remote(src, dst, send, got, axis, where):
        return pltpu.make_async_remote_copy(src_ref=src, dst_ref=dst, send_sem=send, recv_sem=got, device_id={axis: where}, device_id_type=MESH)

    def own_pair(c):
        return remote(stage.at[c], ring_ref.at[1, c], own_send.at[0, c], recv.at[1, c], "cp", pair)

    def own_right(c):
        return remote(stage.at[c], ring_ref.at[2 + c, 0], own_send.at[1, c], recv.at[2 + c, 0], "cp", right)

    def own_left(c):
        return remote(stage.at[c], ring_ref.at[2 + c, 1], own_send.at[2, c], recv.at[2 + c, 1], "cp", left)

    def to_pair(s, side):
        return remote(ring_ref.at[s, side], ring_ref.at[s, 2 + side], pair_send.at[s, side], recv.at[s, 2 + side], "cp", pair)

    def from_side(s, side):
        return remote(stage.at[0], ring_ref.at[s, side], own_send.at[0, 0], recv.at[s, side], "cp", pair)

    def hop_right(s):
        return remote(ring_ref.at[s, 0], ring_ref.at[s + 4, 0], hop_send.at[s], recv.at[s + 4, 0], "cp", right)

    def hop_left(s):
        return remote(ring_ref.at[s, 1], ring_ref.at[s + 2, 1], hop_send.at[s], recv.at[s + 2, 1], "cp", left)

    def new_copy(source, send, got, where, own=False):
        src = kvn if own else ringn_ref.at[source]
        return remote(src, ringn_ref.at[source], new_send.at[send], new_recv.at[got], "cp", where)

    new_right = new_copy(me, 0, 0, right, own=True)
    new_left = new_copy(me, 1, 1, left, own=True)
    new_pair = new_copy(me, 2, 3, pair, own=True)
    new_hop = new_copy(left, 3, 2, right)
    new_left_pair = new_copy(left, 4, 4, pair)
    new_right_pair = new_copy(right, 5, 5, pair)
    new_far_pair = new_copy(far, 6, 6, pair)

    def pass_on(s):
        for side in range(2):
            from_side(s, side).wait_recv()
            to_pair(s, side).start()

    def cache_in(i):
        here = pl.ds(i * half, half)
        return (pltpu.make_async_copy(kc_ref.at[here], k_buf.at[i, pl.ds(0, half)], in_sem.at[0, i]),
                pltpu.make_async_copy(vc_ref.at[here], v_buf.at[i, pl.ds(0, half)], in_sem.at[1, i]))

    x_in = pltpu.make_async_copy(x_ref, x_buf, in_sem.at[2, 0])

    def res_in(p):
        here = pl.ds(pl.multiple_of(p * PHASE_TOKENS + rank * rows, rows), rows)
        return pltpu.make_async_copy(x_ref.at[here], res_buf.at[p], in_sem.at[2 + p, 1])

    def w_in(j, slot):
        cols = pl.ds(pl.multiple_of(j * COLS, COLS), COLS)
        here = pl.ds(pl.multiple_of(slot * width, width), width)
        return pltpu.make_async_copy(wq_ref.at[:, cols], w_buf.at[here], w_sem.at[slot])

    def order(j):
        return lax.rem(j + heads * LANES // COLS, w_blocks)

    def wo_at(slot):
        return pl.ds(pl.multiple_of(slot * out_depth, out_depth), out_depth)

    def wo_in(k):
        slot = lax.rem(k, OUT_SLOTS)
        cols = pl.ds(pl.multiple_of(k * COLS, COLS), COLS)
        return pltpu.make_async_copy(wo_ref.at[:, cols], w_buf.at[wo_at(slot)], w_sem.at[slot])

    x_in.start()
    for i in range(2):
        for copy in cache_in(i):
            copy.start()
    for j in range(w_slots):
        w_in(order(j), j).start()
    for p in range(phases):
        res_in(p).start()

    barrier = pltpu.get_barrier_semaphore()
    for other in (pair, right, left):
        pl.semaphore_signal(barrier, inc=1, device_id={"cp": other}, device_id_type=MESH)
    for d in range(1, ranks):
        pl.semaphore_signal(barrier, inc=1, device_id={"tp": lax.rem(rank + d, ranks)}, device_id_type=MESH)

    row = lax.broadcasted_iota(jnp.int32, (tok, NC), 0)
    col = lax.rem(lax.broadcasted_iota(jnp.int32, (tok, NC), 1), PHASE_TOKENS)
    bias_ref[0] = jnp.zeros((tok, NC), F32)
    for p in range(phases):
        bias_ref[1 + p] = jnp.where(row <= col + p * PHASE_TOKENS, 0.0, MASK_VALUE)
    bias_ref[1 + phases] = jnp.full((tok, NC), MASK_VALUE, F32)

    m_ref[...] = jnp.full(m_ref.shape, MASK_VALUE, F32)
    l_ref[...] = jnp.zeros(l_ref.shape, F32)
    acc_ref[...] = jnp.zeros(acc_ref.shape, F32)
    mc_ref[...] = jnp.zeros(mc_ref.shape, F32)
    al_ref[...] = jnp.ones(al_ref.shape, F32)

    with scope("wait_x"):
        x_in.wait()
    gain = g_ref[...].astype(F32).reshape(1, width)

    def norm(i, _):
        here = pl.ds(pl.multiple_of(i * 32, 32), 32)
        x = x_buf[here, :].astype(F32)
        inv_rms = lax.rsqrt(jnp.mean(x * x, axis=-1, keepdims=True) + EPS)
        hid_ref[here, :] = (x * inv_rms * gain).astype(BF16)
        return 0

    with scope("norm"):
        lax.fori_loop(0, tok // 32, norm, 0)
    lane = lax.broadcasted_iota(jnp.int32, (tok, LANES), 1)
    rope_lanes = table_ref.shape[0]
    table = jnp.concatenate([table_ref[...].T, jnp.zeros((tok, LANES - rope_lanes), F32)], axis=1)
    at = jnp.where(lane < rope_lanes, lane // 2, 0)
    sin = jnp.take_along_axis(table, at + rope_lanes // 2, axis=1)
    cos_ref[...] = jnp.take_along_axis(table, at, axis=1)
    sin_ref[...] = jnp.where(lane % 2 == 0, -sin, sin)

    def rotate(head):
        swapped = jnp.where(lane % 2 == 0, pltpu.roll(head, LANES - 1, 1), pltpu.roll(head, 1, 1))
        turned = head * cos_ref[...] + swapped * sin_ref[...]
        return jnp.where(lane < rope_lanes, turned, head)

    pair_rows = groups * LANES
    wide = lax.broadcasted_iota(jnp.int32, (pair_rows, pair_rows), 0)
    tall = lax.broadcasted_iota(jnp.int32, (pair_rows, pair_rows), 1)
    pick = (wide // groups + (wide % groups) * LANES == tall).astype(BF16)
    pick_t = (tall // groups + (tall % groups) * LANES == wide).astype(BF16)
    blocks = part // LANES

    def stage_out(c):
        return pltpu.make_async_copy(stage.at[c], ring_ref.at[0, c], out_sem.at[c])

    for c in range(CHUNKS):
        if c % (CHUNKS // 2) == 0:
            for copy in cache_in(c // (CHUNKS // 2)):
                copy.wait()

        def relayout(i, _):
            i_half = c // (CHUNKS // 2)
            src = pl.ds(pl.multiple_of((c % (CHUNKS // 2)) * part * groups + i * pair_rows, pair_rows), pair_rows)
            here = pl.ds(pl.multiple_of(i * LANES, LANES), LANES)
            keys = dot(pick_t, k_buf[i_half, src, :]).astype(BF16)
            vals = dot(v_buf[i_half, src, :], pick, (((0,), (0,)), ((), ()))).astype(BF16)
            for g in range(groups):
                stage[c, g, 0, here, :] = keys[g * LANES:(g + 1) * LANES, :]
                stage[c, g, 1, here, :] = vals[:, g * LANES:(g + 1) * LANES]
            return 0

        with scope("relayout"):
            lax.fori_loop(0, blocks, relayout, 0, unroll=4)
        stage_out(c).start()

    def send_own(chunks):
        for c in chunks:
            own_right(c).start()
            own_left(c).start()
            own_pair(c).start()

    with scope("barrier"):
        pl.semaphore_wait(barrier, 3 + ranks - 1)
    send_own(range(1))

    pair_left, pair_right, pair_far = lax.rem(pair + n - 2, n), lax.rem(pair + 2, n), lax.rem(pair + 4, n)

    def block_of(s):
        out = me
        for i, source in enumerate((pair, left, right, pair_left, pair_right, far, pair_far)):
            out = jnp.where(s == i + 1, source, out)
        return out

    def fetch_cache(s, g, act):
        for kind, buf in ((0, k_buf), (1, v_buf)):
            for c in range(CHUNKS):
                here = pl.ds(c * part, part)
                getattr(pltpu.make_async_copy(ring_ref.at[s, c, g, kind], buf.at[g, here], fetch_sem.at[g, kind, c]), act)()

    def fetch_block(s, g, act):
        for kind, buf in ((0, k_buf), (1, v_buf)):
            here = pl.ds(CHUNKS * part, tok)
            getattr(pltpu.make_async_copy(ringn_ref.at[block_of(s), g, kind], buf.at[g, here], fetch_sem.at[g, kind, CHUNKS]), act)()

    def fetch(s, g, act):
        fetch_cache(s, g, act)
        fetch_block(s, g, act)

    def a_rows(j):
        return pl.ds(pl.multiple_of(j * tok, tok), tok)

    def queries(j, i):
        head = j * heads_per_block + i
        g, h = head // (heads + 2), lax.rem(head, heads + 2)
        turned = rotate(s_ref[a_rows(j), i * LANES:(i + 1) * LANES]).T.astype(BF16)
        for p in range(phases):
            tile = jnp.where(h < heads, g * per_group + p * tiles + h // heads_per_tile, spare)
            at = pl.multiple_of(lax.rem(h, heads_per_tile) * PHASE_TOKENS, PHASE_TOKENS)
            qt_ref[tile, :, pl.ds(at, PHASE_TOKENS)] = turned[:, p * PHASE_TOKENS:(p + 1) * PHASE_TOKENS]

    def project(j, _):
        slot = lax.rem(j, w_slots)
        block = order(j)
        w_in(block, slot).wait()
        here = pl.ds(pl.multiple_of(slot * width, width), width)
        cols = pl.ds(pl.multiple_of(block * COLS, COLS), COLS)
        before = order(jnp.maximum(j - 1, 0))
        for i in range(heads_per_block):
            queries(before, i)
        s_ref[a_rows(block), :] = dot(hid_ref[...], w_buf[here, :]) + b_ref[cols].astype(F32).reshape(1, COLS)

        @pl.when(j + w_slots < w_blocks)
        def _():
            w_in(order(j + w_slots), slot).start()
        return 0

    for c in range(CHUNKS):
        stage_out(c).wait()
    fetch_cache(0, 0, "start")
    early = ((groups - 1) * (heads + 2) + heads) * LANES // COLS - heads * LANES // COLS + 1
    with scope("project"):
        lax.fori_loop(0, early, project, 0)

    kn_out = pltpu.make_async_copy(kn_buf, kn_ref, out_sem.at[CHUNKS])
    vn_out = pltpu.make_async_copy(vn_buf, vn_ref, out_sem.at[CHUNKS + 1])
    fresh = []
    kvn_out = pltpu.make_async_copy(kvn, ringn_ref.at[me], out_sem.at[CHUNKS + 2])
    for g in range(groups):
        at = (g * (heads + 2) + heads) * LANES
        keys = rotate(s_ref[a_rows(at // COLS), at % COLS:at % COLS + LANES])
        at += LANES
        vals = s_ref[a_rows(at // COLS), at % COLS:at % COLS + LANES]
        fresh.append((keys.astype(BF16), vals.astype(BF16)))
        kvn[g, 0] = keys.astype(BF16)
        for i in range(tok // LANES):
            here = slice(i * LANES, (i + 1) * LANES)
            kvn[g, 1, here, :] = vals[here, :].T.astype(BF16)
    for i in range(tok // LANES):
        here = slice(i * LANES, (i + 1) * LANES)
        for kind, buf in ((0, kn_buf), (1, vn_buf)):
            block = jnp.concatenate([fresh[g][kind][here, :] for g in range(groups)], axis=0)
            buf[i * pair_rows:(i + 1) * pair_rows, :] = dot(pick, block).astype(BF16)
    kvn_out.start()
    for copy in (new_right, new_left, new_pair):
        copy.start()
    send_own(range(1, CHUNKS))
    kn_out.start()
    vn_out.start()
    with scope("project"):
        lax.fori_loop(early, w_blocks, project, 0)
    for i in range(heads_per_block):
        queries(order(w_blocks - 1), i)
    kvn_out.wait()
    fetch_block(0, 0, "start")

    def step(a=None, b=None, c=None):
        alpha_b, alpha_c = al_ref[0], al_ref[1]
        shift = mc_ref[...]
        run = {"max": None, "sum": None, "out": None}

        def scores(i):
            keys = k_buf[a["slot"], i * SUB:(i + 1) * SUB, :]
            s = dot(keys, qt_ref[a["tile"]])
            if i == (span - tok) // SUB:
                edge = 1 + lax.rem(a["tile"], per_group) // tiles
                which = jnp.where(a["block"] < me, 0, jnp.where(a["block"] == me, edge, 1 + phases))
                s = s + bias_ref[which]
            s_ref[i * SUB:(i + 1) * SUB, :] = s
            top = jnp.max(s.reshape(SUB // 8, 8, NC), axis=0)
            run["max"] = top if run["max"] is None else jnp.maximum(run["max"], top)

        def weights(i):
            s = s_ref[i * SUB:(i + 1) * SUB, :]
            e = jnp.exp2((s * scale).reshape(SUB // 8, 8, NC) - shift[None])
            part_sum = jnp.sum(e, axis=0)
            run["sum"] = part_sum if run["sum"] is None else run["sum"] + part_sum
            p_ref[i * SUB:(i + 1) * SUB, :] = e.reshape(SUB, NC).astype(BF16)

        def values(i):
            at = i * SUB
            block = jnp.concatenate([v_buf[c["slot"], at + h * LANES:at + (h + 1) * LANES, :] for h in range(SUB // LANES)], axis=1)
            out = dot(block, p_ref[i * SUB:(i + 1) * SUB, :])
            run["out"] = out if run["out"] is None else run["out"] + out

        stages = ((c, values), (b, weights), (a, scores))
        for i in range(span // SUB):
            for spec, stage_fn in stages:
                if spec is not None:
                    stage_fn(i)
        if c is not None:
            acc_ref[c["tile"]] = acc_ref[c["tile"]] * alpha_c + run["out"]
        if b is not None:
            l_ref[b["tile"]] = l_ref[b["tile"]] * alpha_b + run["sum"]
            al_ref[1] = alpha_b
        if a is not None:
            old = m_ref[a["tile"]]
            new = jnp.maximum(old, jnp.max(run["max"], axis=0, keepdims=True))
            m_ref[a["tile"]] = new
            mc_ref[...] = jnp.broadcast_to(new * scale, mc_ref.shape)
            al_ref[0] = jnp.exp2((old - new) * scale)

    def main(tile, slot, block=None):
        return {"tile": tile, "slot": slot, "block": block}

    def run_unit(s, g, first, tile_count, carry, fetch_next):
        with scope("wait_fetch"):
            fetch(s, g, "wait")
        block = block_of(s)

        def one_tile(t, carry):
            with scope("fetch_next"):
                pl.when(t == tile_count - 1)(fetch_next)
            last, last_slot, older, older_slot = carry
            tile = g * per_group + first + t
            with scope("tile"):
                step(main(tile, g, block), main(last, last_slot), main(older, older_slot))
            return tile, jnp.int32(g), last, last_slot

        return lax.fori_loop(0, tile_count, one_tile, carry)

    start = tuple(jnp.int32(v) for v in (spare, 0, spare, 0))

    def got_new(i):
        new_copy(pair, 0, i, pair).wait_recv()

    def one_set(s, carry):
        nxt = s + 1
        carry = run_unit(s, 0, 0, per_group, carry, lambda: fetch(s, 1, "start"))
        with scope("pass_on"):
            pl.when(s >= 1)(lambda: pass_on(nxt))

        @pl.when(s == 2)
        def _():
            for copy in (new_hop, new_left_pair, new_right_pair):
                copy.start()

        pl.when((s >= 1) & (s <= 2))(lambda: hop_right(nxt).start())
        pl.when((s >= 3) & (s <= 4))(lambda: hop_left(nxt).start())

        @pl.when(s == n - 3)
        def _():
            got_new(2)
            new_far_pair.start()

        def fetch_next():
            @pl.when(s == 0)
            def _():
                for c in range(CHUNKS):
                    own_pair(c).wait_recv()
                got_new(3)

            @pl.when(s >= 1)
            def _():
                for side in range(2):
                    to_pair(nxt, side).wait_recv()

            @pl.when(s == 1)
            def _():
                got_new(0)
                got_new(1)

            pl.when(s == 3)(lambda: got_new(4))
            pl.when(s == 4)(lambda: got_new(5))
            fetch(nxt, 0, "start")

        return run_unit(s, 1, 0, per_group, carry, fetch_next)

    carry = lax.fori_loop(0, n - 2, one_set, start)
    kn_out.wait()
    vn_out.wait()

    right_rank, left_rank, far_rank = lax.rem(rank + 1, ranks), lax.rem(rank + ranks - 1, ranks), lax.rem(rank + 2, ranks)

    def onward(k):
        return jnp.where(lax.rem(k, 2) == 0, right_rank, left_rank)

    def back(k):
        return jnp.where(lax.rem(k, 2) == 0, left_rank, right_rank)

    def band(of):
        return pl.ds(pl.multiple_of(of * rows, rows), rows)

    def far_copy(p, k):
        return remote(send_buf.at[k, band(far_rank)], got_buf.at[p, 0, k], part_send.at[p, 0, k], part_recv.at[p, 0, k], "tp", onward(k))

    def near_copy(p, k):
        return remote(send_buf.at[k, band(back(k))], got_buf.at[p, 1, k], part_send.at[p, 1, k], part_recv.at[p, 1, k], "tp", back(k))

    def comb_copy(p, k):
        return remote(comb_buf.at[p, k], got_buf.at[p, 2, k], part_send.at[p, 2, k], part_recv.at[p, 2, k], "tp", onward(k))

    def piece_cols(k):
        return pl.ds(pl.multiple_of(k * COLS, COLS), COLS)

    def y_rows(p, of):
        return pl.ds(pl.multiple_of(p * PHASE_TOKENS + of * rows, rows), rows)

    def y_copy(p, k, way):
        dst = y_ref.at[y_rows(p, rank), piece_cols(k)]
        return remote(y_buf.at[p, k], dst, y_send.at[p, way, k], y_recv.at[p, way, k], "tp", back(k) if way else onward(k))

    def y_forward(p, k):
        here = y_ref.at[y_rows(p, back(k)), piece_cols(k)]
        return remote(here, here, y_send.at[p, 2, k], y_recv.at[p, 2, k], "tp", onward(k))

    def y_own(p, k):
        return pltpu.make_async_copy(y_buf.at[p, k], y_ref.at[y_rows(p, rank), piece_cols(k)], y_sem.at[p, k])

    def each_piece(body, extra=0):
        def piece(k, _):
            body(k)
            return 0
        lax.fori_loop(0, pieces + extra, piece, 0)

    def project_out(p):
        if p > 0:
            def sent(k):
                far_copy(p - 1, k).wait_send()
                near_copy(p - 1, k).wait_send()
            each_piece(sent)

        def piece(k):
            @pl.when(k < pieces)
            def _():
                wo_in(k).wait()
                out = dot(o_buf[...], w_buf[wo_at(lax.rem(k, OUT_SLOTS)), :])
                full_buf[...] = out
                send_buf[k] = out.astype(BF16)
                mine_buf[k] = full_buf[band(rank), :]
                near_buf[k] = full_buf[band(onward(k)), :]
                pl.when(k + OUT_SLOTS < pieces)(lambda: wo_in(k + OUT_SLOTS).start())

            @pl.when(k >= 1)
            def _():
                far_copy(p, k - 1).start()
                near_copy(p, k - 1).start()

        each_piece(piece, 1)

    def combine(p):
        def piece(k):
            @pl.when(k < pieces)
            def _():
                far_copy(p, k).wait_recv()
                comb_buf[p, k] = (near_buf[k] + got_buf[p, 0, k].astype(F32)).astype(BF16)

            pl.when(k >= 1)(lambda: comb_copy(p, k - 1).start())

        each_piece(piece, 1)

    def reduce(p):
        def piece(k):
            @pl.when(k < pieces)
            def _():
                near_copy(p, k).wait_recv()
                comb_copy(p, k).wait_recv()
                total = mine_buf[k] + got_buf[p, 1, k].astype(F32) + got_buf[p, 2, k].astype(F32)
                y_buf[p, k] = (res_buf[p, :, piece_cols(k)].astype(F32) + total).astype(BF16)

            @pl.when(k >= 1)
            def _():
                y_copy(p, k - 1, 0).start()
                y_copy(p, k - 1, 1).start()
                y_own(p, k - 1).start()

        each_piece(piece, 1)

    def forward(p):
        def piece(k):
            y_copy(p, k, 0).wait_recv()
            y_forward(p, k).start()
        each_piece(piece)

    def finish(p, g):
        def tile(h, _):
            t = g * per_group + p * tiles + h
            total = jnp.sum(l_ref[t], axis=0, keepdims=True)
            out = (acc_ref[t] / total).T.astype(BF16)
            for i in range(heads_per_tile):
                at = pl.multiple_of((g * heads + h * heads_per_tile + i) * LANES, LANES)
                o_buf[:, pl.ds(at, LANES)] = out[i * PHASE_TOKENS:(i + 1) * PHASE_TOKENS, :]
            return 0

        lax.fori_loop(0, tiles, tile, 0)

    for p in range(phases):
        res_in(p).wait()
    for k in range(OUT_SLOTS):
        wo_in(k).start()

    def late(p, carry):
        first = p * tiles

        def between(s, g):
            if p == 0 and g == 0:
                pl.when(s == n - 2)(lambda: pass_on(n - 1))
            if p > 0:
                @pl.when(s == n - 2)
                def _():
                    if g == 0:
                        with scope("project_out"):
                            for other in range(groups):
                                finish(p - 1, other)
                            project_out(p - 1)
                        for k in range(OUT_SLOTS):
                            wo_in(k).start()
                    else:
                        with scope("combine"):
                            combine(p - 1)

                @pl.when(s == n - 1)
                def _():
                    with scope("reduce"):
                        reduce(p - 1) if g == 0 else forward(p - 1)

        def late_set(s, carry):
            carry = run_unit(s, 0, first, tiles, carry, lambda: fetch(s, 1, "start"))
            between(s, 0)

            def fetch_next():
                @pl.when(s == n - 2)
                def _():
                    if p == 0:
                        for side in range(2):
                            to_pair(n - 1, side).wait_recv()
                        got_new(6)
                    fetch(n - 1, 0, "start")
                if p < phases - 1:
                    pl.when(s == n - 1)(lambda: fetch(n - 2, 0, "start"))

            carry = run_unit(s, 1, first, tiles, carry, fetch_next)
            between(s, 1)
            return carry

        return lax.fori_loop(n - 2, n, late_set, carry)

    for p in range(phases):
        carry = late(p, carry)
    last, last_slot, older, older_slot = carry
    with scope("finish"):
        step(None, main(last, last_slot), main(older, older_slot))
        step(None, None, main(last, last_slot))
        for g in range(groups):
            finish(phases - 1, g)
    with scope("project_out"):
        project_out(phases - 1)
    with scope("combine"):
        combine(phases - 1)
    with scope("reduce"):
        reduce(phases - 1)
    with scope("forward"):
        forward(phases - 1)

    for c in range(CHUNKS):
        own_right(c).wait_send()
        own_left(c).wait_send()
        own_pair(c).wait_send()
    for s in range(2, n):
        for side in range(2):
            to_pair(s, side).wait_send()
    for s in (2, 3):
        hop_right(s).wait_send()
    for s in (4, 5):
        hop_left(s).wait_send()
    for copy in (new_right, new_left, new_pair, new_hop, new_left_pair, new_right_pair, new_far_pair):
        copy.wait_send()

    def drain(k):
        far_copy(phases - 1, k).wait_send()
        near_copy(phases - 1, k).wait_send()
        for p in range(phases):
            comb_copy(p, k).wait_send()
            y_own(p, k).wait()
            y_copy(p, k, 0).wait_send()
            y_copy(p, k, 1).wait_send()
            y_copy(p, k, 1).wait_recv()
            y_forward(p, k).wait_send()
            y_forward(p, k).wait_recv()

    with scope("drain_out"):
        each_piece(drain)


def results_kernel(y_in, kn_in, vn_in, y_out, kn_out, vn_out, y_buf, kn_buf, vn_buf, sem):
    rows = y_buf.shape[0] // 4
    copies = []
    for i in range(4):
        here = slice(i * rows, (i + 1) * rows)
        copies.append((y_in.at[here], y_buf.at[here], y_out.at[here]))
    copies += [(kn_in, kn_buf, kn_out), (vn_in, vn_buf, vn_out)]
    for i, (src, buf, _) in enumerate(copies):
        pltpu.make_async_copy(src, buf, sem.at[0, i]).start()
    for i, (src, buf, dst) in enumerate(copies):
        pltpu.make_async_copy(src, buf, sem.at[0, i]).wait()
        pltpu.make_async_copy(buf, dst, sem.at[1, i]).start()
    for i, (_, buf, dst) in enumerate(copies):
        pltpu.make_async_copy(buf, dst, sem.at[1, i]).wait()


def results(*arrays):
    any_spec = pl.BlockSpec(memory_space=pl.ANY)
    return pl.pallas_call(
        results_kernel,
        in_specs=[any_spec] * 3,
        out_specs=[any_spec] * 3,
        out_shape=[jax.ShapeDtypeStruct(a.shape, a.dtype) for a in arrays],
        scratch_shapes=[pltpu.VMEM(a.shape, a.dtype) for a in arrays] + [DMA((2, 6))],
        compiler_params=pltpu.CompilerParams(vmem_limit_bytes=62 << 20),
        name="results",
    )(*arrays)


def local_step(n, ranks, x, k_cache, v_cache, rope_table, norm_gain, w_qkv, b_qkv, w_out):
    positions, groups, head_dim = k_cache.shape
    tok, width = x.shape
    heads = w_qkv.shape[1] // groups // head_dim - 2
    part = positions // CHUNKS
    span = positions + tok
    phases = tok // PHASE_TOKENS
    tiles = heads * PHASE_TOKENS // NC
    count = groups * phases * tiles
    pieces = width // COLS
    rows = PHASE_TOKENS // ranks
    depth = w_out.shape[0]
    any_spec = pl.BlockSpec(memory_space=pl.ANY)
    vmem_spec = pl.BlockSpec(memory_space=pltpu.VMEM)
    flat = (positions * groups, head_dim)
    flops = 4 * count * NC * LANES * n * (span + tok)
    y, new_k, new_v, _, _ = pl.pallas_call(
        functools.partial(block_kernel, (n, ranks, groups, heads)),
        in_specs=[any_spec, any_spec, any_spec, vmem_spec, vmem_spec, any_spec, vmem_spec, any_spec],
        out_specs=[any_spec] * 5,
        out_shape=[
            jax.ShapeDtypeStruct((tok, width), BF16),
            jax.ShapeDtypeStruct((tok * groups, head_dim), BF16),
            jax.ShapeDtypeStruct((tok * groups, head_dim), BF16),
            jax.ShapeDtypeStruct((n, CHUNKS, groups, 2, part, head_dim), BF16),
            jax.ShapeDtypeStruct((n, groups, 2, tok, head_dim), BF16),
        ],
        scratch_shapes=[
            pltpu.VMEM((2, span, LANES), BF16),
            pltpu.VMEM((2, span, LANES), BF16),
            pltpu.VMEM((CHUNKS, groups, 2, part, LANES), BF16),
            pltpu.VMEM((groups, 2, tok, LANES), BF16),
            pltpu.VMEM((count + 1, LANES, NC), BF16),
            pltpu.VMEM((tok, width), BF16),
            pltpu.VMEM((tok, width), BF16),
            pltpu.VMEM((max(3 * width, OUT_SLOTS * depth), COLS), BF16),
            pltpu.VMEM((tok, LANES), F32),
            pltpu.VMEM((tok, LANES), F32),
            pltpu.VMEM((tok * groups, LANES), BF16),
            pltpu.VMEM((tok * groups, LANES), BF16),
            pltpu.VMEM((max(span, w_qkv.shape[1] // COLS * tok), NC), F32),
            pltpu.VMEM((span, NC), BF16),
            pltpu.VMEM((count + 1, LANES, NC), F32),
            pltpu.VMEM((count, 1, NC), F32),
            pltpu.VMEM((count + 1, 8, NC), F32),
            pltpu.VMEM((8, NC), F32),
            pltpu.VMEM((2, 1, NC), F32),
            pltpu.VMEM((2 + phases, tok, NC), F32),
            pltpu.VMEM((PHASE_TOKENS, groups * heads * LANES), BF16),
            pltpu.VMEM((phases, rows, width), BF16),
            pltpu.VMEM((PHASE_TOKENS, COLS), F32),
            pltpu.VMEM((pieces, rows, COLS), F32),
            pltpu.VMEM((pieces, rows, COLS), F32),
            pltpu.VMEM((pieces, PHASE_TOKENS, COLS), BF16),
            pltpu.VMEM((phases, pieces, rows, COLS), BF16),
            pltpu.VMEM((phases, 3, pieces, rows, COLS), BF16),
            pltpu.VMEM((phases, pieces, rows, COLS), BF16),
            DMA((2 + phases, 2)),
            DMA((OUT_SLOTS,)),
            DMA((CHUNKS + 3,)),
            DMA((groups, 2, CHUNKS + 1)),
            DMA((3, CHUNKS)),
            DMA((n, 2)),
            DMA((n,)),
            DMA((7,)),
            DMA((n, CHUNKS)),
            DMA((7,)),
            DMA((phases, 3, pieces)),
            DMA((phases, 3, pieces)),
            DMA((phases, 3, pieces)),
            DMA((phases, 3, pieces)),
            DMA((phases, pieces)),
        ],
        cost_estimate=pl.CostEstimate(flops=flops, bytes_accessed=4 * positions * n * groups * head_dim, transcendentals=flops // (4 * LANES)),
        compiler_params=pltpu.CompilerParams(collective_id=0, has_side_effects=True, vmem_limit_bytes=63 << 20),
        name="block",
    )(x, k_cache.reshape(flat), v_cache.reshape(flat), rope_table.T, norm_gain, w_qkv, b_qkv, w_out)
    y, new_k, new_v = results(y, new_k, new_v)
    new_shape = (tok,) + k_cache.shape[1:]
    return y, new_k.reshape(new_shape), new_v.reshape(new_shape)


def solution(mesh):
    row_spec = P(("dp", "cp"), None)
    cache_spec = P(("dp", "cp"), "tp", None)
    body = functools.partial(local_step, mesh.shape["cp"], mesh.shape["tp"])
    return jax.shard_map(body, mesh=mesh, in_specs=(row_spec, cache_spec, cache_spec, row_spec, P(None), P(None, "tp"), P("tp"), P("tp", None)), out_specs=(row_spec, cache_spec, cache_spec), check_vma=False)
```

```python
import functools
import math

import jax
import jax.numpy as jnp
from jax import lax
from jax.experimental import pallas as pl
from jax.experimental.pallas import tpu as pltpu
from jax.sharding import PartitionSpec as P

EPS = 1.5625e-07
MASK_VALUE = -1e30
LANES = 128
SUB = 256
NC = 512
PHASE_TOKENS = 128
CHUNKS = 4
COLS = 512
OUT_SLOTS = 6
MESH = pl.DeviceIdType.MESH
F32 = jnp.float32
BF16 = jnp.bfloat16
DMA = pltpu.SemaphoreType.DMA
scope = jax.named_scope


def dot(a, b, dims=(((1,), (0,)), ((), ()))):
    return lax.dot_general(a, b, dims, preferred_element_type=F32)


def block_kernel(dims, x_ref, kc_ref, vc_ref, table_ref, g_ref, wq_ref, b_ref, wo_ref,
                 y_ref, kn_ref, vn_ref, ring_ref, ringn_ref,
                 k_buf, v_buf, stage, kvn, qt_ref, hid_ref, x_buf, w_buf, cos_ref, sin_ref, kn_buf, vn_buf,
                 s_ref, p_ref, acc_ref, m_ref, l_ref, mc_ref, al_ref, bias_ref,
                 o_buf, res_buf, full_buf, mine_buf, near_buf, send_buf, comb_buf, got_buf, y_buf,
                 in_sem, w_sem, out_sem, fetch_sem, own_send, pair_send, hop_send, new_send, recv, new_recv,
                 part_send, part_recv, y_send, y_recv, y_last, y_sem):
    n, ranks, groups, heads = dims
    me = lax.axis_index("cp")
    rank = lax.axis_index("tp")
    pair = me + 1 - 2 * lax.rem(me, 2)
    right, left, far = lax.rem(me + 2, n), lax.rem(me + n - 2, n), lax.rem(me + 4, n)
    tok, width = x_ref.shape
    part = stage.shape[3]
    span = CHUNKS * part + tok
    phases = tok // PHASE_TOKENS
    heads_per_tile = NC // PHASE_TOKENS
    tiles = heads // heads_per_tile
    per_group = phases * tiles
    count = groups * per_group
    spare = count
    half = kc_ref.shape[0] // 2
    scale = LANES ** -0.5 * math.log2(math.e)
    head_count = groups * (heads + 2)
    w_blocks = head_count * LANES // COLS
    heads_per_block = COLS // LANES
    pieces = width // COLS
    w_slots = w_buf.shape[0] // width
    out_depth = wo_ref.shape[0]
    rows = PHASE_TOKENS // ranks

    def remote(src, dst, send, got, axis, where):
        return pltpu.make_async_remote_copy(src_ref=src, dst_ref=dst, send_sem=send, recv_sem=got, device_id={axis: where}, device_id_type=MESH)

    def own_pair(c):
        return remote(stage.at[c], ring_ref.at[1, c], own_send.at[0], recv.at[1, c], "cp", pair)

    def own_right(c):
        return remote(stage.at[c], ring_ref.at[2 + c, 0], own_send.at[1], recv.at[2 + c, 0], "cp", right)

    def own_left(c):
        return remote(stage.at[c], ring_ref.at[2 + c, 1], own_send.at[2], recv.at[2 + c, 1], "cp", left)

    def to_pair(s, side):
        return remote(ring_ref.at[s, side], ring_ref.at[s, 2 + side], pair_send, recv.at[s, 2 + side], "cp", pair)

    def from_side(s, side):
        return remote(stage.at[0], ring_ref.at[s, side], own_send.at[0], recv.at[s, side], "cp", pair)

    def hop_right(s):
        return remote(ring_ref.at[s, 0], ring_ref.at[s + 4, 0], hop_send.at[s], recv.at[s + 4, 0], "cp", right)

    def hop_left(s):
        return remote(ring_ref.at[s, 1], ring_ref.at[s + 2, 1], hop_send.at[s], recv.at[s + 2, 1], "cp", left)

    def new_copy(source, send, got, where, own=False):
        src = kvn if own else ringn_ref.at[source]
        return remote(src, ringn_ref.at[source], new_send.at[send], new_recv.at[got], "cp", where)

    new_right = new_copy(me, 0, 0, right, own=True)
    new_left = new_copy(me, 1, 1, left, own=True)
    new_pair = new_copy(me, 2, 3, pair, own=True)
    new_hop = new_copy(left, 3, 2, right)
    new_left_pair = new_copy(left, 4, 4, pair)
    new_right_pair = new_copy(right, 5, 5, pair)
    new_far_pair = new_copy(far, 6, 6, pair)

    def pass_on(s):
        for side in range(2):
            from_side(s, side).wait_recv()
            to_pair(s, side).start()

    def cache_in(i):
        here = pl.ds(i * half, half)
        return (pltpu.make_async_copy(kc_ref.at[here], k_buf.at[i, pl.ds(0, half)], in_sem.at[0, i]),
                pltpu.make_async_copy(vc_ref.at[here], v_buf.at[i, pl.ds(0, half)], in_sem.at[1, i]))

    x_in = pltpu.make_async_copy(x_ref, x_buf, in_sem.at[2, 0])

    def res_in(p):
        here = pl.ds(pl.multiple_of(p * PHASE_TOKENS + rank * rows, rows), rows)
        return pltpu.make_async_copy(x_ref.at[here], res_buf.at[p], in_sem.at[2 + p, 1])

    def w_in(j, slot):
        cols = pl.ds(pl.multiple_of(j * COLS, COLS), COLS)
        here = pl.ds(pl.multiple_of(slot * width, width), width)
        return pltpu.make_async_copy(wq_ref.at[:, cols], w_buf.at[here], w_sem.at[slot])

    def order(j):
        return lax.rem(j + heads * LANES // COLS, w_blocks)

    def wo_at(slot):
        return pl.ds(pl.multiple_of(slot * out_depth, out_depth), out_depth)

    def wo_in(k):
        slot = lax.rem(k, OUT_SLOTS)
        cols = pl.ds(pl.multiple_of(k * COLS, COLS), COLS)
        return pltpu.make_async_copy(wo_ref.at[:, cols], w_buf.at[wo_at(slot)], w_sem.at[slot])

    x_in.start()
    w_in(order(0), 0).start()
    for i in range(2):
        for copy in cache_in(i):
            copy.start()
    for j in range(1, w_slots):
        w_in(order(j), j).start()
    for p in range(phases):
        res_in(p).start()

    barrier = pltpu.get_barrier_semaphore()
    for other in (pair, right, left):
        pl.semaphore_signal(barrier, inc=1, device_id={"cp": other}, device_id_type=MESH)
    for d in range(1, ranks):
        pl.semaphore_signal(barrier, inc=1, device_id={"tp": lax.rem(rank + d, ranks)}, device_id_type=MESH)

    row = lax.broadcasted_iota(jnp.int32, (tok, NC), 0)
    col = lax.rem(lax.broadcasted_iota(jnp.int32, (tok, NC), 1), PHASE_TOKENS)
    bias_ref[0] = jnp.zeros((tok, NC), F32)
    for p in range(phases):
        bias_ref[1 + p] = jnp.where(row <= col + p * PHASE_TOKENS, 0.0, MASK_VALUE)
    bias_ref[1 + phases] = jnp.full((tok, NC), MASK_VALUE, F32)

    m_ref[...] = jnp.full(m_ref.shape, MASK_VALUE, F32)
    l_ref[...] = jnp.zeros(l_ref.shape, F32)
    acc_ref[...] = jnp.zeros(acc_ref.shape, F32)
    mc_ref[...] = jnp.zeros(mc_ref.shape, F32)
    al_ref[...] = jnp.ones(al_ref.shape, F32)

    with scope("wait_x"):
        x_in.wait()
    gain = g_ref[...].astype(F32).reshape(1, width)

    def norm(i, _):
        here = pl.ds(pl.multiple_of(i * 32, 32), 32)
        x = x_buf[here, :].astype(F32)
        inv_rms = lax.rsqrt(jnp.mean(x * x, axis=-1, keepdims=True) + EPS)
        hid_ref[here, :] = (x * inv_rms * gain).astype(BF16)
        return 0

    with scope("norm"):
        lax.fori_loop(0, tok // 32, norm, 0)
    lane = lax.broadcasted_iota(jnp.int32, (tok, LANES), 1)
    rope_lanes = table_ref.shape[0]
    table = jnp.concatenate([table_ref[...].T, jnp.zeros((tok, LANES - rope_lanes), F32)], axis=1)
    at = jnp.where(lane < rope_lanes, lane // 2, 0)
    sin = jnp.take_along_axis(table, at + rope_lanes // 2, axis=1)
    cos_ref[...] = jnp.take_along_axis(table, at, axis=1)
    sin_ref[...] = jnp.where(lane % 2 == 0, -sin, sin)

    def rotate(head):
        swapped = jnp.where(lane % 2 == 0, pltpu.roll(head, LANES - 1, 1), pltpu.roll(head, 1, 1))
        turned = head * cos_ref[...] + swapped * sin_ref[...]
        return jnp.where(lane < rope_lanes, turned, head)

    pair_left, pair_right, pair_far = lax.rem(pair + n - 2, n), lax.rem(pair + 2, n), lax.rem(pair + 4, n)

    def block_of(s):
        out = me
        for i, source in enumerate((pair, left, right, pair_left, pair_right, far, pair_far)):
            out = jnp.where(s == i + 1, source, out)
        return out

    def fetch_cache(s, g, act):
        for kind, buf in ((0, k_buf), (1, v_buf)):
            for c in range(CHUNKS):
                here = pl.ds(c * part, part)
                getattr(pltpu.make_async_copy(ring_ref.at[s, c, g, kind], buf.at[g, here], fetch_sem.at[g, kind, c]), act)()

    def fetch_block(s, g, act):
        for kind, buf in ((0, k_buf), (1, v_buf)):
            here = pl.ds(CHUNKS * part, tok)
            getattr(pltpu.make_async_copy(ringn_ref.at[block_of(s), g, kind], buf.at[g, here], fetch_sem.at[g, kind, CHUNKS]), act)()

    def fetch(s, g, act):
        fetch_cache(s, g, act)
        fetch_block(s, g, act)

    def a_rows(j):
        return pl.ds(pl.multiple_of(j * tok, tok), tok)

    def queries(j, i):
        head = j * heads_per_block + i
        g, h = head // (heads + 2), lax.rem(head, heads + 2)
        turned = rotate(s_ref[a_rows(j), i * LANES:(i + 1) * LANES]).T.astype(BF16)
        for p in range(phases):
            tile = jnp.where(h < heads, g * per_group + p * tiles + h // heads_per_tile, spare)
            at = pl.multiple_of(lax.rem(h, heads_per_tile) * PHASE_TOKENS, PHASE_TOKENS)
            qt_ref[tile, :, pl.ds(at, PHASE_TOKENS)] = turned[:, p * PHASE_TOKENS:(p + 1) * PHASE_TOKENS]

    def project(j, _):
        slot = lax.rem(j, w_slots)
        block = order(j)
        w_in(block, slot).wait()
        here = pl.ds(pl.multiple_of(slot * width, width), width)
        cols = pl.ds(pl.multiple_of(block * COLS, COLS), COLS)
        before = order(jnp.maximum(j - 1, 0))
        for i in range(heads_per_block):
            queries(before, i)
        s_ref[a_rows(block), :] = dot(hid_ref[...], w_buf[here, :]) + b_ref[cols].astype(F32).reshape(1, COLS)

        @pl.when(j + w_slots < w_blocks)
        def _():
            w_in(order(j + w_slots), slot).start()
        return 0

    early = ((groups - 1) * (heads + 2) + heads) * LANES // COLS - heads * LANES // COLS + 1
    with scope("project"):
        lax.fori_loop(0, 2, project, 0)

    pair_rows = groups * LANES
    wide = lax.broadcasted_iota(jnp.int32, (pair_rows, pair_rows), 0)
    tall = lax.broadcasted_iota(jnp.int32, (pair_rows, pair_rows), 1)
    pick = (wide // groups + (wide % groups) * LANES == tall).astype(BF16)
    pick_t = (tall // groups + (tall % groups) * LANES == wide).astype(BF16)
    blocks = part // LANES

    def stage_out(c):
        return pltpu.make_async_copy(stage.at[c], ring_ref.at[0, c], out_sem.at[c])

    for c in range(CHUNKS):
        if c % (CHUNKS // 2) == 0:
            for copy in cache_in(c // (CHUNKS // 2)):
                copy.wait()

        def relayout(i, _):
            i_half = c // (CHUNKS // 2)
            src = pl.ds(pl.multiple_of((c % (CHUNKS // 2)) * part * groups + i * pair_rows, pair_rows), pair_rows)
            here = pl.ds(pl.multiple_of(i * LANES, LANES), LANES)
            keys = dot(pick_t, k_buf[i_half, src, :]).astype(BF16)
            vals = dot(v_buf[i_half, src, :], pick, (((0,), (0,)), ((), ()))).astype(BF16)
            for g in range(groups):
                stage[c, g, 0, here, :] = keys[g * LANES:(g + 1) * LANES, :]
                stage[c, g, 1, here, :] = vals[:, g * LANES:(g + 1) * LANES]
            return 0

        with scope("relayout"):
            lax.fori_loop(0, blocks, relayout, 0, unroll=4)
        stage_out(c).start()

    def send_own(chunks):
        for c in chunks:
            own_right(c).start()
            own_left(c).start()
            own_pair(c).start()

    with scope("barrier"):
        pl.semaphore_wait(barrier, 3 + ranks - 1)
    send_own(range(1))

    with scope("project"):
        lax.fori_loop(2, early, project, 0)
    for c in range(CHUNKS):
        stage_out(c).wait()
    fetch_cache(0, 0, "start")

    kn_out = pltpu.make_async_copy(kn_buf, kn_ref, out_sem.at[CHUNKS])
    vn_out = pltpu.make_async_copy(vn_buf, vn_ref, out_sem.at[CHUNKS + 1])
    fresh = []
    kvn_out = pltpu.make_async_copy(kvn, ringn_ref.at[me], out_sem.at[CHUNKS + 2])
    for g in range(groups):
        at = (g * (heads + 2) + heads) * LANES
        keys = rotate(s_ref[a_rows(at // COLS), at % COLS:at % COLS + LANES])
        at += LANES
        vals = s_ref[a_rows(at // COLS), at % COLS:at % COLS + LANES]
        fresh.append((keys.astype(BF16), vals.astype(BF16)))
        kvn[g, 0] = keys.astype(BF16)
        for i in range(tok // LANES):
            here = slice(i * LANES, (i + 1) * LANES)
            kvn[g, 1, here, :] = vals[here, :].T.astype(BF16)
    for i in range(tok // LANES):
        here = slice(i * LANES, (i + 1) * LANES)
        for kind, buf in ((0, kn_buf), (1, vn_buf)):
            block = jnp.concatenate([fresh[g][kind][here, :] for g in range(groups)], axis=0)
            buf[i * pair_rows:(i + 1) * pair_rows, :] = dot(pick, block).astype(BF16)
    kvn_out.start()
    for copy in (new_right, new_left, new_pair):
        copy.start()
    send_own(range(1, CHUNKS))
    kn_out.start()
    vn_out.start()
    with scope("project"):
        lax.fori_loop(early, w_blocks, project, 0)
    for i in range(heads_per_block):
        queries(order(w_blocks - 1), i)
    kvn_out.wait()
    fetch_block(0, 0, "start")
    for k in range(OUT_SLOTS):
        wo_in(k).start()

    def step(a=None, b=None, c=None):
        alpha_b, alpha_c = al_ref[0], al_ref[1]
        shift = mc_ref[...]
        run = {"max": None, "sum": None, "out": None}

        def scores(i):
            keys = k_buf[a["slot"], i * SUB:(i + 1) * SUB, :]
            s = dot(keys, qt_ref[a["tile"]])
            if i == (span - tok) // SUB:
                edge = 1 + lax.rem(a["tile"], per_group) // tiles
                which = jnp.where(a["block"] < me, 0, jnp.where(a["block"] == me, edge, 1 + phases))
                s = s + bias_ref[which]
            s_ref[i * SUB:(i + 1) * SUB, :] = s
            top = jnp.max(s.reshape(SUB // 8, 8, NC), axis=0)
            run["max"] = top if run["max"] is None else jnp.maximum(run["max"], top)

        def weights(i):
            s = s_ref[i * SUB:(i + 1) * SUB, :]
            e = jnp.exp2((s * scale).reshape(SUB // 8, 8, NC) - shift[None])
            part_sum = jnp.sum(e, axis=0)
            run["sum"] = part_sum if run["sum"] is None else run["sum"] + part_sum
            p_ref[i * SUB:(i + 1) * SUB, :] = e.reshape(SUB, NC).astype(BF16)

        def values(i):
            at = i * SUB
            block = jnp.concatenate([v_buf[c["slot"], at + h * LANES:at + (h + 1) * LANES, :] for h in range(SUB // LANES)], axis=1)
            out = dot(block, p_ref[i * SUB:(i + 1) * SUB, :])
            run["out"] = out if run["out"] is None else run["out"] + out

        stages = ((c, values), (b, weights), (a, scores))
        for i in range(span // SUB):
            for spec, stage_fn in stages:
                if spec is not None:
                    stage_fn(i)
        if c is not None:
            acc_ref[c["tile"]] = acc_ref[c["tile"]] * alpha_c + run["out"]
        if b is not None:
            l_ref[b["tile"]] = l_ref[b["tile"]] * alpha_b + run["sum"]
            al_ref[1] = alpha_b
        if a is not None:
            old = m_ref[a["tile"]]
            new = jnp.maximum(old, jnp.max(run["max"], axis=0, keepdims=True))
            m_ref[a["tile"]] = new
            mc_ref[...] = jnp.broadcast_to(new * scale, mc_ref.shape)
            al_ref[0] = jnp.exp2((old - new) * scale)

    def main(tile, slot, block=None):
        return {"tile": tile, "slot": slot, "block": block}

    def run_unit(s, g, first, tile_count, carry, fetch_next):
        with scope("wait_fetch"):
            fetch(s, g, "wait")
        block = block_of(s)

        def one_tile(t, carry):
            with scope("fetch_next"):
                pl.when(t == tile_count - 1)(fetch_next)
            last, last_slot, older, older_slot = carry
            tile = g * per_group + first + t
            with scope("tile"):
                step(main(tile, g, block), main(last, last_slot), main(older, older_slot))
            return tile, jnp.int32(g), last, last_slot

        return lax.fori_loop(0, tile_count, one_tile, carry)

    start = tuple(jnp.int32(v) for v in (spare, 0, spare, 0))

    def got_new(i):
        new_copy(pair, 0, i, pair).wait_recv()

    def one_set(s, carry):
        nxt = s + 1
        carry = run_unit(s, 0, 0, per_group, carry, lambda: fetch(s, 1, "start"))
        with scope("pass_on"):
            pl.when(s >= 1)(lambda: pass_on(nxt))

        @pl.when(s == 2)
        def _():
            for copy in (new_hop, new_left_pair, new_right_pair):
                copy.start()

        pl.when((s >= 1) & (s <= 2))(lambda: hop_right(nxt).start())
        pl.when((s >= 3) & (s <= 4))(lambda: hop_left(nxt).start())

        @pl.when(s == n - 3)
        def _():
            got_new(2)
            new_far_pair.start()

        def fetch_next():
            @pl.when(s == 0)
            def _():
                for c in range(CHUNKS):
                    own_pair(c).wait_recv()
                got_new(3)

            @pl.when(s >= 1)
            def _():
                for side in range(2):
                    to_pair(nxt, side).wait_recv()

            @pl.when(s == 1)
            def _():
                got_new(0)
                got_new(1)

            pl.when(s == 3)(lambda: got_new(4))
            pl.when(s == 4)(lambda: got_new(5))
            fetch(nxt, 0, "start")

        return run_unit(s, 1, 0, per_group, carry, fetch_next)

    carry = lax.fori_loop(0, n - 2, one_set, start)
    kn_out.wait()
    vn_out.wait()

    right_rank, left_rank, far_rank = lax.rem(rank + 1, ranks), lax.rem(rank + ranks - 1, ranks), lax.rem(rank + 2, ranks)

    def onward(k):
        return jnp.where(lax.rem(k, 2) == 0, right_rank, left_rank)

    def back(k):
        return jnp.where(lax.rem(k, 2) == 0, left_rank, right_rank)

    def band(of):
        return pl.ds(pl.multiple_of(of * rows, rows), rows)

    def far_copy(p, k):
        return remote(send_buf.at[k, band(far_rank)], got_buf.at[p, 0, k], part_send.at[p, 0], part_recv.at[p, 0, k], "tp", onward(k))

    def near_copy(p, k):
        return remote(send_buf.at[k, band(back(k))], got_buf.at[p, 1, k], part_send.at[p, 1], part_recv.at[p, 1, k], "tp", back(k))

    def comb_copy(p, k):
        return remote(comb_buf.at[p, k], got_buf.at[p, 2, k], part_send.at[p, 2], part_recv.at[p, 1, k], "tp", onward(k))

    def piece_cols(k):
        return pl.ds(pl.multiple_of(k * COLS, COLS), COLS)

    def y_rows(p, of):
        return pl.ds(pl.multiple_of(p * PHASE_TOKENS + of * rows, rows), rows)

    def y_copy(p, k, way):
        dst = y_ref.at[y_rows(p, rank), piece_cols(k)]
        got = y_last.at[p, 0] if way else y_recv.at[p, k]
        return remote(y_buf.at[p, k], dst, y_send.at[p, way], got, "tp", back(k) if way else onward(k))

    def y_forward(p, k):
        here = y_ref.at[y_rows(p, back(k)), piece_cols(k)]
        return remote(here, here, y_send.at[p, 2], y_last.at[p, 1], "tp", onward(k))

    def y_own(p, k):
        return pltpu.make_async_copy(y_buf.at[p, k], y_ref.at[y_rows(p, rank), piece_cols(k)], y_sem.at[p])

    def each_piece(body, extra=0):
        def piece(k, _):
            body(k)
            return 0
        lax.fori_loop(0, pieces + extra, piece, 0)

    def part_sent(p, kind):
        every = got_buf.at[p, kind]
        remote(every, every, part_send.at[p, kind], part_recv.at[p, 0, 0], "tp", rank).wait_send()

    def project_out(p):
        if p > 0:
            for kind in range(2):
                part_sent(p - 1, kind)

        def piece(k):
            @pl.when(k < pieces)
            def _():
                wo_in(k).wait()
                out = dot(o_buf[...], w_buf[wo_at(lax.rem(k, OUT_SLOTS)), :])
                full_buf[...] = out
                send_buf[k] = out.astype(BF16)
                mine_buf[k] = full_buf[band(rank), :]
                near_buf[k] = full_buf[band(onward(k)), :]
                pl.when(k + OUT_SLOTS < pieces)(lambda: wo_in(k + OUT_SLOTS).start())

            @pl.when(k >= 1)
            def _():
                far_copy(p, k - 1).start()
                near_copy(p, k - 1).start()

        each_piece(piece, 1)

    def combine(p):
        def piece(k):
            @pl.when(k < pieces)
            def _():
                far_copy(p, k).wait_recv()
                comb_buf[p, k] = (near_buf[k] + got_buf[p, 0, k].astype(F32)).astype(BF16)

            pl.when(k >= 1)(lambda: comb_copy(p, k - 1).start())

        each_piece(piece, 1)

    def reduce(p):
        def piece(k):
            @pl.when(k < pieces)
            def _():
                both = got_buf.at[p, pl.ds(1, 2), k]
                remote(both, both, part_send.at[p, 1], part_recv.at[p, 1, k], "tp", rank).wait_recv()
                total = mine_buf[k] + got_buf[p, 1, k].astype(F32) + got_buf[p, 2, k].astype(F32)
                y_buf[p, k] = (res_buf[p, :, piece_cols(k)].astype(F32) + total).astype(BF16)

            @pl.when(k >= 1)
            def _():
                y_copy(p, k - 1, 0).start()
                y_copy(p, k - 1, 1).start()
                y_own(p, k - 1).start()

        each_piece(piece, 1)

    def forward(p):
        def piece(k):
            y_copy(p, k, 0).wait_recv()
            y_forward(p, k).start()
        each_piece(piece)

    def finish(p, g):
        def tile(h, _):
            t = g * per_group + p * tiles + h
            total = jnp.sum(l_ref[t], axis=0, keepdims=True)
            out = (acc_ref[t] / total).T.astype(BF16)
            for i in range(heads_per_tile):
                at = pl.multiple_of((g * heads + h * heads_per_tile + i) * LANES, LANES)
                o_buf[:, pl.ds(at, LANES)] = out[i * PHASE_TOKENS:(i + 1) * PHASE_TOKENS, :]
            return 0

        lax.fori_loop(0, tiles, tile, 0)

    for p in range(phases):
        res_in(p).wait()

    def late(p, carry):
        first = p * tiles

        def between(s, g):
            if p == 0 and g == 0:
                pl.when(s == n - 2)(lambda: pass_on(n - 1))
            if p > 0:
                @pl.when(s == n - 2)
                def _():
                    if g == 0:
                        with scope("project_out"):
                            for other in range(groups):
                                finish(p - 1, other)
                            project_out(p - 1)
                        for k in range(OUT_SLOTS):
                            wo_in(k).start()
                    else:
                        with scope("combine"):
                            combine(p - 1)

                @pl.when(s == n - 1)
                def _():
                    with scope("reduce"):
                        reduce(p - 1) if g == 0 else forward(p - 1)

        def late_set(s, carry):
            carry = run_unit(s, 0, first, tiles, carry, lambda: fetch(s, 1, "start"))
            between(s, 0)

            def fetch_next():
                @pl.when(s == n - 2)
                def _():
                    if p == 0:
                        for side in range(2):
                            to_pair(n - 1, side).wait_recv()
                        got_new(6)
                    fetch(n - 1, 0, "start")
                if p < phases - 1:
                    pl.when(s == n - 1)(lambda: fetch(n - 2, 0, "start"))

            carry = run_unit(s, 1, first, tiles, carry, fetch_next)
            between(s, 1)
            return carry

        return lax.fori_loop(n - 2, n, late_set, carry)

    for p in range(phases):
        carry = late(p, carry)
    last, last_slot, older, older_slot = carry
    with scope("finish"):
        step(None, main(last, last_slot), main(older, older_slot))
        step(None, None, main(last, last_slot))
        for g in range(groups):
            finish(phases - 1, g)
    with scope("project_out"):
        project_out(phases - 1)
    with scope("combine"):
        combine(phases - 1)
    with scope("reduce"):
        reduce(phases - 1)
    with scope("forward"):
        forward(phases - 1)

    for way in range(3):
        remote(stage, stage, own_send.at[way], recv.at[0, 0], "cp", me).wait_send()
    passed = ring_ref.at[pl.ds(2, n - 2), pl.ds(0, 2)]
    remote(passed, passed, pair_send, recv.at[0, 0], "cp", me).wait_send()
    for s in (2, 3):
        hop_right(s).wait_send()
    for s in (4, 5):
        hop_left(s).wait_send()
    for copy in (new_right, new_left, new_pair, new_hop, new_left_pair, new_right_pair, new_far_pair):
        copy.wait_send()

    with scope("drain_out"):
        part_sent(phases - 1, 0)
        part_sent(phases - 1, 1)
        for p in range(phases):
            part_sent(p, 2)
            every = y_buf.at[p]
            pltpu.make_async_copy(every, every, y_sem.at[p]).wait()
            for way in range(3):
                remote(every, every, y_send.at[p, way], y_last.at[p, 0], "tp", rank).wait_send()
            for way in range(2):
                remote(every, every, y_send.at[p, way], y_last.at[p, way], "tp", rank).wait_recv()


def results_kernel(y_in, kn_in, vn_in, y_out, kn_out, vn_out, y_buf, kn_buf, vn_buf, sem):
    rows = y_buf.shape[0] // 4
    copies = []
    for i in range(4):
        here = slice(i * rows, (i + 1) * rows)
        copies.append((y_in.at[here], y_buf.at[here], y_out.at[here]))
    copies += [(kn_in, kn_buf, kn_out), (vn_in, vn_buf, vn_out)]
    for i, (src, buf, _) in enumerate(copies):
        pltpu.make_async_copy(src, buf, sem.at[0, i]).start()
    for i, (src, buf, dst) in enumerate(copies):
        pltpu.make_async_copy(src, buf, sem.at[0, i]).wait()
        pltpu.make_async_copy(buf, dst, sem.at[1, i]).start()
    for i, (_, buf, dst) in enumerate(copies):
        pltpu.make_async_copy(buf, dst, sem.at[1, i]).wait()


def results(*arrays):
    any_spec = pl.BlockSpec(memory_space=pl.ANY)
    return pl.pallas_call(
        results_kernel,
        in_specs=[any_spec] * 3,
        out_specs=[any_spec] * 3,
        out_shape=[jax.ShapeDtypeStruct(a.shape, a.dtype) for a in arrays],
        scratch_shapes=[pltpu.VMEM(a.shape, a.dtype) for a in arrays] + [DMA((2, 6))],
        compiler_params=pltpu.CompilerParams(vmem_limit_bytes=62 << 20),
        name="results",
    )(*arrays)


def local_step(n, ranks, x, k_cache, v_cache, rope_table, norm_gain, w_qkv, b_qkv, w_out):
    positions, groups, head_dim = k_cache.shape
    tok, width = x.shape
    heads = w_qkv.shape[1] // groups // head_dim - 2
    part = positions // CHUNKS
    span = positions + tok
    phases = tok // PHASE_TOKENS
    tiles = heads * PHASE_TOKENS // NC
    count = groups * phases * tiles
    pieces = width // COLS
    rows = PHASE_TOKENS // ranks
    depth = w_out.shape[0]
    any_spec = pl.BlockSpec(memory_space=pl.ANY)
    vmem_spec = pl.BlockSpec(memory_space=pltpu.VMEM)
    flat = (positions * groups, head_dim)
    flops = 4 * count * NC * LANES * n * (span + tok)
    y, new_k, new_v, _, _ = pl.pallas_call(
        functools.partial(block_kernel, (n, ranks, groups, heads)),
        in_specs=[any_spec, any_spec, any_spec, vmem_spec, vmem_spec, any_spec, vmem_spec, any_spec],
        out_specs=[any_spec] * 5,
        out_shape=[
            jax.ShapeDtypeStruct((tok, width), BF16),
            jax.ShapeDtypeStruct((tok * groups, head_dim), BF16),
            jax.ShapeDtypeStruct((tok * groups, head_dim), BF16),
            jax.ShapeDtypeStruct((n, CHUNKS, groups, 2, part, head_dim), BF16),
            jax.ShapeDtypeStruct((n, groups, 2, tok, head_dim), BF16),
        ],
        scratch_shapes=[
            pltpu.VMEM((2, span, LANES), BF16),
            pltpu.VMEM((2, span, LANES), BF16),
            pltpu.VMEM((CHUNKS, groups, 2, part, LANES), BF16),
            pltpu.VMEM((groups, 2, tok, LANES), BF16),
            pltpu.VMEM((count + 1, LANES, NC), BF16),
            pltpu.VMEM((tok, width), BF16),
            pltpu.VMEM((tok, width), BF16),
            pltpu.VMEM((max(3 * width, OUT_SLOTS * depth), COLS), BF16),
            pltpu.VMEM((tok, LANES), F32),
            pltpu.VMEM((tok, LANES), F32),
            pltpu.VMEM((tok * groups, LANES), BF16),
            pltpu.VMEM((tok * groups, LANES), BF16),
            pltpu.VMEM((max(span, w_qkv.shape[1] // COLS * tok), NC), F32),
            pltpu.VMEM((span, NC), BF16),
            pltpu.VMEM((count + 1, LANES, NC), F32),
            pltpu.VMEM((count, 1, NC), F32),
            pltpu.VMEM((count + 1, 8, NC), F32),
            pltpu.VMEM((8, NC), F32),
            pltpu.VMEM((2, 1, NC), F32),
            pltpu.VMEM((2 + phases, tok, NC), F32),
            pltpu.VMEM((PHASE_TOKENS, groups * heads * LANES), BF16),
            pltpu.VMEM((phases, rows, width), BF16),
            pltpu.VMEM((PHASE_TOKENS, COLS), F32),
            pltpu.VMEM((pieces, rows, COLS), F32),
            pltpu.VMEM((pieces, rows, COLS), F32),
            pltpu.VMEM((pieces, PHASE_TOKENS, COLS), BF16),
            pltpu.VMEM((phases, pieces, rows, COLS), BF16),
            pltpu.VMEM((phases, 3, pieces, rows, COLS), BF16),
            pltpu.VMEM((phases, pieces, rows, COLS), BF16),
            DMA((2 + phases, 2)),
            DMA((OUT_SLOTS,)),
            DMA((CHUNKS + 3,)),
            DMA((groups, 2, CHUNKS + 1)),
            DMA((3,)),
            DMA,
            DMA((n,)),
            DMA((7,)),
            DMA((n, CHUNKS)),
            DMA((7,)),
            DMA((phases, 3)),
            DMA((phases, 2, pieces)),
            DMA((phases, 3)),
            DMA((phases, pieces)),
            DMA((phases, 2)),
            DMA((phases,)),
        ],
        cost_estimate=pl.CostEstimate(flops=flops, bytes_accessed=4 * positions * n * groups * head_dim, transcendentals=flops // (4 * LANES)),
        compiler_params=pltpu.CompilerParams(collective_id=0, has_side_effects=True, vmem_limit_bytes=63 << 20),
        name="block",
    )(x, k_cache.reshape(flat), v_cache.reshape(flat), rope_table.T, norm_gain, w_qkv, b_qkv, w_out)
    y, new_k, new_v = results(y, new_k, new_v)
    new_shape = (tok,) + k_cache.shape[1:]
    return y, new_k.reshape(new_shape), new_v.reshape(new_shape)


def solution(mesh):
    row_spec = P(("dp", "cp"), None)
    cache_spec = P(("dp", "cp"), "tp", None)
    body = functools.partial(local_step, mesh.shape["cp"], mesh.shape["tp"])
    return jax.shard_map(body, mesh=mesh, in_specs=(row_spec, cache_spec, cache_spec, row_spec, P(None), P(None, "tp"), P("tp"), P("tp", None)), out_specs=(row_spec, cache_spec, cache_spec), check_vma=False)
```

```python
import functools
import math

import jax
import jax.numpy as jnp
from jax import lax
from jax.experimental import pallas as pl
from jax.experimental.pallas import tpu as pltpu
from jax.sharding import PartitionSpec as P

EPS = 1.5625e-07
MASK_VALUE = -1e30
LANES = 128
SUB = 256
NC = 512
PHASE_TOKENS = 128
CHUNKS = 4
COLS = 512
OUT_SLOTS = 7
MESH = pl.DeviceIdType.MESH
F32 = jnp.float32
BF16 = jnp.bfloat16
DMA = pltpu.SemaphoreType.DMA
scope = jax.named_scope


def dot(a, b, dims=(((1,), (0,)), ((), ()))):
    return lax.dot_general(a, b, dims, preferred_element_type=F32)


def block_kernel(dims, x_ref, kc_ref, vc_ref, table_ref, g_ref, wq_ref, b_ref, wo_ref,
                 y_ref, kn_ref, vn_ref, ring_ref, ringn_ref,
                 k_buf, v_buf, stage, kvn, qt_ref, hid_ref, x_buf, w_buf, cos_ref, sin_ref, kn_buf, vn_buf,
                 s_ref, p_ref, acc_ref, m_ref, l_ref, mc_ref, al_ref, bias_ref,
                 o_buf, full_buf, mine_buf, near_buf, send_buf, comb_buf, got_buf, y_buf,
                 in_sem, w_sem, out_sem, fetch_sem, own_send, pair_send, hop_send, new_send, recv, new_recv,
                 part_send, part_recv, y_send, y_recv, y_last, y_sem):
    n, ranks, groups, heads = dims
    me = lax.axis_index("cp")
    rank = lax.axis_index("tp")
    pair = me + 1 - 2 * lax.rem(me, 2)
    right, left, far = lax.rem(me + 2, n), lax.rem(me + n - 2, n), lax.rem(me + 4, n)
    tok, width = x_ref.shape
    part = stage.shape[3]
    span = CHUNKS * part + tok
    phases = tok // PHASE_TOKENS
    heads_per_tile = NC // PHASE_TOKENS
    tiles = heads // heads_per_tile
    per_group = phases * tiles
    count = groups * per_group
    spare = count
    half = kc_ref.shape[0] // 2
    scale = LANES ** -0.5 * math.log2(math.e)
    head_count = groups * (heads + 2)
    w_blocks = head_count * LANES // COLS
    heads_per_block = COLS // LANES
    pieces = width // COLS
    w_slots = w_buf.shape[0] // width
    out_depth = wo_ref.shape[0]
    rows = PHASE_TOKENS // ranks

    def remote(src, dst, send, got, axis, where):
        return pltpu.make_async_remote_copy(src_ref=src, dst_ref=dst, send_sem=send, recv_sem=got, device_id={axis: where}, device_id_type=MESH)

    def own_pair(c):
        return remote(stage.at[c], ring_ref.at[1, c], own_send.at[0], recv.at[1, c], "cp", pair)

    def own_right(c):
        return remote(stage.at[c], ring_ref.at[2 + c, 0], own_send.at[1], recv.at[2 + c, 0], "cp", right)

    def own_left(c):
        return remote(stage.at[c], ring_ref.at[2 + c, 1], own_send.at[2], recv.at[2 + c, 1], "cp", left)

    def to_pair(s, side):
        return remote(ring_ref.at[s, side], ring_ref.at[s, 2 + side], pair_send, recv.at[s, 2 + side], "cp", pair)

    def from_side(s, side):
        return remote(stage.at[0], ring_ref.at[s, side], own_send.at[0], recv.at[s, side], "cp", pair)

    def hop_right(s):
        return remote(ring_ref.at[s, 0], ring_ref.at[s + 4, 0], hop_send.at[s], recv.at[s + 4, 0], "cp", right)

    def hop_left(s):
        return remote(ring_ref.at[s, 1], ring_ref.at[s + 2, 1], hop_send.at[s], recv.at[s + 2, 1], "cp", left)

    def new_copy(source, send, got, where, own=False):
        src = kvn if own else ringn_ref.at[source]
        return remote(src, ringn_ref.at[source], new_send.at[send], new_recv.at[got], "cp", where)

    new_right = new_copy(me, 0, 0, right, own=True)
    new_left = new_copy(me, 1, 1, left, own=True)
    new_pair = new_copy(me, 2, 3, pair, own=True)
    new_hop = new_copy(left, 3, 2, right)
    new_left_pair = new_copy(left, 4, 4, pair)
    new_right_pair = new_copy(right, 5, 5, pair)
    new_far_pair = new_copy(far, 6, 6, pair)

    def pass_on(s):
        for side in range(2):
            from_side(s, side).wait_recv()
            to_pair(s, side).start()

    def cache_in(i):
        here = pl.ds(i * half, half)
        return (pltpu.make_async_copy(kc_ref.at[here], k_buf.at[i, pl.ds(0, half)], in_sem.at[0, i]),
                pltpu.make_async_copy(vc_ref.at[here], v_buf.at[i, pl.ds(0, half)], in_sem.at[1, i]))

    x_in = pltpu.make_async_copy(x_ref, x_buf, in_sem.at[2, 0])

    def res_in(p, k):
        here = pl.ds(pl.multiple_of(p * PHASE_TOKENS + rank * rows, rows), rows)
        return pltpu.make_async_copy(x_ref.at[here, k * COLS:(k + 1) * COLS], y_buf.at[p, k], in_sem.at[2 + p, 1])

    def w_in(j, slot):
        cols = pl.ds(pl.multiple_of(j * COLS, COLS), COLS)
        here = pl.ds(pl.multiple_of(slot * width, width), width)
        return pltpu.make_async_copy(wq_ref.at[:, cols], w_buf.at[here], w_sem.at[slot])

    def order(j):
        return lax.rem(j + heads * LANES // COLS, w_blocks)

    def wo_at(slot):
        return pl.ds(pl.multiple_of(slot * out_depth, out_depth), out_depth)

    def wo_in(k):
        slot = lax.rem(k, OUT_SLOTS)
        cols = pl.ds(pl.multiple_of(k * COLS, COLS), COLS)
        return pltpu.make_async_copy(wo_ref.at[:, cols], w_buf.at[wo_at(slot)], w_sem.at[slot])

    x_in.start()
    for i in range(2):
        for copy in cache_in(i):
            copy.start()
    w_in(order(0), 0).start()
    for p in range(phases):
        for k in range(pieces):
            res_in(p, k).start()

    barrier = pltpu.get_barrier_semaphore()
    for other in (pair, right, left):
        pl.semaphore_signal(barrier, inc=1, device_id={"cp": other}, device_id_type=MESH)
    for d in range(1, ranks):
        pl.semaphore_signal(barrier, inc=1, device_id={"tp": lax.rem(rank + d, ranks)}, device_id_type=MESH)

    row = lax.broadcasted_iota(jnp.int32, (tok, NC), 0)
    col = lax.rem(lax.broadcasted_iota(jnp.int32, (tok, NC), 1), PHASE_TOKENS)
    bias_ref[0] = jnp.zeros((tok, NC), BF16)
    for p in range(phases):
        bias_ref[1 + p] = jnp.where(row <= col + p * PHASE_TOKENS, 0.0, MASK_VALUE).astype(BF16)
    bias_ref[1 + phases] = jnp.full((tok, NC), MASK_VALUE, BF16)

    m_ref[...] = jnp.full(m_ref.shape, MASK_VALUE, F32)
    l_ref[...] = jnp.zeros(l_ref.shape, F32)
    acc_ref[...] = jnp.zeros(acc_ref.shape, F32)
    mc_ref[...] = jnp.zeros(mc_ref.shape, F32)
    al_ref[...] = jnp.ones(al_ref.shape, F32)

    x_in.wait()
    for j in range(1, w_slots):
        w_in(order(j), j).start()
    gain = g_ref[...].astype(F32).reshape(1, width)
    norm_rows = tok // (CHUNKS * (part // LANES // 4))

    def norm(i):
        here = pl.ds(pl.multiple_of(i * norm_rows, norm_rows), norm_rows)
        x = x_buf[here, :].astype(F32)
        inv_rms = lax.rsqrt(jnp.mean(x * x, axis=-1, keepdims=True) + EPS)
        hid_ref[here, :] = (x * inv_rms * gain).astype(BF16)

    pair_rows = groups * LANES
    wide = lax.broadcasted_iota(jnp.int32, (pair_rows, pair_rows), 0)
    tall = lax.broadcasted_iota(jnp.int32, (pair_rows, pair_rows), 1)
    pick = (wide // groups + (wide % groups) * LANES == tall).astype(BF16)
    pick_t = (tall // groups + (tall % groups) * LANES == wide).astype(BF16)
    blocks = part // LANES

    def stage_out(c):
        return pltpu.make_async_copy(stage.at[c], ring_ref.at[0, c], out_sem.at[c])

    for c in range(CHUNKS):
        if c % (CHUNKS // 2) == 0:
            for copy in cache_in(c // (CHUNKS // 2)):
                copy.wait()

        def relayout(i, _):
            i_half = c // (CHUNKS // 2)
            for sub in range(4):
                at = i * 4 + sub
                src = pl.ds(pl.multiple_of((c % (CHUNKS // 2)) * part * groups + at * pair_rows, pair_rows), pair_rows)
                here = pl.ds(pl.multiple_of(at * LANES, LANES), LANES)
                keys = dot(pick_t, k_buf[i_half, src, :]).astype(BF16)
                vals = dot(v_buf[i_half, src, :], pick, (((0,), (0,)), ((), ()))).astype(BF16)
                for g in range(groups):
                    stage[c, g, 0, here, :] = keys[g * LANES:(g + 1) * LANES, :]
                    stage[c, g, 1, here, :] = vals[:, g * LANES:(g + 1) * LANES]
            norm(c * (blocks // 4) + i)
            return 0

        with scope("relayout"):
            lax.fori_loop(0, blocks // 4, relayout, 0)
        stage_out(c).start()

    def send_own(chunks):
        for c in chunks:
            own_right(c).start()
            own_left(c).start()
            own_pair(c).start()

    with scope("barrier"):
        pl.semaphore_wait(barrier, 3 + ranks - 1)
    send_own(range(1))

    lane = lax.broadcasted_iota(jnp.int32, (tok, LANES), 1)
    rope_lanes = table_ref.shape[0]
    table = jnp.concatenate([table_ref[...].T, jnp.zeros((tok, LANES - rope_lanes), F32)], axis=1)
    at = jnp.where(lane < rope_lanes, lane // 2, 0)
    sin = jnp.take_along_axis(table, at + rope_lanes // 2, axis=1)
    cos_ref[...] = jnp.take_along_axis(table, at, axis=1)
    sin_ref[...] = jnp.where(lane % 2 == 0, -sin, sin)

    def rotate(head):
        swapped = jnp.where(lane % 2 == 0, pltpu.roll(head, LANES - 1, 1), pltpu.roll(head, 1, 1))
        turned = head * cos_ref[...] + swapped * sin_ref[...]
        return jnp.where(lane < rope_lanes, turned, head)

    pair_left, pair_right, pair_far = lax.rem(pair + n - 2, n), lax.rem(pair + 2, n), lax.rem(pair + 4, n)

    def block_of(s):
        out = me
        for i, source in enumerate((pair, left, right, pair_left, pair_right, far, pair_far)):
            out = jnp.where(s == i + 1, source, out)
        return out

    def fetch_cache(s, g, act):
        for kind, buf in ((0, k_buf), (1, v_buf)):
            for c in range(CHUNKS):
                here = pl.ds(c * part, part)
                getattr(pltpu.make_async_copy(ring_ref.at[s, c, g, kind], buf.at[g, here], fetch_sem.at[g, kind, c]), act)()

    def fetch_block(s, g, act):
        for kind, buf in ((0, k_buf), (1, v_buf)):
            here = pl.ds(CHUNKS * part, tok)
            getattr(pltpu.make_async_copy(ringn_ref.at[block_of(s), g, kind], buf.at[g, here], fetch_sem.at[g, kind, CHUNKS]), act)()

    def fetch(s, g, act):
        fetch_cache(s, g, act)
        fetch_block(s, g, act)

    def a_rows(j):
        return pl.ds(pl.multiple_of(j * tok, tok), tok)

    def queries(j, i):
        head = j * heads_per_block + i
        g, h = head // (heads + 2), lax.rem(head, heads + 2)
        turned = rotate(s_ref[a_rows(j), i * LANES:(i + 1) * LANES]).T.astype(BF16)
        for p in range(phases):
            tile = jnp.where(h < heads, g * per_group + p * tiles + h // heads_per_tile, spare)
            at = pl.multiple_of(lax.rem(h, heads_per_tile) * PHASE_TOKENS, PHASE_TOKENS)
            qt_ref[tile, :, pl.ds(at, PHASE_TOKENS)] = turned[:, p * PHASE_TOKENS:(p + 1) * PHASE_TOKENS]

    def project(j, _):
        slot = lax.rem(j, w_slots)
        block = order(j)
        w_in(block, slot).wait()
        here = pl.ds(pl.multiple_of(slot * width, width), width)
        cols = pl.ds(pl.multiple_of(block * COLS, COLS), COLS)
        before = order(jnp.maximum(j - 1, 0))
        for i in range(heads_per_block):
            queries(before, i)
        s_ref[a_rows(block), :] = dot(hid_ref[...], w_buf[here, :]) + b_ref[cols].astype(F32).reshape(1, COLS)

        @pl.when(j + w_slots < w_blocks)
        def _():
            w_in(order(j + w_slots), slot).start()
        return 0

    early = ((groups - 1) * (heads + 2) + heads) * LANES // COLS - heads * LANES // COLS + 1
    with scope("project"):
        lax.fori_loop(0, early, project, 0)
    for c in range(CHUNKS):
        stage_out(c).wait()
    fetch_cache(0, 0, "start")

    kn_out = pltpu.make_async_copy(kn_buf, kn_ref, out_sem.at[CHUNKS])
    vn_out = pltpu.make_async_copy(vn_buf, vn_ref, out_sem.at[CHUNKS + 1])
    fresh = []
    kvn_out = pltpu.make_async_copy(kvn, ringn_ref.at[me], out_sem.at[CHUNKS + 2])
    for g in range(groups):
        at = (g * (heads + 2) + heads) * LANES
        keys = rotate(s_ref[a_rows(at // COLS), at % COLS:at % COLS + LANES])
        at += LANES
        vals = s_ref[a_rows(at // COLS), at % COLS:at % COLS + LANES]
        fresh.append((keys.astype(BF16), vals.astype(BF16)))
        kvn[g, 0] = keys.astype(BF16)
        for i in range(tok // LANES):
            here = slice(i * LANES, (i + 1) * LANES)
            kvn[g, 1, here, :] = vals[here, :].T.astype(BF16)
    for i in range(tok // LANES):
        here = slice(i * LANES, (i + 1) * LANES)
        for kind, buf in ((0, kn_buf), (1, vn_buf)):
            block = jnp.concatenate([fresh[g][kind][here, :] for g in range(groups)], axis=0)
            buf[i * pair_rows:(i + 1) * pair_rows, :] = dot(pick, block).astype(BF16)
    kvn_out.start()
    for copy in (new_right, new_left, new_pair):
        copy.start()
    send_own(range(1, CHUNKS))
    kn_out.start()
    vn_out.start()
    with scope("project"):
        lax.fori_loop(early, w_blocks, project, 0)
    for i in range(heads_per_block):
        queries(order(w_blocks - 1), i)
    kvn_out.wait()
    fetch_block(0, 0, "start")

    def step(a=None, b=None, c=None):
        alpha_b, alpha_c = al_ref[0], al_ref[1]
        shift = mc_ref[...]
        run = {"max": None, "sum": None, "out": None}

        def scores(i):
            keys = k_buf[a["slot"], i * SUB:(i + 1) * SUB, :]
            s = dot(keys, qt_ref[a["tile"]])
            if i == new_block:
                edge = 1 + lax.rem(a["tile"], per_group) // tiles
                which = jnp.where(a["block"] < me, 0, jnp.where(a["block"] == me, edge, 1 + phases))
                s = s + bias_ref[which].astype(F32)
            s_ref[i * SUB:(i + 1) * SUB, :] = s
            top = jnp.max(s.reshape(SUB // 8, 8, NC), axis=0)
            run["max"] = top if run["max"] is None else jnp.maximum(run["max"], top)

        def weights(i):
            s = s_ref[i * SUB:(i + 1) * SUB, :]
            e = jnp.exp2((s * scale).reshape(SUB // 8, 8, NC) - shift[None])
            part_sum = jnp.sum(e, axis=0)
            run["sum"] = part_sum if run["sum"] is None else run["sum"] + part_sum
            p_ref[i * SUB:(i + 1) * SUB, :] = e.reshape(SUB, NC).astype(BF16)

        def values(i):
            at = i * SUB
            block = jnp.concatenate([v_buf[c["slot"], at + h * LANES:at + (h + 1) * LANES, :] for h in range(SUB // LANES)], axis=1)
            out = dot(block, p_ref[i * SUB:(i + 1) * SUB, :])
            run["out"] = out if run["out"] is None else run["out"] + out

        stages = ((c, values), (b, weights), (a, scores))
        new_block = (span - tok) // SUB
        for i in (new_block, *range(new_block)):
            for spec, stage_fn in stages:
                if spec is not None:
                    stage_fn(i)
        if c is not None:
            acc_ref[c["tile"]] = acc_ref[c["tile"]] * alpha_c + run["out"]
        if b is not None:
            l_ref[b["tile"]] = l_ref[b["tile"]] * alpha_b + run["sum"]
            al_ref[1] = alpha_b
        if a is not None:
            old = m_ref[a["tile"]]
            new = jnp.maximum(old, jnp.max(run["max"], axis=0, keepdims=True))
            m_ref[a["tile"]] = new
            mc_ref[...] = jnp.broadcast_to(new * scale, mc_ref.shape)
            al_ref[0] = jnp.exp2((old - new) * scale)

    def main(tile, slot, block=None):
        return {"tile": tile, "slot": slot, "block": block}

    def run_unit(s, g, first, tile_count, carry, fetch_next, ticks=()):
        with scope("wait_fetch"):
            fetch(s, g, "wait")
        block = block_of(s)

        def one_tile(t, carry):
            for at, what in ticks:
                pl.when((s == at[0]) & (t == at[1]))(what)
            with scope("fetch_next"):
                pl.when(t == tile_count - 1)(fetch_next)
            last, last_slot, older, older_slot = carry
            tile = g * per_group + first + t
            with scope("tile"):
                step(main(tile, g, block), main(last, last_slot), main(older, older_slot))
            return tile, jnp.int32(g), last, last_slot

        return lax.fori_loop(0, tile_count, one_tile, carry)

    start = tuple(jnp.int32(v) for v in (spare, 0, spare, 0))

    def got_new(i):
        new_copy(pair, 0, i, pair).wait_recv()

    def one_set(s, carry):
        nxt = s + 1
        carry = run_unit(s, 0, 0, per_group, carry, lambda: fetch(s, 1, "start"))
        with scope("pass_on"):
            pl.when(s >= 1)(lambda: pass_on(nxt))

        @pl.when(s == 1)
        def _():
            for k in range(OUT_SLOTS):
                wo_in(k).start()

        @pl.when(s == 2)
        def _():
            for copy in (new_hop, new_left_pair, new_right_pair):
                copy.start()

        pl.when((s >= 1) & (s <= 2))(lambda: hop_right(nxt).start())
        pl.when((s >= 3) & (s <= 4))(lambda: hop_left(nxt).start())

        @pl.when(s == n - 3)
        def _():
            got_new(2)
            new_far_pair.start()

        def fetch_next():
            @pl.when(s == 0)
            def _():
                for c in range(CHUNKS):
                    own_pair(c).wait_recv()
                got_new(3)

            @pl.when(s >= 1)
            def _():
                for side in range(2):
                    to_pair(nxt, side).wait_recv()

            @pl.when(s == 1)
            def _():
                got_new(0)
                got_new(1)

            pl.when(s == 3)(lambda: got_new(4))
            pl.when(s == 4)(lambda: got_new(5))
            fetch(nxt, 0, "start")

        return run_unit(s, 1, 0, per_group, carry, fetch_next)

    carry = lax.fori_loop(0, n - 2, one_set, start)
    kn_out.wait()
    vn_out.wait()

    right_rank, left_rank, far_rank = lax.rem(rank + 1, ranks), lax.rem(rank + ranks - 1, ranks), lax.rem(rank + 2, ranks)

    def onward(k):
        return jnp.where(lax.rem(k, 2) == 0, right_rank, left_rank)

    def back(k):
        return jnp.where(lax.rem(k, 2) == 0, left_rank, right_rank)

    def band(of):
        return pl.ds(pl.multiple_of(of * rows, rows), rows)

    def far_copy(p, k):
        return remote(send_buf.at[k, band(far_rank)], got_buf.at[p, 0, k], part_send.at[p, 0], part_recv.at[p, 0, k], "tp", onward(k))

    def near_copy(p, k):
        return remote(send_buf.at[k, band(back(k))], got_buf.at[p, 1, k], part_send.at[p, 1], part_recv.at[p, 1, k], "tp", back(k))

    def comb_copy(p, k):
        return remote(comb_buf.at[k], got_buf.at[p, 2, k], part_send.at[p, 2], part_recv.at[p, 1, k], "tp", onward(k))

    def piece_cols(k):
        return pl.ds(pl.multiple_of(k * COLS, COLS), COLS)

    def y_rows(p, of):
        return pl.ds(pl.multiple_of(p * PHASE_TOKENS + of * rows, rows), rows)

    def y_copy(p, k, way):
        dst = y_ref.at[y_rows(p, rank), piece_cols(k)]
        got = y_last.at[p, 0] if way else y_recv.at[p, k]
        return remote(y_buf.at[p, k], dst, y_send.at[p, way], got, "tp", back(k) if way else onward(k))

    def y_forward(p, k):
        here = y_ref.at[y_rows(p, back(k)), piece_cols(k)]
        return remote(here, here, y_send.at[p, 2], y_last.at[p, 1], "tp", onward(k))

    def y_own(p, k):
        return pltpu.make_async_copy(y_buf.at[p, k], y_ref.at[y_rows(p, rank), piece_cols(k)], y_sem.at[p])

    def each_piece(body, extra=0):
        def piece(k, _):
            body(k)
            return 0
        lax.fori_loop(0, pieces + extra, piece, 0)

    def part_sent(p, kind):
        every = got_buf.at[p, kind]
        remote(every, every, part_send.at[p, kind], part_recv.at[p, 0, 0], "tp", rank).wait_send()

    def project_out(p):
        if p > 0:
            for kind in range(2):
                part_sent(p - 1, kind)

        def two(j, _):
            @pl.when(j < pieces // 2)
            def _():
                both = (2 * j, 2 * j + 1)
                for k in both:
                    wo_in(k).wait()
                for i, k in enumerate(both):
                    out = dot(o_buf[...], w_buf[wo_at(lax.rem(k, OUT_SLOTS)), :])
                    full_buf[i] = out
                    send_buf[k] = out.astype(BF16)
                for i, k in enumerate(both):
                    mine_buf[k] = full_buf[i, band(rank), :]
                    near_buf[k] = full_buf[i, band((right_rank, left_rank)[i]), :]
                for k in both:
                    pl.when(k + OUT_SLOTS < pieces)(lambda k=k: wo_in(k + OUT_SLOTS).start())

            @pl.when(j >= 1)
            def _():
                for k in (2 * j - 2, 2 * j - 1):
                    far_copy(p, k).start()
                    near_copy(p, k).start()
            return 0

        lax.fori_loop(0, pieces // 2 + 1, two, 0)

    def combine(p):
        if p > 0:
            part_sent(p - 1, 2)

        def piece(k):
            @pl.when(k < pieces)
            def _():
                far_copy(p, k).wait_recv()
                comb_buf[k] = (near_buf[k] + got_buf[p, 0, k].astype(F32)).astype(BF16)

            pl.when(k >= 1)(lambda: comb_copy(p, k - 1).start())

        each_piece(piece, 1)

    def reduce(p):
        def piece(k):
            @pl.when(k < pieces)
            def _():
                both = got_buf.at[p, pl.ds(1, 2), k]
                remote(both, both, part_send.at[p, 1], part_recv.at[p, 1, k], "tp", rank).wait_recv()
                total = mine_buf[k] + got_buf[p, 1, k].astype(F32) + got_buf[p, 2, k].astype(F32)
                y_buf[p, k] = (y_buf[p, k].astype(F32) + total).astype(BF16)

            @pl.when(k >= 1)
            def _():
                y_copy(p, k - 1, 0).start()
                y_copy(p, k - 1, 1).start()
                y_own(p, k - 1).start()

        each_piece(piece, 1)

    def forward(p):
        def piece(k):
            y_copy(p, k, 0).wait_recv()
            y_forward(p, k).start()
        each_piece(piece)

    def finish(p, g):
        def tile(h, _):
            t = g * per_group + p * tiles + h
            total = jnp.sum(l_ref[t], axis=0, keepdims=True)
            out = (acc_ref[t] / total).T.astype(BF16)
            for i in range(heads_per_tile):
                at = pl.multiple_of((g * heads + h * heads_per_tile + i) * LANES, LANES)
                o_buf[:, pl.ds(at, LANES)] = out[i * PHASE_TOKENS:(i + 1) * PHASE_TOKENS, :]
            return 0

        lax.fori_loop(0, tiles, tile, 0)

    for p in range(phases):
        pltpu.make_async_copy(y_buf.at[p], y_buf.at[p], in_sem.at[2 + p, 1]).wait()

    def late(p, carry):
        first = p * tiles

        def between(s, g):
            if p == 0 and g == 0:
                pl.when(s == n - 2)(lambda: pass_on(n - 1))
            if p > 0:
                @pl.when((s == n - 2) & (g == 0))
                def _():
                    with scope("project_out"):
                        for other in range(groups):
                            finish(p - 1, other)
                        project_out(p - 1)
                    for k in range(OUT_SLOTS):
                        wo_in(k).start()

        def scoped(name, step_fn):
            def run():
                with scope(name):
                    step_fn(p - 1)
            return run

        ticks = ((), ())
        if p > 0:
            ticks = ((((n - 1, 0), scoped("reduce", reduce)),), (((n - 2, 1), scoped("combine", combine)), ((n - 1, 1), scoped("forward", forward))))

        def late_set(s, carry):
            carry = run_unit(s, 0, first, tiles, carry, lambda: fetch(s, 1, "start"), ticks[0])
            between(s, 0)

            def fetch_next():
                @pl.when(s == n - 2)
                def _():
                    if p == 0:
                        for side in range(2):
                            to_pair(n - 1, side).wait_recv()
                        got_new(6)
                    fetch(n - 1, 0, "start")
                if p < phases - 1:
                    pl.when(s == n - 1)(lambda: fetch(n - 2, 0, "start"))

            return run_unit(s, 1, first, tiles, carry, fetch_next, ticks[1])

        return lax.fori_loop(n - 2, n, late_set, carry)

    for p in range(phases):
        carry = late(p, carry)
    last, last_slot, older, older_slot = carry
    with scope("finish"):
        step(None, main(last, last_slot), main(older, older_slot))
        step(None, None, main(last, last_slot))
        for g in range(groups):
            finish(phases - 1, g)
    with scope("project_out"):
        project_out(phases - 1)
    with scope("combine"):
        combine(phases - 1)
    with scope("reduce"):
        reduce(phases - 1)
    with scope("forward"):
        forward(phases - 1)

    for way in range(3):
        remote(stage, stage, own_send.at[way], recv.at[0, 0], "cp", me).wait_send()
    passed = ring_ref.at[pl.ds(2, n - 2), pl.ds(0, 2)]
    remote(passed, passed, pair_send, recv.at[0, 0], "cp", me).wait_send()
    for s in (2, 3):
        hop_right(s).wait_send()
    for s in (4, 5):
        hop_left(s).wait_send()
    for copy in (new_right, new_left, new_pair, new_hop, new_left_pair, new_right_pair, new_far_pair):
        copy.wait_send()

    with scope("drain_out"):
        for kind in range(3):
            part_sent(phases - 1, kind)
        for p in range(phases):
            every = y_buf.at[p]
            pltpu.make_async_copy(every, every, y_sem.at[p]).wait()
            for way in range(3):
                remote(every, every, y_send.at[p, way], y_last.at[p, 0], "tp", rank).wait_send()
            for way in range(2):
                remote(every, every, y_send.at[p, way], y_last.at[p, way], "tp", rank).wait_recv()


def results_kernel(y_in, kn_in, vn_in, y_out, kn_out, vn_out, y_buf, kn_buf, vn_buf, sem):
    rows = y_buf.shape[0] // 4
    copies = []
    for i in range(4):
        here = slice(i * rows, (i + 1) * rows)
        copies.append((y_in.at[here], y_buf.at[here], y_out.at[here]))
    copies += [(kn_in, kn_buf, kn_out), (vn_in, vn_buf, vn_out)]
    for i, (src, buf, _) in enumerate(copies):
        pltpu.make_async_copy(src, buf, sem.at[0, i]).start()
    for i, (src, buf, dst) in enumerate(copies):
        pltpu.make_async_copy(src, buf, sem.at[0, i]).wait()
        pltpu.make_async_copy(buf, dst, sem.at[1, i]).start()
    for i, (_, buf, dst) in enumerate(copies):
        pltpu.make_async_copy(buf, dst, sem.at[1, i]).wait()


def results(*arrays):
    any_spec = pl.BlockSpec(memory_space=pl.ANY)
    return pl.pallas_call(
        results_kernel,
        in_specs=[any_spec] * 3,
        out_specs=[any_spec] * 3,
        out_shape=[jax.ShapeDtypeStruct(a.shape, a.dtype) for a in arrays],
        scratch_shapes=[pltpu.VMEM(a.shape, a.dtype) for a in arrays] + [DMA((2, 6))],
        compiler_params=pltpu.CompilerParams(vmem_limit_bytes=62 << 20),
        name="results",
    )(*arrays)


def local_step(n, ranks, x, k_cache, v_cache, rope_table, norm_gain, w_qkv, b_qkv, w_out):
    positions, groups, head_dim = k_cache.shape
    tok, width = x.shape
    heads = w_qkv.shape[1] // groups // head_dim - 2
    part = positions // CHUNKS
    span = positions + tok
    phases = tok // PHASE_TOKENS
    tiles = heads * PHASE_TOKENS // NC
    count = groups * phases * tiles
    pieces = width // COLS
    rows = PHASE_TOKENS // ranks
    depth = w_out.shape[0]
    any_spec = pl.BlockSpec(memory_space=pl.ANY)
    vmem_spec = pl.BlockSpec(memory_space=pltpu.VMEM)
    flat = (positions * groups, head_dim)
    flops = 4 * count * NC * LANES * n * (span + tok)
    y, new_k, new_v, _, _ = pl.pallas_call(
        functools.partial(block_kernel, (n, ranks, groups, heads)),
        in_specs=[any_spec, any_spec, any_spec, vmem_spec, vmem_spec, any_spec, vmem_spec, any_spec],
        out_specs=[any_spec] * 5,
        out_shape=[
            jax.ShapeDtypeStruct((tok, width), BF16),
            jax.ShapeDtypeStruct((tok * groups, head_dim), BF16),
            jax.ShapeDtypeStruct((tok * groups, head_dim), BF16),
            jax.ShapeDtypeStruct((n, CHUNKS, groups, 2, part, head_dim), BF16),
            jax.ShapeDtypeStruct((n, groups, 2, tok, head_dim), BF16),
        ],
        scratch_shapes=[
            pltpu.VMEM((2, span, LANES), BF16),
            pltpu.VMEM((2, span, LANES), BF16),
            pltpu.VMEM((CHUNKS, groups, 2, part, LANES), BF16),
            pltpu.VMEM((groups, 2, tok, LANES), BF16),
            pltpu.VMEM((count + 1, LANES, NC), BF16),
            pltpu.VMEM((tok, width), BF16),
            pltpu.VMEM((tok, width), BF16),
            pltpu.VMEM((max(3 * width, OUT_SLOTS * depth), COLS), BF16),
            pltpu.VMEM((tok, LANES), F32),
            pltpu.VMEM((tok, LANES), F32),
            pltpu.VMEM((tok * groups, LANES), BF16),
            pltpu.VMEM((tok * groups, LANES), BF16),
            pltpu.VMEM((max(span, w_qkv.shape[1] // COLS * tok), NC), F32),
            pltpu.VMEM((span, NC), BF16),
            pltpu.VMEM((count + 1, LANES, NC), F32),
            pltpu.VMEM((count, 1, NC), F32),
            pltpu.VMEM((count + 1, 8, NC), F32),
            pltpu.VMEM((8, NC), F32),
            pltpu.VMEM((2, 1, NC), F32),
            pltpu.VMEM((2 + phases, tok, NC), BF16),
            pltpu.VMEM((PHASE_TOKENS, groups * heads * LANES), BF16),
            pltpu.VMEM((2, PHASE_TOKENS, COLS), F32),
            pltpu.VMEM((pieces, rows, COLS), F32),
            pltpu.VMEM((pieces, rows, COLS), F32),
            pltpu.VMEM((pieces, PHASE_TOKENS, COLS), BF16),
            pltpu.VMEM((pieces, rows, COLS), BF16),
            pltpu.VMEM((phases, 3, pieces, rows, COLS), BF16),
            pltpu.VMEM((phases, pieces, rows, COLS), BF16),
            DMA((2 + phases, 2)),
            DMA((OUT_SLOTS,)),
            DMA((CHUNKS + 3,)),
            DMA((groups, 2, CHUNKS + 1)),
            DMA((3,)),
            DMA,
            DMA((n,)),
            DMA((7,)),
            DMA((n, CHUNKS)),
            DMA((7,)),
            DMA((phases, 3)),
            DMA((phases, 2, pieces)),
            DMA((phases, 3)),
            DMA((phases, pieces)),
            DMA((phases, 2)),
            DMA((phases,)),
        ],
        cost_estimate=pl.CostEstimate(flops=flops, bytes_accessed=4 * positions * n * groups * head_dim, transcendentals=flops // (4 * LANES)),
        compiler_params=pltpu.CompilerParams(collective_id=0, has_side_effects=True, vmem_limit_bytes=63 << 20),
        name="block",
    )(x, k_cache.reshape(flat), v_cache.reshape(flat), rope_table.T, norm_gain, w_qkv, b_qkv, w_out)
    y, new_k, new_v = results(y, new_k, new_v)
    new_shape = (tok,) + k_cache.shape[1:]
    return y, new_k.reshape(new_shape), new_v.reshape(new_shape)


def solution(mesh):
    row_spec = P(("dp", "cp"), None)
    cache_spec = P(("dp", "cp"), "tp", None)
    body = functools.partial(local_step, mesh.shape["cp"], mesh.shape["tp"])
    return jax.shard_map(body, mesh=mesh, in_specs=(row_spec, cache_spec, cache_spec, row_spec, P(None), P(None, "tp"), P("tp"), P("tp", None)), out_specs=(row_spec, cache_spec, cache_spec), check_vma=False)
```

```python
import functools
import math

import jax
import jax.numpy as jnp
from jax import lax
from jax.experimental import pallas as pl
from jax.experimental.pallas import tpu as pltpu
from jax.sharding import PartitionSpec as P

EPS = 1.5625e-07
MASK_VALUE = -1e30
LANES = 128
SUB = 256
NC = 512
PHASE_TOKENS = 128
CHUNKS = 4
COLS = 512
OUT_SLOTS = 7
MESH = pl.DeviceIdType.MESH
F32 = jnp.float32
BF16 = jnp.bfloat16
DMA = pltpu.SemaphoreType.DMA
scope = jax.named_scope


def dot(a, b, dims=(((1,), (0,)), ((), ()))):
    return lax.dot_general(a, b, dims, preferred_element_type=F32)


def block_kernel(dims, x_ref, kc_ref, vc_ref, table_ref, g_ref, wq_ref, b_ref, wo_ref,
                 y_ref, kn_ref, vn_ref, ring_ref, ringn_ref,
                 k_buf, v_buf, stage, kvn, qt_ref, hid_ref, x_buf, w_buf, cos_ref, sin_ref, kn_buf, vn_buf,
                 s_ref, p_ref, acc_ref, m_ref, l_ref, mc_ref, al_ref, diff_ref,
                 o_buf, full_buf, mine_buf, near_buf, send_buf, comb_buf, got_buf, y_buf,
                 in_sem, w_sem, out_sem, fetch_sem, own_send, pair_send, hop_send, new_send, recv, new_recv,
                 part_send, part_recv, y_send, y_recv, y_last, y_sem):
    n, ranks, groups, heads = dims
    me = lax.axis_index("cp")
    rank = lax.axis_index("tp")
    pair = me + 1 - 2 * lax.rem(me, 2)
    right, left, far = lax.rem(me + 2, n), lax.rem(me + n - 2, n), lax.rem(me + 4, n)
    tok, width = x_ref.shape
    part = stage.shape[3]
    span = CHUNKS * part + tok
    phases = tok // PHASE_TOKENS
    heads_per_tile = NC // PHASE_TOKENS
    tiles = heads // heads_per_tile
    per_group = phases * tiles
    count = groups * per_group
    spare = count
    half = kc_ref.shape[0] // 2
    scale = LANES ** -0.5 * math.log2(math.e)
    head_count = groups * (heads + 2)
    w_blocks = head_count * LANES // COLS
    heads_per_block = COLS // LANES
    pieces = width // COLS
    w_slots = w_buf.shape[0] // width
    out_depth = wo_ref.shape[0]
    rows = PHASE_TOKENS // ranks

    def remote(src, dst, send, got, axis, where):
        return pltpu.make_async_remote_copy(src_ref=src, dst_ref=dst, send_sem=send, recv_sem=got, device_id={axis: where}, device_id_type=MESH)

    def own_pair(c):
        return remote(stage.at[c], ring_ref.at[1, c], own_send.at[0], recv.at[1, c], "cp", pair)

    def own_right(c):
        return remote(stage.at[c], ring_ref.at[2 + c, 0], own_send.at[1], recv.at[2 + c, 0], "cp", right)

    def own_left(c):
        return remote(stage.at[c], ring_ref.at[2 + c, 1], own_send.at[2], recv.at[2 + c, 1], "cp", left)

    def to_pair(s, side):
        return remote(ring_ref.at[s, side], ring_ref.at[s, 2 + side], pair_send, recv.at[s, 2 + side], "cp", pair)

    def from_side(s, side):
        return remote(stage.at[0], ring_ref.at[s, side], own_send.at[0], recv.at[s, side], "cp", pair)

    def hop_right(s):
        return remote(ring_ref.at[s, 0], ring_ref.at[s + 4, 0], hop_send.at[s], recv.at[s + 4, 0], "cp", right)

    def hop_left(s):
        return remote(ring_ref.at[s, 1], ring_ref.at[s + 2, 1], hop_send.at[s], recv.at[s + 2, 1], "cp", left)

    def new_copy(source, send, got, where, own=False):
        src = kvn if own else ringn_ref.at[source]
        return remote(src, ringn_ref.at[source], new_send.at[send], new_recv.at[got], "cp", where)

    new_right = new_copy(me, 0, 0, right, own=True)
    new_left = new_copy(me, 1, 1, left, own=True)
    new_pair = new_copy(me, 2, 3, pair, own=True)
    new_hop = new_copy(left, 3, 2, right)
    new_left_pair = new_copy(left, 4, 4, pair)
    new_right_pair = new_copy(right, 5, 5, pair)
    new_far_pair = new_copy(far, 6, 6, pair)

    def pass_on(s):
        for side in range(2):
            from_side(s, side).wait_recv()
            to_pair(s, side).start()

    def cache_in(i):
        here = pl.ds(i * half, half)
        return (pltpu.make_async_copy(kc_ref.at[here], k_buf.at[i, pl.ds(0, half)], in_sem.at[0, i]),
                pltpu.make_async_copy(vc_ref.at[here], v_buf.at[i, pl.ds(0, half)], in_sem.at[1, i]))

    x_in = pltpu.make_async_copy(x_ref, x_buf, in_sem.at[2, 0])

    def res_in(p, k):
        here = pl.ds(pl.multiple_of(p * PHASE_TOKENS + rank * rows, rows), rows)
        return pltpu.make_async_copy(x_ref.at[here, k * COLS:(k + 1) * COLS], y_buf.at[p, k], in_sem.at[2 + p, 1])

    def w_in(j, slot):
        cols = pl.ds(pl.multiple_of(j * COLS, COLS), COLS)
        here = pl.ds(pl.multiple_of(slot * width, width), width)
        return pltpu.make_async_copy(wq_ref.at[:, cols], w_buf.at[here], w_sem.at[slot])

    def order(j):
        return lax.rem(j + heads * LANES // COLS, w_blocks)

    def wo_at(slot):
        return pl.ds(pl.multiple_of(slot * out_depth, out_depth), out_depth)

    def wo_in(k):
        slot = lax.rem(k, OUT_SLOTS)
        cols = pl.ds(pl.multiple_of(k * COLS, COLS), COLS)
        return pltpu.make_async_copy(wo_ref.at[:, cols], w_buf.at[wo_at(slot)], w_sem.at[slot])

    x_in.start()
    for i in range(2):
        for copy in cache_in(i):
            copy.start()
    w_in(order(0), 0).start()
    for p in range(phases):
        for k in range(pieces):
            res_in(p, k).start()

    barrier = pltpu.get_barrier_semaphore()
    for other in (pair, right, left):
        pl.semaphore_signal(barrier, inc=1, device_id={"cp": other}, device_id_type=MESH)
    for d in range(1, ranks):
        pl.semaphore_signal(barrier, inc=1, device_id={"tp": lax.rem(rank + d, ranks)}, device_id_type=MESH)

    row = lax.broadcasted_iota(jnp.int32, (tok, NC), 0)
    diff_ref[...] = row - lax.rem(lax.broadcasted_iota(jnp.int32, (tok, NC), 1), PHASE_TOKENS)

    m_ref[...] = jnp.full(m_ref.shape, MASK_VALUE, F32)
    l_ref[...] = jnp.zeros(l_ref.shape, F32)
    acc_ref[...] = jnp.zeros(acc_ref.shape, F32)
    mc_ref[...] = jnp.zeros(mc_ref.shape, F32)
    al_ref[...] = jnp.ones(al_ref.shape, F32)

    x_in.wait()
    for j in range(1, w_slots):
        w_in(order(j), j).start()
    gain = g_ref[...].astype(F32).reshape(1, width)
    norm_rows = tok // (CHUNKS * (part // LANES // 4))

    def norm(i):
        here = pl.ds(pl.multiple_of(i * norm_rows, norm_rows), norm_rows)
        x = x_buf[here, :].astype(F32)
        inv_rms = lax.rsqrt(jnp.mean(x * x, axis=-1, keepdims=True) + EPS)
        hid_ref[here, :] = (x * inv_rms * gain).astype(BF16)

    pair_rows = groups * LANES
    wide = lax.broadcasted_iota(jnp.int32, (pair_rows, pair_rows), 0)
    tall = lax.broadcasted_iota(jnp.int32, (pair_rows, pair_rows), 1)
    pick = (wide // groups + (wide % groups) * LANES == tall).astype(BF16)
    pick_t = (tall // groups + (tall % groups) * LANES == wide).astype(BF16)
    blocks = part // LANES

    def stage_out(c):
        return pltpu.make_async_copy(stage.at[c], ring_ref.at[0, c], out_sem.at[c])

    for c in range(CHUNKS):
        if c % (CHUNKS // 2) == 0:
            for copy in cache_in(c // (CHUNKS // 2)):
                copy.wait()

        def relayout(i, _):
            i_half = c // (CHUNKS // 2)
            for sub in range(4):
                at = i * 4 + sub
                src = pl.ds(pl.multiple_of((c % (CHUNKS // 2)) * part * groups + at * pair_rows, pair_rows), pair_rows)
                here = pl.ds(pl.multiple_of(at * LANES, LANES), LANES)
                keys = dot(pick_t, k_buf[i_half, src, :]).astype(BF16)
                vals = dot(v_buf[i_half, src, :], pick, (((0,), (0,)), ((), ()))).astype(BF16)
                for g in range(groups):
                    stage[c, g, 0, here, :] = keys[g * LANES:(g + 1) * LANES, :]
                    stage[c, g, 1, here, :] = vals[:, g * LANES:(g + 1) * LANES]
            norm(c * (blocks // 4) + i)
            return 0

        with scope("relayout"):
            lax.fori_loop(0, blocks // 4, relayout, 0)
        stage_out(c).start()

    def send_own(chunks):
        for c in chunks:
            own_right(c).start()
            own_left(c).start()
            own_pair(c).start()

    with scope("barrier"):
        pl.semaphore_wait(barrier, 3 + ranks - 1)
    send_own(range(1))

    lane = lax.broadcasted_iota(jnp.int32, (tok, LANES), 1)
    rope_lanes = table_ref.shape[0]
    table = jnp.concatenate([table_ref[...].T, jnp.zeros((tok, LANES - rope_lanes), F32)], axis=1)
    at = jnp.where(lane < rope_lanes, lane // 2, 0)
    sin = jnp.take_along_axis(table, at + rope_lanes // 2, axis=1)
    cos_ref[...] = jnp.take_along_axis(table, at, axis=1)
    sin_ref[...] = jnp.where(lane % 2 == 0, -sin, sin)

    def rotate(head):
        swapped = jnp.where(lane % 2 == 0, pltpu.roll(head, LANES - 1, 1), pltpu.roll(head, 1, 1))
        turned = head * cos_ref[...] + swapped * sin_ref[...]
        return jnp.where(lane < rope_lanes, turned, head)

    pair_left, pair_right, pair_far = lax.rem(pair + n - 2, n), lax.rem(pair + 2, n), lax.rem(pair + 4, n)

    def block_of(s):
        out = me
        for i, source in enumerate((pair, left, right, pair_left, pair_right, far, pair_far)):
            out = jnp.where(s == i + 1, source, out)
        return out

    def fetch_cache(s, g, act):
        for kind, buf in ((0, k_buf), (1, v_buf)):
            for c in range(CHUNKS):
                here = pl.ds(c * part, part)
                getattr(pltpu.make_async_copy(ring_ref.at[s, c, g, kind], buf.at[g, here], fetch_sem.at[g, kind, c]), act)()

    def fetch_block(s, g, act):
        for kind, buf in ((0, k_buf), (1, v_buf)):
            here = pl.ds(CHUNKS * part, tok)
            getattr(pltpu.make_async_copy(ringn_ref.at[block_of(s), g, kind], buf.at[g, here], fetch_sem.at[g, kind, CHUNKS]), act)()

    def fetch(s, g, act):
        fetch_cache(s, g, act)
        fetch_block(s, g, act)

    def a_rows(j):
        return pl.ds(pl.multiple_of(j * tok, tok), tok)

    def queries(j, i):
        head = j * heads_per_block + i
        g, h = head // (heads + 2), lax.rem(head, heads + 2)
        turned = rotate(s_ref[a_rows(j), i * LANES:(i + 1) * LANES]).T.astype(BF16)
        for p in range(phases):
            tile = jnp.where(h < heads, g * per_group + p * tiles + h // heads_per_tile, spare)
            at = pl.multiple_of(lax.rem(h, heads_per_tile) * PHASE_TOKENS, PHASE_TOKENS)
            qt_ref[tile, :, pl.ds(at, PHASE_TOKENS)] = turned[:, p * PHASE_TOKENS:(p + 1) * PHASE_TOKENS]

    def project(j, _):
        slot = lax.rem(j, w_slots)
        block = order(j)
        w_in(block, slot).wait()
        here = pl.ds(pl.multiple_of(slot * width, width), width)
        cols = pl.ds(pl.multiple_of(block * COLS, COLS), COLS)
        before = order(jnp.maximum(j - 1, 0))
        for i in range(heads_per_block):
            queries(before, i)
        s_ref[a_rows(block), :] = dot(hid_ref[...], w_buf[here, :]) + b_ref[cols].astype(F32).reshape(1, COLS)

        @pl.when(j + w_slots < w_blocks)
        def _():
            w_in(order(j + w_slots), slot).start()
        return 0

    early = ((groups - 1) * (heads + 2) + heads) * LANES // COLS - heads * LANES // COLS + 1
    with scope("project"):
        lax.fori_loop(0, early, project, 0)
    for c in range(CHUNKS):
        stage_out(c).wait()
    fetch_cache(0, 0, "start")

    kn_out = pltpu.make_async_copy(kn_buf, kn_ref, out_sem.at[CHUNKS])
    vn_out = pltpu.make_async_copy(vn_buf, vn_ref, out_sem.at[CHUNKS + 1])
    fresh = []
    kvn_out = pltpu.make_async_copy(kvn, ringn_ref.at[me], out_sem.at[CHUNKS + 2])
    for g in range(groups):
        at = (g * (heads + 2) + heads) * LANES
        keys = rotate(s_ref[a_rows(at // COLS), at % COLS:at % COLS + LANES])
        at += LANES
        vals = s_ref[a_rows(at // COLS), at % COLS:at % COLS + LANES]
        fresh.append((keys.astype(BF16), vals.astype(BF16)))
        kvn[g, 0] = keys.astype(BF16)
        for i in range(tok // LANES):
            here = slice(i * LANES, (i + 1) * LANES)
            kvn[g, 1, here, :] = vals[here, :].T.astype(BF16)
    for i in range(tok // LANES):
        here = slice(i * LANES, (i + 1) * LANES)
        for kind, buf in ((0, kn_buf), (1, vn_buf)):
            block = jnp.concatenate([fresh[g][kind][here, :] for g in range(groups)], axis=0)
            buf[i * pair_rows:(i + 1) * pair_rows, :] = dot(pick, block).astype(BF16)
    kvn_out.start()
    for copy in (new_right, new_left, new_pair):
        copy.start()
    send_own(range(1, CHUNKS))
    kn_out.start()
    vn_out.start()
    with scope("project"):
        lax.fori_loop(early, w_blocks, project, 0)
    for i in range(heads_per_block):
        queries(order(w_blocks - 1), i)
    kvn_out.wait()
    fetch_block(0, 0, "start")

    def step(a=None, b=None, c=None):
        alpha_b, alpha_c = al_ref[0], al_ref[1]
        shift = mc_ref[...]
        run = {"max": None, "sum": None, "out": None}

        def scores(i):
            keys = k_buf[a["slot"], i * SUB:(i + 1) * SUB, :]
            s = dot(keys, qt_ref[a["tile"]])
            if i == new_block:
                limit = (me - a["block"]) * tok + lax.rem(a["tile"], per_group) // tiles * PHASE_TOKENS
                s = jnp.where(diff_ref[...] <= limit, s, MASK_VALUE)
            s_ref[i * SUB:(i + 1) * SUB, :] = s
            top = jnp.max(s.reshape(SUB // 8, 8, NC), axis=0)
            run["max"] = top if run["max"] is None else jnp.maximum(run["max"], top)

        def weights(i):
            s = s_ref[i * SUB:(i + 1) * SUB, :]
            e = jnp.exp2((s * scale).reshape(SUB // 8, 8, NC) - shift[None])
            part_sum = jnp.sum(e, axis=0)
            run["sum"] = part_sum if run["sum"] is None else run["sum"] + part_sum
            p_ref[i * SUB:(i + 1) * SUB, :] = e.reshape(SUB, NC).astype(BF16)

        def values(i):
            at = i * SUB
            block = jnp.concatenate([v_buf[c["slot"], at + h * LANES:at + (h + 1) * LANES, :] for h in range(SUB // LANES)], axis=1)
            out = dot(block, p_ref[i * SUB:(i + 1) * SUB, :])
            run["out"] = out if run["out"] is None else run["out"] + out

        stages = ((c, values), (b, weights), (a, scores))
        new_block = (span - tok) // SUB
        for i in (new_block, *range(new_block)):
            for spec, stage_fn in stages:
                if spec is not None:
                    stage_fn(i)
        if c is not None:
            acc_ref[c["tile"]] = acc_ref[c["tile"]] * alpha_c + run["out"]
        if b is not None:
            l_ref[b["tile"]] = l_ref[b["tile"]] * alpha_b + run["sum"]
            al_ref[1] = alpha_b
        if a is not None:
            old = m_ref[a["tile"]]
            new = jnp.maximum(old, jnp.max(run["max"], axis=0, keepdims=True))
            m_ref[a["tile"]] = new
            mc_ref[...] = jnp.broadcast_to(new * scale, mc_ref.shape)
            al_ref[0] = jnp.exp2((old - new) * scale)

    def main(tile, slot, block=None):
        return {"tile": tile, "slot": slot, "block": block}

    def run_unit(s, g, first, tile_count, carry, fetch_next, ticks=()):
        with scope("wait_fetch"):
            fetch(s, g, "wait")
        block = block_of(s)

        def one_tile(t, carry):
            for at, what in ticks:
                pl.when((s == at[0]) & (t == at[1]))(what)
            with scope("fetch_next"):
                pl.when(t == tile_count - 1)(fetch_next)
            last, last_slot, older, older_slot = carry
            tile = g * per_group + first + t
            with scope("tile"):
                step(main(tile, g, block), main(last, last_slot), main(older, older_slot))
            return tile, jnp.int32(g), last, last_slot

        return lax.fori_loop(0, tile_count, one_tile, carry)

    start = tuple(jnp.int32(v) for v in (spare, 0, spare, 0))

    def got_new(i):
        new_copy(pair, 0, i, pair).wait_recv()

    def one_set(s, carry):
        nxt = s + 1
        carry = run_unit(s, 0, 0, per_group, carry, lambda: fetch(s, 1, "start"))
        with scope("pass_on"):
            pl.when(s >= 1)(lambda: pass_on(nxt))

        @pl.when(s == 1)
        def _():
            for k in range(OUT_SLOTS):
                wo_in(k).start()

        @pl.when(s == 2)
        def _():
            for copy in (new_hop, new_left_pair, new_right_pair):
                copy.start()

        pl.when((s >= 1) & (s <= 2))(lambda: hop_right(nxt).start())
        pl.when((s >= 3) & (s <= 4))(lambda: hop_left(nxt).start())

        @pl.when(s == n - 3)
        def _():
            got_new(2)
            new_far_pair.start()

        def fetch_next():
            @pl.when(s == 0)
            def _():
                for c in range(CHUNKS):
                    own_pair(c).wait_recv()
                got_new(3)

            @pl.when(s >= 1)
            def _():
                for side in range(2):
                    to_pair(nxt, side).wait_recv()

            @pl.when(s == 1)
            def _():
                got_new(0)
                got_new(1)

            pl.when(s == 3)(lambda: got_new(4))
            pl.when(s == 4)(lambda: got_new(5))
            fetch(nxt, 0, "start")

        return run_unit(s, 1, 0, per_group, carry, fetch_next)

    carry = lax.fori_loop(0, n - 2, one_set, start)
    kn_out.wait()
    vn_out.wait()

    right_rank, left_rank, far_rank = lax.rem(rank + 1, ranks), lax.rem(rank + ranks - 1, ranks), lax.rem(rank + 2, ranks)

    pairs = pieces // 2 - 1
    singles = ((pairs, pieces - 2), (pairs + 1, pieces - 1))

    def onward(i):
        return jnp.where(lax.rem(i, 2) == 0, right_rank, left_rank)

    def back(i):
        return jnp.where(lax.rem(i, 2) == 0, left_rank, right_rank)

    def band(of):
        return pl.ds(pl.multiple_of(of * rows, rows), rows)

    def far_copy(p, i, at):
        return remote(send_buf.at[at, band(far_rank)], got_buf.at[p, 0, at], part_send.at[p, 0], part_recv.at[p, 0, i], "tp", onward(i))

    def near_copy(p, i, at):
        return remote(send_buf.at[at, band(back(i))], got_buf.at[p, 1, at], part_send.at[p, 1], part_recv.at[p, 1, i], "tp", back(i))

    def comb_copy(p, i, at):
        return remote(comb_buf.at[at], got_buf.at[p, 2, at], part_send.at[p, 2], part_recv.at[p, 1, i], "tp", onward(i))

    def y_rows(p, of):
        return pl.ds(pl.multiple_of(p * PHASE_TOKENS + of * rows, rows), rows)

    def y_copy(p, i, at, way):
        got = y_last.at[p, 0] if way else y_recv.at[p, i]
        return remote(y_buf.at[p, at], y_ref.at[at, y_rows(p, rank)], y_send.at[p, way], got, "tp", back(i) if way else onward(i))

    def y_forward(p, i, at):
        here = y_ref.at[at, y_rows(p, back(i))]
        return remote(here, here, y_send.at[p, 2], y_last.at[p, 1], "tp", onward(i))

    def y_own(p, at):
        return pltpu.make_async_copy(y_buf.at[p, at], y_ref.at[at, y_rows(p, rank)], y_sem.at[p])

    def pair_at(i):
        return pl.ds(2 * i, 2)

    def each_group(work, send):
        def step_of(i, _):
            pl.when(i < pairs)(lambda: [work(i, 2 * i, 2), None][1])
            pl.when(i > 0)(lambda: [send(i - 1, pair_at(i - 1)), None][1])
            return 0

        lax.fori_loop(0, pairs + 1, step_of, 0)
        for i, k in singles:
            work(i, k, 1)
        for i, k in singles:
            send(i, pl.ds(k, 1))

    def part_sent(p, kind):
        every = got_buf.at[p, kind]
        remote(every, every, part_send.at[p, kind], part_recv.at[p, 0, 0], "tp", rank).wait_send()

    def project_out(p):
        if p > 0:
            for kind in range(2):
                part_sent(p - 1, kind)

        def two(j, _):
            @pl.when(j < pieces // 2)
            def _():
                both = (2 * j, 2 * j + 1)
                for k in both:
                    wo_in(k).wait()
                for i, k in enumerate(both):
                    out = dot(o_buf[...], w_buf[wo_at(lax.rem(k, OUT_SLOTS)), :])
                    full_buf[i] = out
                    send_buf[k] = out.astype(BF16)
                for i, k in enumerate(both):
                    mine_buf[k] = full_buf[i, band(rank), :]
                    way = jnp.where(j < pairs, j, pairs + i)
                    near_buf[k] = full_buf[i, band(onward(way)), :]
                for k in both:
                    pl.when(k + OUT_SLOTS < pieces)(lambda k=k: wo_in(k + OUT_SLOTS).start())

            @pl.when(j >= 1)
            def _():
                @pl.when(j <= pairs)
                def _():
                    far_copy(p, j - 1, pair_at(j - 1)).start()
                    near_copy(p, j - 1, pair_at(j - 1)).start()

                @pl.when(j > pairs)
                def _():
                    for i, k in singles:
                        far_copy(p, i, pl.ds(k, 1)).start()
                        near_copy(p, i, pl.ds(k, 1)).start()
            return 0

        lax.fori_loop(0, pieces // 2 + 1, two, 0)

    def combine(p):
        if p > 0:
            part_sent(p - 1, 2)

        def work(i, k, size):
            far_copy(p, i, pl.ds(k, size)).wait_recv()
            for j in range(size):
                comb_buf[k + j] = (near_buf[k + j] + got_buf[p, 0, k + j].astype(F32)).astype(BF16)

        each_group(work, lambda i, at: comb_copy(p, i, at).start())

    def reduce(p):
        def work(i, k, size):
            both = got_buf.at[p, pl.ds(1, 2), pl.ds(k, size)]
            remote(both, both, part_send.at[p, 1], part_recv.at[p, 1, i], "tp", rank).wait_recv()
            for j in range(size):
                total = mine_buf[k + j] + got_buf[p, 1, k + j].astype(F32) + got_buf[p, 2, k + j].astype(F32)
                y_buf[p, k + j] = (y_buf[p, k + j].astype(F32) + total).astype(BF16)

        def send(i, at):
            y_copy(p, i, at, 0).start()
            y_copy(p, i, at, 1).start()
            y_own(p, at).start()

        each_group(work, send)

    def forward(p):
        def work(i, k, size):
            at = pl.ds(k, size)
            y_copy(p, i, at, 0).wait_recv()
            y_forward(p, i, at).start()

        def pair_of(i, _):
            work(i, 2 * i, 2)
            return 0

        lax.fori_loop(0, pairs, pair_of, 0)
        for i, k in singles:
            work(i, k, 1)

    def finish(p, g):
        def tile(h, _):
            t = g * per_group + p * tiles + h
            total = jnp.sum(l_ref[t], axis=0, keepdims=True)
            out = (acc_ref[t] / total).T.astype(BF16)
            for i in range(heads_per_tile):
                at = pl.multiple_of((g * heads + h * heads_per_tile + i) * LANES, LANES)
                o_buf[:, pl.ds(at, LANES)] = out[i * PHASE_TOKENS:(i + 1) * PHASE_TOKENS, :]
            return 0

        lax.fori_loop(0, tiles, tile, 0)

    for p in range(phases):
        pltpu.make_async_copy(y_buf.at[p], y_buf.at[p], in_sem.at[2 + p, 1]).wait()

    def late(p, carry):
        first = p * tiles

        def between(s, g):
            if p == 0 and g == 0:
                pl.when(s == n - 2)(lambda: pass_on(n - 1))
            if p > 0:
                @pl.when((s == n - 2) & (g == 0))
                def _():
                    with scope("project_out"):
                        for other in range(groups):
                            finish(p - 1, other)
                        project_out(p - 1)
                    for k in range(OUT_SLOTS):
                        wo_in(k).start()

        def scoped(name, step_fn):
            def run():
                with scope(name):
                    step_fn(p - 1)
            return run

        ticks = ((), ())
        if p > 0:
            ticks = ((((n - 1, 1), scoped("reduce", reduce)),), (((n - 2, 2), scoped("combine", combine)), ((n - 1, 2), scoped("forward", forward))))

        def late_set(s, carry):
            carry = run_unit(s, 0, first, tiles, carry, lambda: fetch(s, 1, "start"), ticks[0])
            between(s, 0)

            def fetch_next():
                @pl.when(s == n - 2)
                def _():
                    if p == 0:
                        for side in range(2):
                            to_pair(n - 1, side).wait_recv()
                        got_new(6)
                    fetch(n - 1, 0, "start")
                if p < phases - 1:
                    pl.when(s == n - 1)(lambda: fetch(n - 2, 0, "start"))

            return run_unit(s, 1, first, tiles, carry, fetch_next, ticks[1])

        return lax.fori_loop(n - 2, n, late_set, carry)

    for p in range(phases):
        carry = late(p, carry)
    last, last_slot, older, older_slot = carry
    with scope("finish"):
        step(None, main(last, last_slot), main(older, older_slot))
        step(None, None, main(last, last_slot))
        for g in range(groups):
            finish(phases - 1, g)
    with scope("project_out"):
        project_out(phases - 1)
    with scope("combine"):
        combine(phases - 1)
    with scope("reduce"):
        reduce(phases - 1)
    with scope("forward"):
        forward(phases - 1)

    for way in range(3):
        remote(stage, stage, own_send.at[way], recv.at[0, 0], "cp", me).wait_send()
    passed = ring_ref.at[pl.ds(2, n - 2), pl.ds(0, 2)]
    remote(passed, passed, pair_send, recv.at[0, 0], "cp", me).wait_send()
    for s in (2, 3):
        hop_right(s).wait_send()
    for s in (4, 5):
        hop_left(s).wait_send()
    for copy in (new_right, new_left, new_pair, new_hop, new_left_pair, new_right_pair, new_far_pair):
        copy.wait_send()

    with scope("drain_out"):
        for kind in range(3):
            part_sent(phases - 1, kind)
        for p in range(phases):
            every = y_buf.at[p]
            pltpu.make_async_copy(every, every, y_sem.at[p]).wait()
            for way in range(3):
                remote(every, every, y_send.at[p, way], y_last.at[p, 0], "tp", rank).wait_send()
            for way in range(2):
                remote(every, every, y_send.at[p, way], y_last.at[p, way], "tp", rank).wait_recv()


def results_kernel(y_in, kn_in, vn_in, y_out, kn_out, vn_out, y_buf, kn_buf, vn_buf, sem):
    pieces, _, cols = y_in.shape
    copies = [(y_in.at[k], y_buf.at[k], y_out.at[:, k * cols:(k + 1) * cols]) for k in range(pieces)]
    copies += [(kn_in, kn_buf, kn_out), (vn_in, vn_buf, vn_out)]
    for i, (src, buf, _) in enumerate(copies):
        pltpu.make_async_copy(src, buf, sem.at[0, i]).start()
    for i, (src, buf, dst) in enumerate(copies):
        pltpu.make_async_copy(src, buf, sem.at[0, i]).wait()
        pltpu.make_async_copy(buf, dst, sem.at[1, i]).start()
    for i, (_, buf, dst) in enumerate(copies):
        pltpu.make_async_copy(buf, dst, sem.at[1, i]).wait()


def results(y, new_k, new_v):
    any_spec = pl.BlockSpec(memory_space=pl.ANY)
    shapes = ((y.shape[1], y.shape[0] * y.shape[2]), new_k.shape, new_v.shape)
    return pl.pallas_call(
        results_kernel,
        in_specs=[any_spec] * 3,
        out_specs=[any_spec] * 3,
        out_shape=[jax.ShapeDtypeStruct(shape, BF16) for shape in shapes],
        scratch_shapes=[pltpu.VMEM(a.shape, a.dtype) for a in (y, new_k, new_v)] + [DMA((2, y.shape[0] + 2))],
        compiler_params=pltpu.CompilerParams(vmem_limit_bytes=62 << 20),
        name="results",
    )(y, new_k, new_v)


def local_step(n, ranks, x, k_cache, v_cache, rope_table, norm_gain, w_qkv, b_qkv, w_out):
    positions, groups, head_dim = k_cache.shape
    tok, width = x.shape
    heads = w_qkv.shape[1] // groups // head_dim - 2
    part = positions // CHUNKS
    span = positions + tok
    phases = tok // PHASE_TOKENS
    tiles = heads * PHASE_TOKENS // NC
    count = groups * phases * tiles
    pieces = width // COLS
    rows = PHASE_TOKENS // ranks
    depth = w_out.shape[0]
    any_spec = pl.BlockSpec(memory_space=pl.ANY)
    vmem_spec = pl.BlockSpec(memory_space=pltpu.VMEM)
    flat = (positions * groups, head_dim)
    flops = 4 * count * NC * LANES * n * (span + tok)
    y, new_k, new_v, _, _ = pl.pallas_call(
        functools.partial(block_kernel, (n, ranks, groups, heads)),
        in_specs=[any_spec, any_spec, any_spec, vmem_spec, vmem_spec, any_spec, vmem_spec, any_spec],
        out_specs=[any_spec] * 5,
        out_shape=[
            jax.ShapeDtypeStruct((pieces, tok, COLS), BF16),
            jax.ShapeDtypeStruct((tok * groups, head_dim), BF16),
            jax.ShapeDtypeStruct((tok * groups, head_dim), BF16),
            jax.ShapeDtypeStruct((n, CHUNKS, groups, 2, part, head_dim), BF16),
            jax.ShapeDtypeStruct((n, groups, 2, tok, head_dim), BF16),
        ],
        scratch_shapes=[
            pltpu.VMEM((2, span, LANES), BF16),
            pltpu.VMEM((2, span, LANES), BF16),
            pltpu.VMEM((CHUNKS, groups, 2, part, LANES), BF16),
            pltpu.VMEM((groups, 2, tok, LANES), BF16),
            pltpu.VMEM((count + 1, LANES, NC), BF16),
            pltpu.VMEM((tok, width), BF16),
            pltpu.VMEM((tok, width), BF16),
            pltpu.VMEM((max(3 * width, OUT_SLOTS * depth), COLS), BF16),
            pltpu.VMEM((tok, LANES), F32),
            pltpu.VMEM((tok, LANES), F32),
            pltpu.VMEM((tok * groups, LANES), BF16),
            pltpu.VMEM((tok * groups, LANES), BF16),
            pltpu.VMEM((max(span, w_qkv.shape[1] // COLS * tok), NC), F32),
            pltpu.VMEM((span, NC), BF16),
            pltpu.VMEM((count + 1, LANES, NC), F32),
            pltpu.VMEM((count, 1, NC), F32),
            pltpu.VMEM((count + 1, 8, NC), F32),
            pltpu.VMEM((8, NC), F32),
            pltpu.VMEM((2, 1, NC), F32),
            pltpu.VMEM((tok, NC), jnp.int32),
            pltpu.VMEM((PHASE_TOKENS, groups * heads * LANES), BF16),
            pltpu.VMEM((2, PHASE_TOKENS, COLS), F32),
            pltpu.VMEM((pieces, rows, COLS), F32),
            pltpu.VMEM((pieces, rows, COLS), F32),
            pltpu.VMEM((pieces, PHASE_TOKENS, COLS), BF16),
            pltpu.VMEM((pieces, rows, COLS), BF16),
            pltpu.VMEM((phases, 3, pieces, rows, COLS), BF16),
            pltpu.VMEM((phases, pieces, rows, COLS), BF16),
            DMA((2 + phases, 2)),
            DMA((OUT_SLOTS,)),
            DMA((CHUNKS + 3,)),
            DMA((groups, 2, CHUNKS + 1)),
            DMA((3,)),
            DMA,
            DMA((n,)),
            DMA((7,)),
            DMA((n, CHUNKS)),
            DMA((7,)),
            DMA((phases, 3)),
            DMA((phases, 2, pieces // 2 + 1)),
            DMA((phases, 3)),
            DMA((phases, pieces // 2 + 1)),
            DMA((phases, 2)),
            DMA((phases,)),
        ],
        cost_estimate=pl.CostEstimate(flops=flops, bytes_accessed=4 * positions * n * groups * head_dim, transcendentals=flops // (4 * LANES)),
        compiler_params=pltpu.CompilerParams(collective_id=0, has_side_effects=True, vmem_limit_bytes=63 << 20),
        name="block",
    )(x, k_cache.reshape(flat), v_cache.reshape(flat), rope_table.T, norm_gain, w_qkv, b_qkv, w_out)
    y, new_k, new_v = results(y, new_k, new_v)
    new_shape = (tok,) + k_cache.shape[1:]
    return y, new_k.reshape(new_shape), new_v.reshape(new_shape)


def solution(mesh):
    row_spec = P(("dp", "cp"), None)
    cache_spec = P(("dp", "cp"), "tp", None)
    body = functools.partial(local_step, mesh.shape["cp"], mesh.shape["tp"])
    return jax.shard_map(body, mesh=mesh, in_specs=(row_spec, cache_spec, cache_spec, row_spec, P(None), P(None, "tp"), P("tp"), P("tp", None)), out_specs=(row_spec, cache_spec, cache_spec), check_vma=False)
```

```python
import functools
import math

import jax
import jax.numpy as jnp
from jax import lax
from jax.experimental import pallas as pl
from jax.experimental.pallas import tpu as pltpu
from jax.sharding import PartitionSpec as P

EPS = 1.5625e-07
MASK_VALUE = -1e30
LANES = 128
SUB = 256
NC = 512
PHASE_TOKENS = 128
CHUNKS = 4
COLS = 512
OUT_SLOTS = 7
MESH = pl.DeviceIdType.MESH
F32 = jnp.float32
BF16 = jnp.bfloat16
DMA = pltpu.SemaphoreType.DMA


def dot(a, b, dims=(((1,), (0,)), ((), ()))):
    return lax.dot_general(a, b, dims, preferred_element_type=F32)


def block_kernel(dims, x_ref, kc_ref, vc_ref, table_ref, g_ref, wq_ref, b_ref, wo_ref,
                 y_ref, kn_ref, vn_ref, ring_ref, ringn_ref,
                 k_buf, v_buf, stage, kvn, qt_ref, hid_ref, x_buf, w_buf, cos_ref, sin_ref, kn_buf, vn_buf,
                 s_ref, p_ref, acc_ref, m_ref, l_ref, mc_ref, al_ref, diff_ref,
                 o_buf, full_buf, mine_buf, near_buf, send_buf, comb_buf, got_buf, y_buf,
                 in_sem, w_sem, out_sem, fetch_sem, own_send, pair_send, hop_send, new_send, recv, new_recv,
                 part_send, part_recv, y_send, y_recv, y_last, y_sem):
    n, ranks, groups, heads = dims
    me = lax.axis_index("cp")
    rank = lax.axis_index("tp")
    pair = me + 1 - 2 * lax.rem(me, 2)
    right, left, far = lax.rem(me + 2, n), lax.rem(me + n - 2, n), lax.rem(me + 4, n)
    tok, width = x_ref.shape
    part = stage.shape[3]
    span = CHUNKS * part + tok
    phases = tok // PHASE_TOKENS
    heads_per_tile = NC // PHASE_TOKENS
    tiles = heads // heads_per_tile
    per_group = phases * tiles
    count = groups * per_group
    spare = count
    half = kc_ref.shape[0] // 2
    scale = LANES ** -0.5 * math.log2(math.e)
    head_count = groups * (heads + 2)
    w_blocks = head_count * LANES // COLS
    heads_per_block = COLS // LANES
    pieces = width // COLS
    w_slots = w_buf.shape[0] // width
    out_depth = wo_ref.shape[0]
    rows = PHASE_TOKENS // ranks

    def remote(src, dst, send, got, axis, where):
        return pltpu.make_async_remote_copy(src_ref=src, dst_ref=dst, send_sem=send, recv_sem=got, device_id={axis: where}, device_id_type=MESH)

    def own_pair(c):
        return remote(stage.at[c], ring_ref.at[1, c], own_send.at[0], recv.at[1, c], "cp", pair)

    def own_right(c):
        return remote(stage.at[c], ring_ref.at[2 + c, 0], own_send.at[1], recv.at[2 + c, 0], "cp", right)

    def own_left(c):
        return remote(stage.at[c], ring_ref.at[2 + c, 1], own_send.at[2], recv.at[2 + c, 1], "cp", left)

    def to_pair(s, side):
        return remote(ring_ref.at[s, side], ring_ref.at[s, 2 + side], pair_send, recv.at[s, 2 + side], "cp", pair)

    def from_side(s, side):
        return remote(stage.at[0], ring_ref.at[s, side], own_send.at[0], recv.at[s, side], "cp", pair)

    def hop_right(s):
        return remote(ring_ref.at[s, 0], ring_ref.at[s + 4, 0], hop_send.at[s], recv.at[s + 4, 0], "cp", right)

    def hop_left(s):
        return remote(ring_ref.at[s, 1], ring_ref.at[s + 2, 1], hop_send.at[s], recv.at[s + 2, 1], "cp", left)

    def new_copy(source, send, got, where, own=False):
        src = kvn if own else ringn_ref.at[source]
        return remote(src, ringn_ref.at[source], new_send.at[send], new_recv.at[got], "cp", where)

    new_right = new_copy(me, 0, 0, right, own=True)
    new_left = new_copy(me, 1, 1, left, own=True)
    new_pair = new_copy(me, 2, 3, pair, own=True)
    new_hop = new_copy(left, 3, 2, right)
    new_left_pair = new_copy(left, 4, 4, pair)
    new_right_pair = new_copy(right, 5, 5, pair)
    new_far_pair = new_copy(far, 6, 6, pair)

    def pass_on(s):
        for side in range(2):
            from_side(s, side).wait_recv()
            to_pair(s, side).start()

    def cache_in(i):
        here = pl.ds(i * half, half)
        return (pltpu.make_async_copy(kc_ref.at[here], k_buf.at[i, pl.ds(0, half)], in_sem.at[0, i]),
                pltpu.make_async_copy(vc_ref.at[here], v_buf.at[i, pl.ds(0, half)], in_sem.at[1, i]))

    x_in = pltpu.make_async_copy(x_ref, x_buf, in_sem.at[2, 0])

    def res_in(p, k):
        here = pl.ds(pl.multiple_of(p * PHASE_TOKENS + rank * rows, rows), rows)
        return pltpu.make_async_copy(x_ref.at[here, k * COLS:(k + 1) * COLS], y_buf.at[p, k], in_sem.at[2 + p, 1])

    def w_in(j, slot):
        cols = pl.ds(pl.multiple_of(j * COLS, COLS), COLS)
        here = pl.ds(pl.multiple_of(slot * width, width), width)
        return pltpu.make_async_copy(wq_ref.at[:, cols], w_buf.at[here], w_sem.at[slot])

    def order(j):
        return lax.rem(j + heads * LANES // COLS, w_blocks)

    def wo_at(slot):
        return pl.ds(pl.multiple_of(slot * out_depth, out_depth), out_depth)

    def wo_in(k):
        slot = lax.rem(k, OUT_SLOTS)
        cols = pl.ds(pl.multiple_of(k * COLS, COLS), COLS)
        return pltpu.make_async_copy(wo_ref.at[:, cols], w_buf.at[wo_at(slot)], w_sem.at[slot])

    x_in.start()
    for i in range(2):
        for copy in cache_in(i):
            copy.start()
    w_in(order(0), 0).start()
    for p in range(phases):
        for k in range(pieces):
            res_in(p, k).start()

    barrier = pltpu.get_barrier_semaphore()
    for other in (pair, right, left):
        pl.semaphore_signal(barrier, inc=1, device_id={"cp": other}, device_id_type=MESH)
    for d in range(1, ranks):
        pl.semaphore_signal(barrier, inc=1, device_id={"tp": lax.rem(rank + d, ranks)}, device_id_type=MESH)

    row = lax.broadcasted_iota(jnp.int32, (tok, NC), 0)
    diff_ref[...] = row - lax.rem(lax.broadcasted_iota(jnp.int32, (tok, NC), 1), PHASE_TOKENS)

    m_ref[...] = jnp.full(m_ref.shape, MASK_VALUE, F32)
    l_ref[...] = jnp.zeros(l_ref.shape, F32)
    acc_ref[...] = jnp.zeros(acc_ref.shape, F32)
    mc_ref[...] = jnp.zeros(mc_ref.shape, F32)
    al_ref[...] = jnp.ones(al_ref.shape, F32)

    x_in.wait()
    for j in range(1, w_slots):
        w_in(order(j), j).start()
    gain = g_ref[...].astype(F32).reshape(1, width)
    norm_rows = tok // (CHUNKS * (part // LANES // 4))

    def norm(i):
        here = pl.ds(pl.multiple_of(i * norm_rows, norm_rows), norm_rows)
        x = x_buf[here, :].astype(F32)
        inv_rms = lax.rsqrt(jnp.mean(x * x, axis=-1, keepdims=True) + EPS)
        hid_ref[here, :] = (x * inv_rms * gain).astype(BF16)

    pair_rows = groups * LANES
    wide = lax.broadcasted_iota(jnp.int32, (pair_rows, pair_rows), 0)
    tall = lax.broadcasted_iota(jnp.int32, (pair_rows, pair_rows), 1)
    pick = (wide // groups + (wide % groups) * LANES == tall).astype(BF16)
    pick_t = (tall // groups + (tall % groups) * LANES == wide).astype(BF16)
    blocks = part // LANES

    def stage_out(c):
        return pltpu.make_async_copy(stage.at[c], ring_ref.at[0, c], out_sem.at[c])

    for c in range(CHUNKS):
        if c % (CHUNKS // 2) == 0:
            for copy in cache_in(c // (CHUNKS // 2)):
                copy.wait()

        def relayout(i, _):
            i_half = c // (CHUNKS // 2)
            for sub in range(4):
                at = i * 4 + sub
                src = pl.ds(pl.multiple_of((c % (CHUNKS // 2)) * part * groups + at * pair_rows, pair_rows), pair_rows)
                here = pl.ds(pl.multiple_of(at * LANES, LANES), LANES)
                keys = dot(pick_t, k_buf[i_half, src, :]).astype(BF16)
                vals = dot(v_buf[i_half, src, :], pick, (((0,), (0,)), ((), ()))).astype(BF16)
                for g in range(groups):
                    stage[c, g, 0, here, :] = keys[g * LANES:(g + 1) * LANES, :]
                    stage[c, g, 1, here, :] = vals[:, g * LANES:(g + 1) * LANES]
            norm(c * (blocks // 4) + i)
            return 0

        lax.fori_loop(0, blocks // 4, relayout, 0)
        stage_out(c).start()

    def send_own(chunks):
        for c in chunks:
            own_right(c).start()
            own_left(c).start()
            own_pair(c).start()

    pl.semaphore_wait(barrier, 3 + ranks - 1)
    send_own(range(1))

    lane = lax.broadcasted_iota(jnp.int32, (tok, LANES), 1)
    rope_lanes = table_ref.shape[0]
    table = jnp.concatenate([table_ref[...].T, jnp.zeros((tok, LANES - rope_lanes), F32)], axis=1)
    at = jnp.where(lane < rope_lanes, lane // 2, 0)
    sin = jnp.take_along_axis(table, at + rope_lanes // 2, axis=1)
    cos_ref[...] = jnp.take_along_axis(table, at, axis=1)
    sin_ref[...] = jnp.where(lane % 2 == 0, -sin, sin)

    def rotate(head):
        swapped = jnp.where(lane % 2 == 0, pltpu.roll(head, LANES - 1, 1), pltpu.roll(head, 1, 1))
        turned = head * cos_ref[...] + swapped * sin_ref[...]
        return jnp.where(lane < rope_lanes, turned, head)

    pair_left, pair_right, pair_far = lax.rem(pair + n - 2, n), lax.rem(pair + 2, n), lax.rem(pair + 4, n)

    def block_of(s):
        out = me
        for i, source in enumerate((pair, left, right, pair_left, pair_right, far, pair_far)):
            out = jnp.where(s == i + 1, source, out)
        return out

    def fetch_cache(s, g, act):
        for kind, buf in ((0, k_buf), (1, v_buf)):
            for c in range(CHUNKS):
                here = pl.ds(c * part, part)
                getattr(pltpu.make_async_copy(ring_ref.at[s, c, g, kind], buf.at[g, here], fetch_sem.at[g, kind, c]), act)()

    def fetch_block(s, g, act):
        for kind, buf in ((0, k_buf), (1, v_buf)):
            here = pl.ds(CHUNKS * part, tok)
            getattr(pltpu.make_async_copy(ringn_ref.at[block_of(s), g, kind], buf.at[g, here], fetch_sem.at[g, kind, CHUNKS]), act)()

    def fetch(s, g, act):
        fetch_cache(s, g, act)
        fetch_block(s, g, act)

    def a_rows(j):
        return pl.ds(pl.multiple_of(j * tok, tok), tok)

    def queries(j, i):
        head = j * heads_per_block + i
        g, h = head // (heads + 2), lax.rem(head, heads + 2)
        turned = rotate(s_ref[a_rows(j), i * LANES:(i + 1) * LANES]).T.astype(BF16)
        for p in range(phases):
            tile = jnp.where(h < heads, g * per_group + p * tiles + h // heads_per_tile, spare)
            at = pl.multiple_of(lax.rem(h, heads_per_tile) * PHASE_TOKENS, PHASE_TOKENS)
            qt_ref[tile, :, pl.ds(at, PHASE_TOKENS)] = turned[:, p * PHASE_TOKENS:(p + 1) * PHASE_TOKENS]

    def project(j, _):
        slot = lax.rem(j, w_slots)
        block = order(j)
        w_in(block, slot).wait()
        here = pl.ds(pl.multiple_of(slot * width, width), width)
        cols = pl.ds(pl.multiple_of(block * COLS, COLS), COLS)
        before = order(jnp.maximum(j - 1, 0))
        for i in range(heads_per_block):
            queries(before, i)
        s_ref[a_rows(block), :] = dot(hid_ref[...], w_buf[here, :]) + b_ref[cols].astype(F32).reshape(1, COLS)

        @pl.when(j + w_slots < w_blocks)
        def _():
            w_in(order(j + w_slots), slot).start()
        return 0

    early = ((groups - 1) * (heads + 2) + heads) * LANES // COLS - heads * LANES // COLS + 1
    lax.fori_loop(0, early, project, 0)
    for c in range(CHUNKS):
        stage_out(c).wait()
    fetch_cache(0, 0, "start")

    kn_out = pltpu.make_async_copy(kn_buf, kn_ref, out_sem.at[CHUNKS])
    vn_out = pltpu.make_async_copy(vn_buf, vn_ref, out_sem.at[CHUNKS + 1])
    fresh = []
    kvn_out = pltpu.make_async_copy(kvn, ringn_ref.at[me], out_sem.at[CHUNKS + 2])
    for g in range(groups):
        at = (g * (heads + 2) + heads) * LANES
        keys = rotate(s_ref[a_rows(at // COLS), at % COLS:at % COLS + LANES])
        at += LANES
        vals = s_ref[a_rows(at // COLS), at % COLS:at % COLS + LANES]
        fresh.append((keys.astype(BF16), vals.astype(BF16)))
        kvn[g, 0] = keys.astype(BF16)
        for i in range(tok // LANES):
            here = slice(i * LANES, (i + 1) * LANES)
            kvn[g, 1, here, :] = vals[here, :].T.astype(BF16)
    for i in range(tok // LANES):
        here = slice(i * LANES, (i + 1) * LANES)
        for kind, buf in ((0, kn_buf), (1, vn_buf)):
            block = jnp.concatenate([fresh[g][kind][here, :] for g in range(groups)], axis=0)
            buf[i * pair_rows:(i + 1) * pair_rows, :] = dot(pick, block).astype(BF16)
    kvn_out.start()
    for copy in (new_right, new_left, new_pair):
        copy.start()
    send_own(range(1, CHUNKS))
    kn_out.start()
    vn_out.start()
    lax.fori_loop(early, w_blocks, project, 0)
    for i in range(heads_per_block):
        queries(order(w_blocks - 1), i)
    kvn_out.wait()
    fetch_block(0, 0, "start")

    def step(a=None, b=None, c=None):
        alpha_b, alpha_c = al_ref[0], al_ref[1]
        shift = mc_ref[...]
        run = {"max": None, "sum": None, "out": None}

        def scores(i):
            keys = k_buf[a["slot"], i * SUB:(i + 1) * SUB, :]
            s = dot(keys, qt_ref[a["tile"]])
            if i == new_block:
                limit = (me - a["block"]) * tok + lax.rem(a["tile"], per_group) // tiles * PHASE_TOKENS
                s = jnp.where(diff_ref[...] <= limit, s, MASK_VALUE)
            s_ref[i * SUB:(i + 1) * SUB, :] = s
            top = jnp.max(s.reshape(SUB // 8, 8, NC), axis=0)
            run["max"] = top if run["max"] is None else jnp.maximum(run["max"], top)

        def weights(i):
            s = s_ref[i * SUB:(i + 1) * SUB, :]
            e = jnp.exp2((s * scale).reshape(SUB // 8, 8, NC) - shift[None])
            part_sum = jnp.sum(e, axis=0)
            run["sum"] = part_sum if run["sum"] is None else run["sum"] + part_sum
            p_ref[i * SUB:(i + 1) * SUB, :] = e.reshape(SUB, NC).astype(BF16)

        def values(i):
            at = i * SUB
            block = jnp.concatenate([v_buf[c["slot"], at + h * LANES:at + (h + 1) * LANES, :] for h in range(SUB // LANES)], axis=1)
            out = dot(block, p_ref[i * SUB:(i + 1) * SUB, :])
            run["out"] = out if run["out"] is None else run["out"] + out

        stages = ((c, values), (b, weights), (a, scores))
        new_block = (span - tok) // SUB
        for i in (new_block, *range(new_block)):
            for spec, stage_fn in stages:
                if spec is not None:
                    stage_fn(i)
        if c is not None:
            acc_ref[c["tile"]] = acc_ref[c["tile"]] * alpha_c + run["out"]
        if b is not None:
            l_ref[b["tile"]] = l_ref[b["tile"]] * alpha_b + run["sum"]
            al_ref[1] = alpha_b
        if a is not None:
            old = m_ref[a["tile"]]
            new = jnp.maximum(old, jnp.max(run["max"], axis=0, keepdims=True))
            m_ref[a["tile"]] = new
            mc_ref[...] = jnp.broadcast_to(new * scale, mc_ref.shape)
            al_ref[0] = jnp.exp2((old - new) * scale)

    def main(tile, slot, block=None):
        return {"tile": tile, "slot": slot, "block": block}

    def run_unit(s, g, first, tile_count, carry, fetch_next, ticks=()):
        fetch(s, g, "wait")
        block = block_of(s)

        def one_tile(t, carry):
            for at, what in ticks:
                pl.when((s == at[0]) & (t == at[1]))(what)
            pl.when(t == tile_count - 1)(fetch_next)
            last, last_slot, older, older_slot = carry
            tile = g * per_group + first + t
            step(main(tile, g, block), main(last, last_slot), main(older, older_slot))
            return tile, jnp.int32(g), last, last_slot

        return lax.fori_loop(0, tile_count, one_tile, carry)

    start = tuple(jnp.int32(v) for v in (spare, 0, spare, 0))

    def got_new(i):
        new_copy(pair, 0, i, pair).wait_recv()

    def one_set(s, carry):
        nxt = s + 1
        carry = run_unit(s, 0, 0, per_group, carry, lambda: fetch(s, 1, "start"))
        pl.when(s >= 1)(lambda: pass_on(nxt))

        @pl.when(s == 1)
        def _():
            for k in range(OUT_SLOTS):
                wo_in(k).start()

        @pl.when(s == 2)
        def _():
            for copy in (new_hop, new_left_pair, new_right_pair):
                copy.start()

        pl.when((s >= 1) & (s <= 2))(lambda: hop_right(nxt).start())
        pl.when((s >= 3) & (s <= 4))(lambda: hop_left(nxt).start())

        @pl.when(s == n - 3)
        def _():
            got_new(2)
            new_far_pair.start()

        def fetch_next():
            @pl.when(s == 0)
            def _():
                for c in range(CHUNKS):
                    own_pair(c).wait_recv()
                got_new(3)

            @pl.when(s >= 1)
            def _():
                for side in range(2):
                    to_pair(nxt, side).wait_recv()

            @pl.when(s == 1)
            def _():
                got_new(0)
                got_new(1)

            pl.when(s == 3)(lambda: got_new(4))
            pl.when(s == 4)(lambda: got_new(5))
            fetch(nxt, 0, "start")

        return run_unit(s, 1, 0, per_group, carry, fetch_next)

    carry = lax.fori_loop(0, n - 2, one_set, start)
    kn_out.wait()
    vn_out.wait()

    right_rank, left_rank, far_rank = lax.rem(rank + 1, ranks), lax.rem(rank + ranks - 1, ranks), lax.rem(rank + 2, ranks)

    pairs = pieces // 2 - 1
    singles = ((pairs, pieces - 2), (pairs + 1, pieces - 1))

    def onward(i):
        return jnp.where(lax.rem(i, 2) == 0, right_rank, left_rank)

    def back(i):
        return jnp.where(lax.rem(i, 2) == 0, left_rank, right_rank)

    def band(of):
        return pl.ds(pl.multiple_of(of * rows, rows), rows)

    def far_copy(p, i, at):
        return remote(send_buf.at[at, band(far_rank)], got_buf.at[p, 0, at], part_send.at[p, 0], part_recv.at[p, 0, i], "tp", onward(i))

    def near_copy(p, i, at):
        return remote(send_buf.at[at, band(back(i))], got_buf.at[p, 1, at], part_send.at[p, 1], part_recv.at[p, 1, i], "tp", back(i))

    def comb_copy(p, i, at):
        return remote(comb_buf.at[at], got_buf.at[p, 2, at], part_send.at[p, 2], part_recv.at[p, 1, i], "tp", onward(i))

    def y_rows(p, of):
        return pl.ds(pl.multiple_of(p * PHASE_TOKENS + of * rows, rows), rows)

    def y_copy(p, i, at, way):
        got = y_last.at[p, 0] if way else y_recv.at[p, i]
        return remote(y_buf.at[p, at], y_ref.at[at, y_rows(p, rank)], y_send.at[p, way], got, "tp", back(i) if way else onward(i))

    def y_forward(p, i, at):
        here = y_ref.at[at, y_rows(p, back(i))]
        return remote(here, here, y_send.at[p, 2], y_last.at[p, 1], "tp", onward(i))

    def y_own(p, at):
        return pltpu.make_async_copy(y_buf.at[p, at], y_ref.at[at, y_rows(p, rank)], y_sem.at[p])

    def pair_at(i):
        return pl.ds(2 * i, 2)

    def each_group(work, send):
        def step_of(i, _):
            pl.when(i < pairs)(lambda: [work(i, 2 * i, 2), None][1])
            pl.when(i > 0)(lambda: [send(i - 1, pair_at(i - 1)), None][1])
            return 0

        lax.fori_loop(0, pairs + 1, step_of, 0)
        for i, k in singles:
            work(i, k, 1)
        for i, k in singles:
            send(i, pl.ds(k, 1))

    def part_sent(p, kind):
        every = got_buf.at[p, kind]
        remote(every, every, part_send.at[p, kind], part_recv.at[p, 0, 0], "tp", rank).wait_send()

    def project_out(p):
        if p > 0:
            for kind in range(2):
                part_sent(p - 1, kind)

        def two(j, _):
            @pl.when(j < pieces // 2)
            def _():
                both = (2 * j, 2 * j + 1)
                for k in both:
                    wo_in(k).wait()
                for i, k in enumerate(both):
                    out = dot(o_buf[...], w_buf[wo_at(lax.rem(k, OUT_SLOTS)), :])
                    full_buf[i] = out
                    send_buf[k] = out.astype(BF16)
                for i, k in enumerate(both):
                    mine_buf[k] = full_buf[i, band(rank), :]
                    way = jnp.where(j < pairs, j, pairs + i)
                    near_buf[k] = full_buf[i, band(onward(way)), :]
                for k in both:
                    pl.when(k + OUT_SLOTS < pieces)(lambda k=k: wo_in(k + OUT_SLOTS).start())

            @pl.when(j >= 1)
            def _():
                @pl.when(j <= pairs)
                def _():
                    far_copy(p, j - 1, pair_at(j - 1)).start()
                    near_copy(p, j - 1, pair_at(j - 1)).start()

                @pl.when(j > pairs)
                def _():
                    for i, k in singles:
                        far_copy(p, i, pl.ds(k, 1)).start()
                        near_copy(p, i, pl.ds(k, 1)).start()
            return 0

        lax.fori_loop(0, pieces // 2 + 1, two, 0)

    def combine(p):
        if p > 0:
            part_sent(p - 1, 2)

        def work(i, k, size):
            far_copy(p, i, pl.ds(k, size)).wait_recv()
            for j in range(size):
                comb_buf[k + j] = (near_buf[k + j] + got_buf[p, 0, k + j].astype(F32)).astype(BF16)

        each_group(work, lambda i, at: comb_copy(p, i, at).start())

    def reduce(p):
        def work(i, k, size):
            both = got_buf.at[p, pl.ds(1, 2), pl.ds(k, size)]
            remote(both, both, part_send.at[p, 1], part_recv.at[p, 1, i], "tp", rank).wait_recv()
            for j in range(size):
                total = mine_buf[k + j] + got_buf[p, 1, k + j].astype(F32) + got_buf[p, 2, k + j].astype(F32)
                y_buf[p, k + j] = (y_buf[p, k + j].astype(F32) + total).astype(BF16)

        def send(i, at):
            y_copy(p, i, at, 0).start()
            y_copy(p, i, at, 1).start()
            y_own(p, at).start()

        each_group(work, send)

    def forward(p):
        def work(i, k, size):
            at = pl.ds(k, size)
            y_copy(p, i, at, 0).wait_recv()
            y_forward(p, i, at).start()

        def pair_of(i, _):
            work(i, 2 * i, 2)
            return 0

        lax.fori_loop(0, pairs, pair_of, 0)
        for i, k in singles:
            work(i, k, 1)

    def finish(p, g):
        def tile(h, _):
            t = g * per_group + p * tiles + h
            total = jnp.sum(l_ref[t], axis=0, keepdims=True)
            out = (acc_ref[t] / total).T.astype(BF16)
            for i in range(heads_per_tile):
                at = pl.multiple_of((g * heads + h * heads_per_tile + i) * LANES, LANES)
                o_buf[:, pl.ds(at, LANES)] = out[i * PHASE_TOKENS:(i + 1) * PHASE_TOKENS, :]
            return 0

        lax.fori_loop(0, tiles, tile, 0)

    for p in range(phases):
        pltpu.make_async_copy(y_buf.at[p], y_buf.at[p], in_sem.at[2 + p, 1]).wait()

    def late(p, carry):
        first = p * tiles

        def between(s, g):
            if p == 0 and g == 0:
                pl.when(s == n - 2)(lambda: pass_on(n - 1))
            if p > 0:
                @pl.when((s == n - 2) & (g == 0))
                def _():
                    for other in range(groups):
                        finish(p - 1, other)
                    project_out(p - 1)
                    for k in range(OUT_SLOTS):
                        wo_in(k).start()

        ticks = ((), ())
        if p > 0:
            ticks = ((((n - 1, 1), lambda: reduce(p - 1)),), (((n - 2, 2), lambda: combine(p - 1)), ((n - 1, 2), lambda: forward(p - 1))))

        def late_set(s, carry):
            carry = run_unit(s, 0, first, tiles, carry, lambda: fetch(s, 1, "start"), ticks[0])
            between(s, 0)

            def fetch_next():
                @pl.when(s == n - 2)
                def _():
                    if p == 0:
                        for side in range(2):
                            to_pair(n - 1, side).wait_recv()
                        got_new(6)
                    fetch(n - 1, 0, "start")
                if p < phases - 1:
                    pl.when(s == n - 1)(lambda: fetch(n - 2, 0, "start"))

            return run_unit(s, 1, first, tiles, carry, fetch_next, ticks[1])

        return lax.fori_loop(n - 2, n, late_set, carry)

    for p in range(phases):
        carry = late(p, carry)
    last, last_slot, older, older_slot = carry
    step(None, main(last, last_slot), main(older, older_slot))
    step(None, None, main(last, last_slot))
    for g in range(groups):
        finish(phases - 1, g)
    project_out(phases - 1)
    combine(phases - 1)
    reduce(phases - 1)
    forward(phases - 1)

    for way in range(3):
        remote(stage, stage, own_send.at[way], recv.at[0, 0], "cp", me).wait_send()
    passed = ring_ref.at[pl.ds(2, n - 2), pl.ds(0, 2)]
    remote(passed, passed, pair_send, recv.at[0, 0], "cp", me).wait_send()
    for s in (2, 3):
        hop_right(s).wait_send()
    for s in (4, 5):
        hop_left(s).wait_send()
    for copy in (new_right, new_left, new_pair, new_hop, new_left_pair, new_right_pair, new_far_pair):
        copy.wait_send()

    for kind in range(3):
        part_sent(phases - 1, kind)
    for p in range(phases):
        every = y_buf.at[p]
        pltpu.make_async_copy(every, every, y_sem.at[p]).wait()
        for way in range(3):
            remote(every, every, y_send.at[p, way], y_last.at[p, 0], "tp", rank).wait_send()
        for way in range(2):
            remote(every, every, y_send.at[p, way], y_last.at[p, way], "tp", rank).wait_recv()


def results_kernel(y_in, kn_in, vn_in, y_out, kn_out, vn_out, y_buf, kn_buf, vn_buf, sem):
    pieces, _, cols = y_in.shape
    copies = [(y_in.at[k], y_buf.at[k], y_out.at[:, k * cols:(k + 1) * cols]) for k in range(pieces)]
    copies += [(kn_in, kn_buf, kn_out), (vn_in, vn_buf, vn_out)]
    for i, (src, buf, _) in enumerate(copies):
        pltpu.make_async_copy(src, buf, sem.at[0, i]).start()
    for i, (src, buf, dst) in enumerate(copies):
        pltpu.make_async_copy(src, buf, sem.at[0, i]).wait()
        pltpu.make_async_copy(buf, dst, sem.at[1, i]).start()
    for i, (_, buf, dst) in enumerate(copies):
        pltpu.make_async_copy(buf, dst, sem.at[1, i]).wait()


def results(y, new_k, new_v):
    any_spec = pl.BlockSpec(memory_space=pl.ANY)
    shapes = ((y.shape[1], y.shape[0] * y.shape[2]), new_k.shape, new_v.shape)
    return pl.pallas_call(
        results_kernel,
        in_specs=[any_spec] * 3,
        out_specs=[any_spec] * 3,
        out_shape=[jax.ShapeDtypeStruct(shape, BF16) for shape in shapes],
        scratch_shapes=[pltpu.VMEM(a.shape, a.dtype) for a in (y, new_k, new_v)] + [DMA((2, y.shape[0] + 2))],
        compiler_params=pltpu.CompilerParams(vmem_limit_bytes=62 << 20),
        name="results",
    )(y, new_k, new_v)


def local_step(n, ranks, x, k_cache, v_cache, rope_table, norm_gain, w_qkv, b_qkv, w_out):
    positions, groups, head_dim = k_cache.shape
    tok, width = x.shape
    heads = w_qkv.shape[1] // groups // head_dim - 2
    part = positions // CHUNKS
    span = positions + tok
    phases = tok // PHASE_TOKENS
    tiles = heads * PHASE_TOKENS // NC
    count = groups * phases * tiles
    pieces = width // COLS
    rows = PHASE_TOKENS // ranks
    depth = w_out.shape[0]
    any_spec = pl.BlockSpec(memory_space=pl.ANY)
    vmem_spec = pl.BlockSpec(memory_space=pltpu.VMEM)
    flat = (positions * groups, head_dim)
    flops = 4 * count * NC * LANES * n * (span + tok)
    y, new_k, new_v, _, _ = pl.pallas_call(
        functools.partial(block_kernel, (n, ranks, groups, heads)),
        in_specs=[any_spec, any_spec, any_spec, vmem_spec, vmem_spec, any_spec, vmem_spec, any_spec],
        out_specs=[any_spec] * 5,
        out_shape=[
            jax.ShapeDtypeStruct((pieces, tok, COLS), BF16),
            jax.ShapeDtypeStruct((tok * groups, head_dim), BF16),
            jax.ShapeDtypeStruct((tok * groups, head_dim), BF16),
            jax.ShapeDtypeStruct((n, CHUNKS, groups, 2, part, head_dim), BF16),
            jax.ShapeDtypeStruct((n, groups, 2, tok, head_dim), BF16),
        ],
        scratch_shapes=[
            pltpu.VMEM((2, span, LANES), BF16),
            pltpu.VMEM((2, span, LANES), BF16),
            pltpu.VMEM((CHUNKS, groups, 2, part, LANES), BF16),
            pltpu.VMEM((groups, 2, tok, LANES), BF16),
            pltpu.VMEM((count + 1, LANES, NC), BF16),
            pltpu.VMEM((tok, width), BF16),
            pltpu.VMEM((tok, width), BF16),
            pltpu.VMEM((max(3 * width, OUT_SLOTS * depth), COLS), BF16),
            pltpu.VMEM((tok, LANES), F32),
            pltpu.VMEM((tok, LANES), F32),
            pltpu.VMEM((tok * groups, LANES), BF16),
            pltpu.VMEM((tok * groups, LANES), BF16),
            pltpu.VMEM((max(span, w_qkv.shape[1] // COLS * tok), NC), F32),
            pltpu.VMEM((span, NC), BF16),
            pltpu.VMEM((count + 1, LANES, NC), F32),
            pltpu.VMEM((count, 1, NC), F32),
            pltpu.VMEM((count + 1, 8, NC), F32),
            pltpu.VMEM((8, NC), F32),
            pltpu.VMEM((2, 1, NC), F32),
            pltpu.VMEM((tok, NC), jnp.int32),
            pltpu.VMEM((PHASE_TOKENS, groups * heads * LANES), BF16),
            pltpu.VMEM((2, PHASE_TOKENS, COLS), F32),
            pltpu.VMEM((pieces, rows, COLS), F32),
            pltpu.VMEM((pieces, rows, COLS), F32),
            pltpu.VMEM((pieces, PHASE_TOKENS, COLS), BF16),
            pltpu.VMEM((pieces, rows, COLS), BF16),
            pltpu.VMEM((phases, 3, pieces, rows, COLS), BF16),
            pltpu.VMEM((phases, pieces, rows, COLS), BF16),
            DMA((2 + phases, 2)),
            DMA((OUT_SLOTS,)),
            DMA((CHUNKS + 3,)),
            DMA((groups, 2, CHUNKS + 1)),
            DMA((3,)),
            DMA,
            DMA((n,)),
            DMA((7,)),
            DMA((n, CHUNKS)),
            DMA((7,)),
            DMA((phases, 3)),
            DMA((phases, 2, pieces // 2 + 1)),
            DMA((phases, 3)),
            DMA((phases, pieces // 2 + 1)),
            DMA((phases, 2)),
            DMA((phases,)),
        ],
        cost_estimate=pl.CostEstimate(flops=flops, bytes_accessed=4 * positions * n * groups * head_dim, transcendentals=flops // (4 * LANES)),
        compiler_params=pltpu.CompilerParams(collective_id=0, has_side_effects=True, vmem_limit_bytes=63 << 20),
        name="block",
    )(x, k_cache.reshape(flat), v_cache.reshape(flat), rope_table.T, norm_gain, w_qkv, b_qkv, w_out)
    y, new_k, new_v = results(y, new_k, new_v)
    new_shape = (tok,) + k_cache.shape[1:]
    return y, new_k.reshape(new_shape), new_v.reshape(new_shape)


def solution(mesh):
    row_spec = P(("dp", "cp"), None)
    cache_spec = P(("dp", "cp"), "tp", None)
    body = functools.partial(local_step, mesh.shape["cp"], mesh.shape["tp"])
    return jax.shard_map(body, mesh=mesh, in_specs=(row_spec, cache_spec, cache_spec, row_spec, P(None), P(None, "tp"), P("tp"), P("tp", None)), out_specs=(row_spec, cache_spec, cache_spec), check_vma=False)
```
